512 devices in a mesh: parts: 2 (over y), slab: 16 (over x, core), pencil: 16 (over z).
Axes of the slice: x: 8, y: 2, z: 16, core: 2. Of those that a mesh axis runs over, the one named last changes fastest.
The devices are a block of a 8x8x16 slice.
Arguments:
- solution: float32 [3, 64, 192, 256], P(None, 'slab', 'pencil', 'parts'), parts along dimension 3, may hold values from -6 to 6
- residual: float32 [3, 64, 192, 256], P(None, 'slab', 'pencil', 'parts'), parts along dimension 3, may hold values from -6 to 6
- direction: float32 [3, 64, 192, 256], P(None, 'slab', 'pencil', 'parts'), parts along dimension 3, may hold values from -18 to 18
- material: int32 [64, 192, 256], P('slab', 'pencil', 'parts'), parts along dimension 2, may hold values from 0 to 1, as said below
- fixed: int32 [64, 192, 256], P('slab', 'pencil', 'parts'), parts along dimension 2, may hold values from 0 to 1, as said below
Outputs:
- next_solution: float32 [3, 64, 192, 256], P(None, 'slab', 'pencil', 'parts'), parts along dimension 3
- next_residual: float32 [3, 64, 192, 256], P(None, 'slab', 'pencil', 'parts'), parts along dimension 3
- next_direction: float32 [3, 64, 192, 256], P(None, 'slab', 'pencil', 'parts'), parts along dimension 3
The draws below stay inside these ranges and needn't reach their ends.
There are 2 independent parts, one for each index of `parts`. The reference program is written for one: setup_inputs(seed, part) draws one part's arguments, and reference() takes and returns one part's arrays. A program takes and returns all parts, laid end to end along the dimension named above; each array names one. Nothing has to cross between parts.
Inputs may be any that keep to these rules, and one draw needn't show every extreme that they name: `material`: a 1 marks a solid voxel. `fixed`: 1 exactly on the first and the last node plane along the first grid dimension and on every node that no solid voxel touches (voxels on the last index of any dimension count as absent).
All inputs are finite; a program needn't handle non-finite values.
Results may differ from the reference program's by a relative error of at most 0.0003.
Values sent between devices are 32-bit elements; how exact they have to be, the bound alone decides.
A program may use at most 64 MiB of HBM per device.

```python
import jax
import jax.numpy as jnp
import numpy as np
from jax import lax

NX = 128
SWEEPS = 4
NZ = 64
NY = 192


def solid_voxels(key):
    scores = jax.random.randint(jax.random.fold_in(key, 7), (NZ, NY, NX), 0, 100)
    return (scores < 35).astype(jnp.int32)


def draw_material(key, part):
    return solid_voxels(key)


def draw_fixed(key, part):
    solid = solid_voxels(key)
    plane_index = jnp.arange(NZ, dtype=jnp.int32)[:, None, None]
    row_index = jnp.arange(NY, dtype=jnp.int32)[None, :, None]
    column_index = jnp.arange(NX, dtype=jnp.int32)[None, None, :]
    exists = (plane_index < NZ - 1) & (row_index < NY - 1) & (column_index < NX - 1)
    present = jnp.pad(solid * exists.astype(jnp.int32), ((1, 0), (1, 0), (1, 0)))
    touching = jnp.zeros((NZ, NY, NX), jnp.int32)
    for corner in range(8):
        shift_x = corner % 2
        shift_y = corner // 2 % 2
        shift_z = corner // 4
        touching = touching + present[1 - shift_z:1 - shift_z + NZ, 1 - shift_y:1 - shift_y + NY, 1 - shift_x:1 - shift_x + NX]
    plates = (plane_index == 0) | (plane_index == NZ - 1)
    return (plates | (touching == 0)).astype(jnp.int32)


def draw_direction(key, part):
    plane_pos = jnp.arange(NZ, dtype=jnp.float32)[:, None, None] / max(NZ - 1, 1)
    row_pos = jnp.arange(NY, dtype=jnp.float32)[None, :, None] / max(NY - 1, 1)
    inner_key = jax.random.fold_in(key, 11)
    base = jnp.clip(jax.random.normal(inner_key, (3, NZ, NY, NX), jnp.float32), -6.0, 6.0)
    growth = 3.0
    profile = jnp.power(growth, 0.5 * plane_pos + 0.5 * row_pos)
    return (base * profile[None]).astype(jnp.float32)


def block_levels(stream_key, extent, shards, least, top_value):
    factor_of, own = 1.0, jax.random.fold_in(stream_key, 6)
    for axis_at, parts in shards:
        steps = jnp.exp(jax.random.uniform(jax.random.fold_in(own, axis_at), (parts,), jnp.float32, least / len(shards), top_value / len(shards)))
        factor_of = factor_of * jnp.repeat(steps, extent[axis_at] // parts).reshape([-1 if axis == axis_at else 1 for axis in range(len(extent))])
    return factor_of


def noise(stream_key, dims, width, bound, cuts=(), kind=jnp.bfloat16):
    values = jax.random.normal(stream_key, dims, jnp.float32) * width
    if len(cuts) > 0:
        values = block_levels(stream_key, dims, cuts, -0.22, 0.18) * values
    return jnp.clip(values, min=-bound, max=bound).astype(kind)


def setup_inputs(seed: int = 0, part: int = 0) -> dict:
    splits = jax.random.split(jax.random.key(seed), 6)
    own_keys = jax.random.split(jax.random.fold_in(splits[5], part), 6)
    solution = noise(own_keys[0], (3, NZ, NY, NX), 1.0, 6.0, ((1, 16), (2, 16)), jnp.float32)
    residual = noise(own_keys[1], (3, NZ, NY, NX), 1.0, 6.0, ((1, 16), (2, 16)), jnp.float32)
    direction = draw_direction(jax.random.fold_in(jax.random.fold_in(splits[5], part), 71), part)
    material = draw_material(jax.random.fold_in(jax.random.fold_in(splits[5], part), 71), part)
    fixed = draw_fixed(jax.random.fold_in(jax.random.fold_in(splits[5], part), 71), part)
    return {"solution": solution, "residual": residual, "direction": direction, "material": material, "fixed": fixed}


POISSON = 0.3
VOID_MODULUS = 0.1
DAMPING = 0.6

def corner_shift(corner):
    return (corner % 2, corner // 2 % 2, corner // 4)

def element_matrix(size_x, size_y, size_z):
    lame_first = POISSON / ((1.0 + POISSON) * (1.0 - 2.0 * POISSON))
    shear_mod = 0.5 / (1.0 + POISSON)
    elastic = np.zeros((6, 6))
    elastic[:3, :3] = lame_first
    for entry in range(3):
        elastic[entry, entry] = lame_first + 2.0 * shear_mod
        elastic[entry + 3, entry + 3] = shear_mod
    lengths = (size_x, size_y, size_z)
    points = (0.5 - 0.5 / np.sqrt(3.0), 0.5 + 0.5 / np.sqrt(3.0))
    stiffness = np.zeros((24, 24))
    for point_x in points:
        for point_y in points:
            for point_z in points:
                where_at = (point_x, point_y, point_z)
                gradient = np.zeros((3, 8))
                for corner in range(8):
                    corner_bits = corner_shift(corner)
                    shapes = [where_at[axis_no] if corner_bits[axis_no] else 1.0 - where_at[axis_no] for axis_no in range(3)]
                    for axis_no in range(3):
                        factor = (1.0 if corner_bits[axis_no] else -1.0) / lengths[axis_no]
                        for second in range(3):
                            if second != axis_no:
                                factor = factor * shapes[second]
                        gradient[axis_no, corner] = factor
                strain = np.zeros((6, 24))
                for corner in range(8):
                    for axis_no in range(3):
                        strain[axis_no, axis_no * 8 + corner] = gradient[axis_no, corner]
                    strain[3, 8 + corner] = gradient[2, corner]
                    strain[3, 16 + corner] = gradient[1, corner]
                    strain[4, corner] = gradient[2, corner]
                    strain[4, 16 + corner] = gradient[0, corner]
                    strain[5, corner] = gradient[1, corner]
                    strain[5, 8 + corner] = gradient[0, corner]
                stiffness = stiffness + strain.T @ elastic @ strain * (size_x * size_y * size_z / 8.0)
    return jnp.asarray(stiffness, jnp.float32)

def corner_forces(window, moduli, matrix):
    plane_count, row_count, column_count = moduli.shape
    pieces = []
    for corner in range(8):
        shift_x, shift_y, shift_z = corner_shift(corner)
        piece = window[:, shift_z:shift_z + plane_count, shift_y:shift_y + row_count, :]
        pieces.append(jnp.roll(piece, -shift_x, axis=3))
    values = jnp.stack(pieces, axis=1).reshape(24, plane_count * row_count * column_count)
    forces = jnp.dot(matrix, values, precision=lax.Precision.HIGHEST)
    return forces.reshape(3, 8, plane_count, row_count, column_count) * moduli[None, None]

def node_sums(forces, plane_count, row_count):
    summed = None
    for corner in range(8):
        shift_x, shift_y, shift_z = corner_shift(corner)
        piece = forces[..., corner, 1 - shift_z:1 - shift_z + plane_count, 1 - shift_y:1 - shift_y + row_count, :]
        piece = jnp.roll(piece, shift_x, axis=-1)
        summed = piece if summed is None else summed + piece
    return summed

def diagonal_of(window, free_mask, matrix, plane_count, row_count):
    copies = jnp.broadcast_to(window[None], (8,) + window.shape)
    summed = node_sums(copies, plane_count, row_count)
    scale = jnp.stack([matrix[0, 0], matrix[8, 8], matrix[16, 16]])
    return free_mask[None] * scale[:, None, None, None] * summed[None] + (1.0 - free_mask[None])

def pool_moduli(moduli, first_plane, first_row, plane_total, row_total):
    plane_count, row_count, column_count = moduli.shape
    pooled = moduli.reshape(plane_count // 2, 2, row_count // 2, 2, column_count).mean(axis=(1, 3))
    plane_keep = first_plane + jnp.arange(plane_count // 2, dtype=jnp.int32) < plane_total - 1
    row_keep = first_row + jnp.arange(row_count // 2, dtype=jnp.int32) < row_total - 1
    return pooled * plane_keep.astype(pooled.dtype)[:, None, None] * row_keep.astype(pooled.dtype)[None, :, None]

def pool_free(free_mask):
    plane_count, row_count, column_count = free_mask.shape
    return free_mask.reshape(plane_count // 2, 2, row_count // 2, 2, column_count).max(axis=(1, 3))

def restrict(vector):
    comps, plane_count, row_count, column_count = vector.shape
    return vector.reshape(comps, plane_count // 2, 2, row_count // 2, 2, column_count).sum(axis=(2, 4))

def prolong(vector):
    return jnp.repeat(jnp.repeat(vector, 2, axis=1), 2, axis=2)

def apply_window(padded, vector, level):
    free_mask, window, diagonal, matrix, border = level
    forces = corner_forces(padded, window, matrix)
    return free_mask * node_sums(forces, vector.shape[1], vector.shape[2]) + (1.0 - free_mask) * vector

def operate(vector, level):
    return apply_window(level[4](level[0] * vector), vector, level)

def smooth(estimate, remain, level, final):
    update = DAMPING * remain / level[2]
    estimate = estimate + update
    if not final:
        remain = remain - operate(update, level)
    return (estimate, remain)

def solve_bottom(rhs, level):
    estimate = jnp.zeros_like(rhs)
    remain = rhs
    for sweep in range(SWEEPS):
        estimate, remain = smooth(estimate, remain, level, sweep == SWEEPS - 1)
    return estimate

def pad_both(vector):
    return jnp.pad(vector, ((0, 0), (1, 1), (1, 1), (0, 0)))

def make_level(moduli, free_mask, matrix):
    plane_count, row_count = (moduli.shape[0], moduli.shape[1])
    window = jnp.pad(moduli, ((1, 0), (1, 0), (0, 0)))
    diagonal = diagonal_of(window, free_mask, matrix, plane_count, row_count)
    return (free_mask, window, diagonal, matrix, pad_both)

def precondition(residual, fine, middle, bottom):
    estimate, remain = smooth(jnp.zeros_like(residual), residual, fine, False)
    estimate, remain = smooth(estimate, remain, fine, False)
    mid_rhs = middle[0] * restrict(fine[0] * remain)
    mid_est, mid_rem = smooth(jnp.zeros_like(mid_rhs), mid_rhs, middle, False)
    low_rhs = bottom[0] * restrict(middle[0] * mid_rem)
    low_est = solve_bottom(low_rhs, bottom)
    lift = middle[0] * prolong(low_est)
    mid_est = mid_est + lift
    mid_rem = mid_rem - operate(lift, middle)
    mid_est, mid_rem = smooth(mid_est, mid_rem, middle, True)
    lift = fine[0] * prolong(mid_est)
    estimate = estimate + lift
    remain = remain - operate(lift, fine)
    estimate, remain = smooth(estimate, remain, fine, False)
    estimate, remain = smooth(estimate, remain, fine, True)
    return estimate

def reference(solution, residual, direction, material, fixed):
    plane_count, row_count, column_count = material.shape
    plane_index = jnp.arange(plane_count, dtype=jnp.int32)[:, None, None]
    row_index = jnp.arange(row_count, dtype=jnp.int32)[None, :, None]
    column_index = jnp.arange(column_count, dtype=jnp.int32)[None, None, :]
    exists = (plane_index < plane_count - 1) & (row_index < row_count - 1) & (column_index < column_count - 1)
    moduli_fine = jnp.where(material == 1, 1.0, VOID_MODULUS).astype(jnp.float32) * exists.astype(jnp.float32)
    free_fine = (1 - fixed).astype(jnp.float32)
    moduli_mid = pool_moduli(moduli_fine, 0, 0, plane_count // 2, row_count // 2)
    free_mid = pool_free(free_fine)
    moduli_low = pool_moduli(moduli_mid, 0, 0, plane_count // 4, row_count // 4)
    free_low = pool_free(free_mid)
    fine = make_level(moduli_fine, free_fine, element_matrix(1.0, 1.0, 1.0))
    middle = make_level(moduli_mid, free_mid, element_matrix(1.0, 2.0, 2.0))
    bottom = make_level(moduli_low, free_low, element_matrix(1.0, 4.0, 4.0))
    precond = precondition(residual, fine, middle, bottom)
    image_old = operate(direction, fine)
    beta_coef = -jnp.sum(precond * image_old) / jnp.sum(direction * image_old)
    next_direction = precond + beta_coef * direction
    image = operate(next_direction, fine)
    step_size = jnp.sum(residual * next_direction) / jnp.sum(next_direction * image)
    next_solution = solution + step_size * next_direction
    next_residual = residual - step_size * image
    return (next_solution, next_residual, next_direction)
```

```python
import functools

import jax
import jax.numpy as jnp
import numpy as np
from jax import lax
from jax.experimental import pallas as pl
from jax.experimental.pallas import tpu as pltpu
from jax.sharding import PartitionSpec as P

SWEEPS = 4
POISSON = 0.3
VOID_MODULUS = 0.1
DAMPING = 0.6
LAME = POISSON / ((1.0 + POISSON) * (1.0 - 2.0 * POISSON))
SHEAR = 0.5 / (1.0 + POISSON)
LANES = 128
COMPS = range(3)
MESH = pl.DeviceIdType.MESH

PLANES, ROWS = 4, 12
FINE_O, FINE_S = (6, 8), (14, 32)
MID_O, MID_S = (3, 4), (8, 24)
LOW_O, LOW_S = (3, 4), (7, 24)


def diagonal_entries(lengths):
    volume = lengths[0] * lengths[1] * lengths[2]
    entries = []
    for c in COMPS:
        total = 0.0
        for axis in COMPS:
            weight = (LAME + 2.0 * SHEAR) if axis == c else SHEAR
            total += weight / lengths[axis] ** 2 / 9.0
        entries.append(total * volume)
    return entries


def scaled(value, factor):
    return value if factor == 1.0 else value * factor


def element_forces(modes, modulus, lengths):
    volume = lengths[0] * lengths[1] * lengths[2]
    inv = [1.0 / length for length in lengths]

    def key(*axes):
        return tuple(1 if axis in axes else 0 for axis in COMPS)

    out = [dict() for _ in COMPS]
    e_norm = modulus * (volume / 16.0)
    e_pair = modulus * (volume / 48.0)
    e_last = modulus * (volume / 144.0)
    stretch = [scaled(modes[c][key(c)], inv[c]) for c in COMPS]
    trace = (stretch[0] + stretch[1] + stretch[2]) * LAME
    for c in COMPS:
        out[c][key(c)] = scaled(trace + stretch[c] * (2.0 * SHEAR), inv[c]) * e_norm
    for b, t in ((0, 1), (0, 2), (1, 2)):
        glide = (scaled(modes[b][key(t)], inv[t]) + scaled(modes[t][key(b)], inv[b])) * SHEAR
        glide = glide * e_norm
        out[b][key(t)] = scaled(glide, inv[t])
        out[t][key(b)] = scaled(glide, inv[b])
    for b in COMPS:
        c, t = [axis for axis in COMPS if axis != b]
        one, two = modes[c][key(c, b)], modes[t][key(t, b)]
        both = (scaled(one, inv[c]) + scaled(two, inv[t])) * LAME
        for comp, mine in ((c, one), (t, two)):
            own = 2.0 * SHEAR * inv[comp] ** 2 + SHEAR * inv[b] ** 2
            out[comp][key(comp, b)] = (scaled(both, inv[comp]) + mine * own) * e_pair
    for c in COMPS:
        b, t = [axis for axis in COMPS if axis != c]
        mine = modes[c][key(b, t)]
        first = scaled(mine, inv[b]) + scaled(modes[b][key(c, t)], inv[c])
        second = scaled(mine, inv[t]) + scaled(modes[t][key(c, b)], inv[c])
        both = scaled(first, inv[b]) + scaled(second, inv[t])
        out[c][key(b, t)] = both * SHEAR * e_pair
    for c in COMPS:
        total = 0.0
        for axis in COMPS:
            total += ((LAME + 2.0 * SHEAR) if axis == c else SHEAR) * inv[axis] ** 2
        out[c][key(0, 1, 2)] = modes[c][key(0, 1, 2)] * total * e_last
    return out


class Plane:
    def __init__(self, count, shift, factor=1):
        self.count, self.shift, self.factor = count, shift, factor

    def __add__(self, other):
        return Plane(self.count, self.shift + other, self.factor)

    def doubled(self, extra):
        return Plane(self.count, 2 * self.shift + extra, 2 * self.factor)

    def index(self, origin=0):
        return self.count * self.factor + (self.shift + origin)


def place(plane, origin):
    return plane.index(origin) if isinstance(plane, Plane) else plane + origin


def twice(plane, extra):
    return plane.doubled(extra) if isinstance(plane, Plane) else 2 * plane + extra


def over(planes, body):
    lax.fori_loop(0, planes[1] + 1 - planes[0], lambda i, _: (body(Plane(i, planes[0])), 0)[1], 0)


class Level:
    def __init__(self, origin, lengths, split, sums, modulus, inverse, free):
        self.oz, self.oy = origin
        self.lengths = lengths
        self.split, self.sums = split, sums
        self.modulus, self.inverse, self.free = modulus, inverse, free
        entries = diagonal_entries(lengths)
        self.entries = [entries[0]] if lengths[0] == lengths[1] else [entries[0], entries[1]]

    def at(self, plane, row):
        return place(plane, self.oz), pl.ds(row + self.oy, 8)

    def which(self, c):
        return min(c, len(self.entries) - 1)

    def inverse_of(self, c, plane, row):
        p, r = self.at(plane, row)
        return self.inverse[self.which(c), p, r, :]

    def put_split(self, c, plane, row, value):
        p, r = self.at(plane, row)
        after = pltpu.roll(value, LANES - 1, 1)
        self.split[2 * c, p, r, :] = value + after
        self.split[2 * c + 1, p, r, :] = after - value

    def set_diagonal(self, planes, rows):
        def body(plane):
            for row in rows:
                p, r = self.at(plane, row)
                free = self.free[p, r, :]
                total = self.node_total(plane, row)
                for n, entry in enumerate(self.entries):
                    self.inverse[n, p, r, :] = DAMPING / (free * total * entry + (1.0 - free))

        over(planes, body)

    def node_total(self, plane, row):
        total = None
        for dz in (-1, 0):
            for dy in (-1, 0):
                p, r = self.at(plane + dz, row + dy)
                piece = self.modulus[p, r, :]
                total = piece if total is None else total + piece
        return total + pltpu.roll(total, 1, 1)

    def voxels(self, planes, rows):
        def pieces(plane, row):
            found = []
            for cm in range(6):
                p, r = self.at(plane, row)
                near = self.split[cm, p, r, :]
                p, r = self.at(plane, row + 1)
                far = self.split[cm, p, r, :]
                found += [near + far, far - near]
            return found

        for row in rows:

            def body(count, carry, row=row):
                plane = Plane(count, planes[0])
                lower, held = carry
                upper = pieces(plane + 1, row)
                p, r = self.at(plane, row)
                modes = []
                for c in COMPS:
                    mine = {}
                    for m in range(2):
                        for iy in range(2):
                            k = (2 * c + m) * 2 + iy
                            if m + iy > 0:
                                mine[(m, iy, 0)] = lower[k] + upper[k]
                            mine[(m, iy, 1)] = upper[k] - lower[k]
                    modes.append(mine)
                forces = element_forces(modes, self.modulus[p, r, :], self.lengths)
                keep = []
                for c in COMPS:
                    for m in range(2):
                        node = []
                        for iy in range(2):
                            k = (2 * c + m) * 2 + iy
                            diff = forces[c][(m, iy, 1)]
                            if m + iy > 0:
                                same = forces[c][(m, iy, 0)]
                                node.append(held[k] + (same - diff))
                                keep.append(same + diff)
                            else:
                                node.append(held[k] - diff)
                                keep.append(diff)
                        self.sums[(2 * c + m) * 2, p, r, :] = node[0] - node[1]
                        self.sums[(2 * c + m) * 2 + 1, p, r, :] = node[0] + node[1]
                return upper, keep

            zero = [jnp.zeros((8, LANES), jnp.float32)] * 12
            lax.fori_loop(0, planes[1] + 1 - planes[0], body, (pieces(planes[0], row), zero))

    def applied(self, c, plane, row):
        parts = []
        for m in range(2):
            k = (2 * c + m) * 2
            p, r = self.at(plane, row)
            here = self.sums[k, p, r, :]
            p, r = self.at(plane, row - 1)
            parts.append(here + self.sums[k + 1, p, r, :])
        return (parts[0] - parts[1]) + pltpu.roll(parts[0] + parts[1], 1, 1)


def messages():
    found = []
    for oz in (0, -1, 1):
        for oy in (0, -1, 1):
            if (oz, oy) != (0, 0):
                found.append(("wide", oz, oy, ("wide", oy), {0: 192, -1: 72, 1: 64}[oy]))
    for oy in (0, -1, 1):
        found.append(("far", -2, oy, ("far", oy), {0: 24, -1: 16, 1: 8}[oy]))
    for oz in (0, -1, 1):
        for oy in (0, -1, 1):
            if (oz, oy) != (0, 0):
                rows = (8 if oy else 40) if oz else 16
                found.append(("dir", oz, oy, ("dir", oz, oy), rows))
    for oz in (0, -1, 1, -2, 2, -3, 3):
        for oy in (0, -1, 1):
            if (oz, oy) != (0, 0):
                found.append(("fixlow", oz, oy, ("fixlow",), 16))
    for oz in (0, -1, 1, -2, 2, -3, 3):
        for oy in (0, -1, 1):
            if (oz, oy) != (0, 0):
                found.append(("low", oz, oy, ("low",), 16))
    for oz in (0, -1, 1):
        for oy in (0, -1, 1):
            if (oz, oy) != (0, 0):
                found.append(("mid", oz, oy, ("mid", oy), 24 if oy else 72))
    for oz in (0, -1, 1, -2, 2):
        for oy in (0, -1, 1):
            if (oz, oy) != (0, 0):
                each = 16 if oy else 24
                part = {-2: 1, 2: 0}.get(oz)
                found.append(("lift", oz, oy, ("lift", oy, part), each if part is not None else 2 * each))
    return found


def layout():
    sends, receives = {}, {}
    at_send = at_receive = 0
    for oy in (0, -1, 1):
        each = 16 if oy else 24
        sends[("lift", oy, None)] = at_send
        sends[("lift", oy, 0)] = at_send
        sends[("lift", oy, 1)] = at_send + each
        at_send += 2 * each
    for name, oz, oy, key, rows in messages():
        if key not in sends:
            sends[key] = at_send
            at_send += rows
        receives[(name, oz, oy)] = at_receive
        at_receive += rows
    return sends, at_send, receives, at_receive


def kernel(
    slab_count,
    pencil_count,
    solution_ref,
    residual_ref,
    direction_ref,
    material_ref,
    next_solution_ref,
    next_residual_ref,
    next_direction_ref,
    sol_in,
    res_in,
    dir_in,
    mat,
    res,
    dirn,
    s0,
    e0,
    old,
    e_fine,
    f_fine,
    i_fine,
    x_fine,
    b_fine,
    s1,
    u1,
    c1,
    e_mid,
    f_mid,
    i_mid,
    x_mid,
    b_mid,
    s2,
    e_low,
    f_low,
    m_low,
    i_low,
    x_low,
    b_low,
    outbox,
    inbox,
    part_out,
    slab_in,
    line_out,
    pencil_in,
    local_sem,
    send_sem,
    recv_sem,
    sum_send,
    sum_recv,
):
    slab_at, pencil_at = lax.axis_index("slab"), lax.axis_index("pencil")
    sends, _, receives, _ = layout()
    all_messages = messages()
    fine = Level(FINE_O, (1.0, 1.0, 1.0), x_fine, b_fine, e_fine, i_fine, f_fine)
    mid = Level(MID_O, (1.0, 2.0, 2.0), x_mid, b_mid, e_mid, i_mid, f_mid)
    low = Level(LOW_O, (1.0, 4.0, 4.0), x_low, b_low, e_low, i_low, f_low)

    loads = [
        pltpu.make_async_copy(source, target, local_sem.at[n])
        for n, (source, target) in enumerate(
            ((material_ref, mat), (residual_ref, res_in), (direction_ref, dir_in), (solution_ref, sol_in))
        )
    ]
    for load in loads:
        load.start()

    def there(oz, oy):
        z, y = slab_at + oz, pencil_at + oy
        return (z >= 0) & (z < slab_count) & (y >= 0) & (y < pencil_count)

    inbox[...] = jnp.zeros_like(inbox)

    barrier = pltpu.get_barrier_semaphore()
    greeted = jnp.int32(slab_count + pencil_count - 2)

    def greet_slab(k, _):
        pl.semaphore_signal(
            barrier, inc=1, device_id={"slab": lax.rem(slab_at + k, slab_count)}, device_id_type=MESH
        )
        return 0

    def greet_pencil(k, _):
        pl.semaphore_signal(
            barrier, inc=1, device_id={"pencil": lax.rem(pencil_at + k, pencil_count)}, device_id_type=MESH
        )
        return 0

    lax.fori_loop(1, slab_count, greet_slab, 0)
    lax.fori_loop(1, pencil_count, greet_pencil, 0)
    for oz in (-3, -2, -1, 1, 2, 3):
        for oy in (-1, 1):
            near = there(oz, oy)
            greeted = greeted + jnp.where(near, 1, 0)

            @pl.when(near)
            def _(oz=oz, oy=oy):
                pl.semaphore_signal(
                    barrier,
                    inc=1,
                    device_id={"slab": slab_at + oz, "pencil": pencil_at + oy},
                    device_id_type=MESH,
                )

    for ref in (s0, e_fine, x_fine, b_fine, s1, u1, c1, x_mid, b_mid, s2, e_low, f_low, m_low, i_low, x_low, b_low):
        ref[...] = jnp.zeros_like(ref)
    e_mid[...] = jnp.zeros_like(e_mid)
    f_mid[...] = jnp.zeros_like(f_mid)
    i_mid[...] = jnp.zeros_like(i_mid)
    f_fine[...] = jnp.zeros_like(f_fine)
    i_fine[...] = jnp.zeros_like(i_fine)

    def copy_of(number, oz, oy, key, rows):
        name = all_messages[number][0]
        return pltpu.make_async_remote_copy(
            src_ref=outbox.at[pl.ds(sends[key], rows)],
            dst_ref=inbox.at[pl.ds(receives[(name, oz, oy)], rows)],
            send_sem=send_sem.at[number],
            recv_sem=recv_sem.at[number],
            device_id={"slab": slab_at - oz, "pencil": pencil_at - oy},
            device_id_type=MESH,
        )

    def start(*names):
        for number, (name, oz, oy, key, rows) in enumerate(all_messages):
            if name in names:

                @pl.when(there(-oz, -oy))
                def _(number=number, oz=oz, oy=oy, key=key, rows=rows):
                    copy_of(number, oz, oy, key, rows).start()

    def arrive(*names):
        for number, (name, oz, oy, key, rows) in enumerate(all_messages):
            if name in names:

                @pl.when(there(oz, oy))
                def _(number=number, oz=oz, oy=oy, key=key, rows=rows):
                    copy_of(number, oz, oy, key, rows).wait_recv()

    def take(name, oz, oy):
        return receives[(name, oz, oy)]

    def strided(p, first, count):
        return pl.ds(p + PLANES * first, count, stride=PLANES)

    def planes_first(source, target):
        for c in COMPS:
            for p in range(PLANES):
                for first, count in ((0, 8), (8, 4)):
                    target[c, p, pl.ds(first, count), :] = source[c, strided(p, first, count), :]

    loads[0].wait()
    loads[1].wait()
    planes_first(res_in, res)

    taken_rows = {0: (0, 12), -1: (8, 4), 1: (0, 4)}
    voxel_rows = {0: (0, 12), -1: (6, 6), 1: (0, 4)}
    for oy in (0, -1, 1):
        at = sends[("wide", oy)]
        first, count = taken_rows[oy]
        for c in COMPS:
            for p in range(PLANES):
                outbox[pl.ds(at, count), :] = res[c, p, pl.ds(first, count), :]
                at += count
        first, count = voxel_rows[oy]
        for p in range(PLANES):
            outbox[pl.ds(at, count), :] = (mat[strided(p, first, count), :] == 1).astype(jnp.float32)
            at += count
        at = sends[("far", oy)]
        for p in (2, 3):
            outbox[pl.ds(at, count), :] = (mat[strided(p, first, count), :] == 1).astype(jnp.float32)
            at += count

    loads[2].wait()
    planes_first(dir_in, dirn)
    for name, oz, oy, key, rows in all_messages:
        if name == "dir":
            at = sends[key]
            planes = {0: range(PLANES), -1: (3,), 1: (0,)}[oz]
            first, count = {0: (0, 12), -1: (11, 1), 1: (0, 1)}[oy]
            for c in COMPS:
                for p in planes:
                    outbox[pl.ds(at, count), :] = dirn[c, p, pl.ds(first, count), :]
                    at += count

    pl.semaphore_wait(barrier, greeted)
    start("wide", "far")
    start("dir")

    for c in COMPS:
        for p in range(PLANES):
            s0[c, p + FINE_O[0], pl.ds(FINE_O[1], ROWS), :] = res[c, p, pl.ds(0, ROWS), :]
    for p in range(PLANES):
        for first, count in ((0, 8), (8, 4)):
            e_fine[p + FINE_O[0], pl.ds(first + FINE_O[1], count), :] = (mat[strided(p, first, count), :] == 1).astype(
                jnp.float32
            )

    arrive("wide", "far")
    for oz in (0, -1, 1):
        for oy in (0, -1, 1):
            if (oz, oy) == (0, 0):
                continue
            at = receives[("wide", oz, oy)]
            first, count = {0: (0, 12), -1: (-4, 4), 1: (12, 4)}[oy]
            for c in COMPS:
                for p in range(PLANES):
                    s0[c, p + oz * PLANES + FINE_O[0], pl.ds(first + FINE_O[1], count), :] = inbox[pl.ds(at, count), :]
                    at += count
            first, count = {0: (0, 12), -1: (-6, 6), 1: (12, 4)}[oy]
            for p in range(PLANES):
                e_fine[p + oz * PLANES + FINE_O[0], pl.ds(first + FINE_O[1], count), :] = inbox[pl.ds(at, count), :]
                at += count
    for oy in (0, -1, 1):
        at = receives[("far", -2, oy)]
        first, count = {0: (0, 12), -1: (-6, 6), 1: (12, 4)}[oy]
        for p in (-6, -5):
            e_fine[p + FINE_O[0], pl.ds(first + FINE_O[1], count), :] = inbox[pl.ds(at, count), :]
            at += count

    total_planes, total_rows = slab_count * PLANES, pencil_count * ROWS
    row_iota = lax.broadcasted_iota(jnp.int32, (8, LANES), 0)
    lane_iota = lax.broadcasted_iota(jnp.int32, (8, LANES), 1)

    def moduli_body(p):
        plane = slab_at * PLANES + p.index()
        plane_ok = (plane >= 0) & (plane < total_planes - 1)
        for row in (-8, 0, 8):
            ip, ir = fine.at(p, row)
            rows = row_iota + (pencil_at * ROWS + row)
            keep = (rows >= 0) & (rows < total_rows - 1) & (lane_iota < LANES - 1) & plane_ok
            value = jnp.where(e_fine[ip, ir, :] > 0.5, 1.0, VOID_MODULUS)
            e_fine[ip, ir, :] = jnp.where(keep, value, 0.0)

    over((-6, 7), moduli_body)

    def fine_body(p):
        plane = slab_at * PLANES + p.index()
        inside = (plane > 0) & (plane < total_planes - 1)
        for row in (-5, 3, 8):
            ip, ir = fine.at(p, row)
            total = fine.node_total(p, row)
            free = jnp.where((total > 0.9) & inside, 1.0, 0.0)
            f_fine[ip, ir, :] = free
            i_fine[0, ip, ir, :] = DAMPING / (free * total * fine.entries[0] + (1.0 - free))

    over((-5, 7), fine_body)

    def first_update(p):
        for row in (-4, 4, 8):
            ip, ir = fine.at(p, row)
            weight = i_fine[0, ip, ir, :] * f_fine[ip, ir, :]
            for c in COMPS:
                fine.put_split(c, p, row, s0[c, ip, ir, :] * weight)

    over((-4, 7), first_update)

    def halves(ref, c, p, row):
        found = []
        for dp in range(2):
            for dr in range(2):
                r = pl.ds(2 * row + dr + FINE_O[1], 8, stride=2)
                ip = place(twice(p, dp), FINE_O[0])
                found.append(ref[ip, r, :] if c is None else ref[c, ip, r, :])
        return found

    def mid_moduli(p):
        plane_ok = slab_at * (PLANES // 2) + p.index() < total_planes // 2 - 1
        for row in (-3, 0):
            ip, ir = mid.at(p, row)
            a, b, c, d = halves(e_fine, None, p, row)
            rows = row_iota + (pencil_at * (ROWS // 2) + row)
            keep = (rows < total_rows // 2 - 1) & plane_ok
            e_mid[ip, ir, :] = jnp.where(keep, (a + b + c + d) * 0.25, 0.0)

    over((-3, 3), mid_moduli)

    def mid_free(p):
        for row in (-2, 0):
            ip, ir = mid.at(p, row)
            a, b, c, d = halves(f_fine, None, p, row)
            f_mid[ip, ir, :] = jnp.maximum(jnp.maximum(a, b), jnp.maximum(c, d))

    over((-2, 3), mid_free)
    mid.set_diagonal((-2, 3), (-2, 0))

    def mid_pair(ref, c, p, row):
        found = []
        for dp in range(2):
            for dr in range(2):
                r = pl.ds(2 * row + dr + MID_O[1], 8, stride=2)
                ip = place(twice(p, dp), MID_O[0])
                found.append(ref[ip, r, :] if c is None else ref[c, ip, r, :])
        return found

    for p in (-1, 0):
        ip, ir = low.at(p, -1)
        a, b, c, d = mid_pair(e_mid, None, p, -1)
        rows = row_iota + (pencil_at * (ROWS // 4) - 1)
        keep = (rows < total_rows // 4 - 1) & (slab_at * (PLANES // 4) + p < total_planes // 4 - 1) & (row_iota < 4)
        e_low[ip, ir, :] = jnp.where(keep, (a + b + c + d) * 0.25, 0.0)
    a, b, c, d = mid_pair(f_mid, None, 0, 0)
    ip, ir = low.at(0, 0)
    f_low[ip, ir, :] = jnp.where(row_iota < 3, jnp.maximum(jnp.maximum(a, b), jnp.maximum(c, d)), 0.0)
    m_low[ip, ir, :] = jnp.where(row_iota < 3, low.node_total(0, 0), 0.0)
    at = sends[("fixlow",)]
    own_rows = pl.ds(LOW_O[1], 3)
    for n, ref in enumerate((e_low, f_low, m_low)):
        outbox[pl.ds(at + 3 * n, 3), :] = ref[LOW_O[0], own_rows, :]
    start("fixlow")

    fine.voxels((-4, 6), (-4, 4, 12))

    def fine_step(rows, starting):
        def body(p):
            for row in rows:
                ip, ir = fine.at(p, row)
                free = f_fine[ip, ir, :]
                weight = i_fine[0, ip, ir, :]
                for c in COMPS:
                    remain = s0[c, ip, ir, :]
                    update = weight * remain
                    remain = remain - free * fine.applied(c, p, row) - (1.0 - free) * update
                    s0[c, ip, ir, :] = remain
                    if starting:
                        fine.put_split(c, p, row, free * (weight * remain))

        return body

    def estimate_add(starting):
        def body(p):
            for row in (0, 8):
                ip, ir = fine.at(p, row)
                weight = i_fine[0, ip, ir, :]
                for c in COMPS:
                    update = weight * s0[c, ip, ir, :]
                    e0[c, p.index(), pl.ds(row, 8), :] = update if starting else e0[c, p.index(), pl.ds(row, 8), :] + update

        over((0, 3), body)

    estimate_add(True)
    over((-3, 6), fine_step((-3, 5, 13), True))
    estimate_add(False)
    fine.voxels((-3, 5), (-3, 5, 13))
    over((-2, 5), fine_step((-2, 6), False))

    def mid_first(p):
        ip, ir = mid.at(p, -1)
        free = f_mid[ip, ir, :]
        masks = halves(f_fine, None, p, -1)
        for c in COMPS:
            parts = halves(s0, c, p, -1)
            rhs = free * (
                (parts[0] * masks[0] + parts[1] * masks[1]) + (parts[2] * masks[2] + parts[3] * masks[3])
            )
            s1[c, ip, ir, :] = rhs
            update = mid.inverse_of(c, p, -1) * rhs
            u1[c, ip, ir, :] = update
            mid.put_split(c, p, -1, free * update)

    over((-1, 2), mid_first)
    mid.voxels((-1, 1), (-1,))

    def mid_remain(p):
        ip, ir = mid.at(p, 0)
        free = f_mid[ip, ir, :]
        for c in COMPS:
            s1[c, ip, ir, :] = s1[c, ip, ir, :] - free * mid.applied(c, p, 0) - (1.0 - free) * u1[c, ip, ir, :]

    over((0, 1), mid_remain)

    masks = mid_pair(f_mid, None, 0, 0)
    ip, ir = low.at(0, 0)
    free = f_low[ip, ir, :]
    at = sends[("low",)]
    for c in COMPS:
        parts = mid_pair(s1, c, 0, 0)
        rhs = free * ((parts[0] * masks[0] + parts[1] * masks[1]) + (parts[2] * masks[2] + parts[3] * masks[3]))
        rhs = jnp.where(row_iota < 3, rhs, 0.0)
        s2[c, ip, ir, :] = rhs
        outbox[pl.ds(at + 3 * c, 3), :] = rhs[0:3, :]
    start("low")
    mid_rows = {0: (0, 6), -1: (4, 2), 1: (0, 2)}
    for oy in (0, -1, 1):
        at = sends[("mid", oy)]
        first, count = mid_rows[oy]
        for ref in (s1, u1):
            for c in COMPS:
                for p in range(2):
                    outbox[pl.ds(at, count), :] = ref[c, p + MID_O[0], pl.ds(first + MID_O[1], count), :]
                    at += count
    start("mid")

    arrive("dir")
    arrive("fixlow")
    def direction_rows(plane, first, count, c, value):
        ip, ir = plane + FINE_O[0], pl.ds(first + FINE_O[1], count)
        value = value * f_fine[ip, ir, :]
        after = pltpu.roll(value, LANES - 1, 1)
        x_fine[2 * c, ip, ir, :] = value + after
        x_fine[2 * c + 1, ip, ir, :] = after - value

    for oz in (0, -1, 1):
        for oy in (0, -1, 1):
            planes = {0: range(PLANES), -1: (-1,), 1: (PLANES,)}[oz]
            first, count = {0: (0, 12), -1: (-1, 1), 1: (12, 1)}[oy]
            at = None if (oz, oy) == (0, 0) else receives[("dir", oz, oy)]
            for c in COMPS:
                for p in planes:
                    if at is None:
                        direction_rows(p, first, count, c, dirn[c, p, pl.ds(0, ROWS), :])
                    else:
                        direction_rows(p, first, count, c, inbox[pl.ds(at, count), :])
                        at += count
    fine.voxels((-1, 3), (-1, 7))

    def old_image(p):
        for row in (0, 4):
            ip, ir = fine.at(p, row)
            free = f_fine[ip, ir, :]
            for c in COMPS:
                value = dirn[c, p.index(), pl.ds(row, 8), :]
                old[c, p.index(), pl.ds(row, 8), :] = free * fine.applied(c, p, row) + (1.0 - free) * value

    over((0, 3), old_image)

    def low_window(name, refs):
        for oz in (0, -1, 1, -2, 2, -3, 3):
            for oy in (0, -1, 1):
                if (oz, oy) == (0, 0):
                    continue
                at = receives[(name, oz, oy)]
                for n, ref in enumerate(refs):
                    ref[oz + LOW_O[0], pl.ds(3 * oy + LOW_O[1], 3), :] = inbox[pl.ds(at + 3 * n, 3), :]

    low_window("fixlow", (e_low, f_low, m_low))

    def low_inverse(p):
        for row in (-4, 4):
            ip, ir = low.at(p, row)
            free = f_low[ip, ir, :]
            total = m_low[ip, ir, :]
            for n, entry in enumerate(low.entries):
                i_low[n, ip, ir, :] = DAMPING / (free * total * entry + (1.0 - free))

    over((-3, 3), low_inverse)

    arrive("low")
    low_window("low", [s2.at[c] for c in COMPS])

    def low_split(planes, rows):
        def body(p):
            for row in rows:
                ip, ir = low.at(p, row)
                free = f_low[ip, ir, :]
                for c in COMPS:
                    low.put_split(c, p, row, free * (low.inverse_of(c, p, row) * s2[c, ip, ir, :]))

        over(planes, body)

    ip, ir = low.at(0, 0)
    bottom = [low.inverse_of(c, 0, 0) * s2[c, ip, ir, :] for c in COMPS]
    low_split((-3, 3), (-3, 5))
    for depth in (2, 1, 0):
        low.voxels((-1 - depth, depth), (-1 - depth,))

        def low_step(p, depth=depth):
            row = -depth
            ip, ir = low.at(p, row)
            free = f_low[ip, ir, :]
            for c in COMPS:
                remain = s2[c, ip, ir, :]
                update = low.inverse_of(c, p, row) * remain
                remain = remain - free * low.applied(c, p, row) - (1.0 - free) * update
                s2[c, ip, ir, :] = remain
                if depth:
                    low.put_split(c, p, row, free * (low.inverse_of(c, p, row) * remain))

        over((-depth, depth), low_step)
        ip, ir = low.at(0, 0)
        for c in COMPS:
            bottom[c] = bottom[c] + low.inverse_of(c, 0, 0) * s2[c, ip, ir, :]

    for c in COMPS:
        for p in range(2):
            for dr in range(2):
                c1[c, p + MID_O[0], pl.ds(MID_O[1] + dr, 3, stride=2), :] = bottom[c][0:3, :]
    for c in COMPS:
        for p in range(2):
            ip, ir = p + MID_O[0], pl.ds(MID_O[1], 6)
            c1[c, ip, ir, :] = c1[c, ip, ir, :] * f_mid[ip, ir, :]
    for oy in (0, -1, 1):
        first, count = {0: (0, 6), -1: (3, 3), 1: (0, 3)}[oy]
        for p in range(2):
            at = sends[("lift", oy, p)]
            for c in COMPS:
                outbox[pl.ds(at, count), :] = c1[c, p + MID_O[0], pl.ds(first + MID_O[1], count), :]
                at += count
    start("lift")
    arrive("mid")
    for oz in (0, -1, 1):
        for oy in (0, -1, 1):
            if (oz, oy) == (0, 0):
                continue
            at = receives[("mid", oz, oy)]
            first, count = {0: (0, 6), -1: (-2, 2), 1: (6, 2)}[oy]
            for ref in (s1, u1):
                for c in COMPS:
                    for p in range(2):
                        ref[c, p + 2 * oz + MID_O[0], pl.ds(first + MID_O[1], count), :] = inbox[pl.ds(at, count), :]
                        at += count
    arrive("lift")
    for oz in (0, -1, 1, -2, 2):
        for oy in (0, -1, 1):
            if (oz, oy) == (0, 0):
                continue
            base = receives[("lift", oz, oy)]
            first, count = {0: (0, 6), -1: (-3, 3), 1: (6, 3)}[oy]
            planes = {-2: (-3,), 2: (4,)}.get(oz, (2 * oz, 2 * oz + 1))
            for n, p in enumerate(planes):
                at = base + n * (16 if oy else 24)
                for c in COMPS:
                    c1[c, p + MID_O[0], pl.ds(first + MID_O[1], count), :] = inbox[pl.ds(at, count), :]
                    at += count

    def lift_split(p):
        for row in (-3, 5):
            ip, ir = mid.at(p, row)
            for c in COMPS:
                mid.put_split(c, p, row, c1[c, ip, ir, :])

    over((-3, 4), lift_split)
    mid.voxels((-3, 3), (-3, 5))

    def mid_second(p):
        for row in (-2, 6):
            ip, ir = mid.at(p, row)
            free = f_mid[ip, ir, :]
            for c in COMPS:
                remain = s1[c, ip, ir, :] - free * mid.applied(c, p, row)
                u1[c, ip, ir, :] = u1[c, ip, ir, :] + c1[c, ip, ir, :] + mid.inverse_of(c, p, row) * remain

    over((-2, 3), mid_second)

    def lift_fine(p):
        for row in (-2, 0):
            ip, ir = mid.at(p, row)
            for c in COMPS:
                value = u1[c, ip, ir, :]
                for dp in range(2):
                    for dr in range(2):
                        out = pl.ds(2 * row + dr + FINE_O[1], 8, stride=2)
                        x_fine[2 * c, place(twice(p, dp), FINE_O[0]), out, :] = value

    over((-2, 3), lift_fine)

    def lift_parts(p):
        for row in (-4, 4, 12):
            ip, ir = fine.at(p, row)
            free = f_fine[ip, ir, :]
            for c in COMPS:
                fine.put_split(c, p, row, free * x_fine[2 * c, ip, ir, :])

    def lift_own(p):
        for row in (0, 4):
            ip, ir = fine.at(p, row)
            free = f_fine[ip, ir, :]
            for c in COMPS:
                part = free * x_fine[2 * c, ip, ir, :]
                if row:
                    part = jnp.where(row_iota >= 4, part, 0.0)
                e0[c, p.index(), pl.ds(row, 8), :] = e0[c, p.index(), pl.ds(row, 8), :] + part

    over((0, 3), lift_own)
    over((-4, 7), lift_parts)
    fine.voxels((-3, 5), (-3, 5, 13))

    def lift_step(p):
        for row in (-2, 6):
            ip, ir = fine.at(p, row)
            free = f_fine[ip, ir, :]
            weight = i_fine[0, ip, ir, :]
            for c in COMPS:
                remain = s0[c, ip, ir, :] - free * fine.applied(c, p, row)
                s0[c, ip, ir, :] = remain
                fine.put_split(c, p, row, free * (weight * remain))

    over((-2, 5), lift_step)
    estimate_add(False)
    fine.voxels((-2, 4), (-2, 6))
    over((-1, 4), fine_step((-1, 7), True))
    estimate_add(False)
    fine.voxels((-1, 3), (-1, 7))
    over((0, 3), fine_step((0, 8), False))

    def dots(p, totals):
        totals = list(totals)
        for row in (0, 4):
            ip, ir = p + FINE_O[0], pl.ds(row + FINE_O[1], 8)
            keep = None if row == 0 else row_iota >= 4
            for c in COMPS:
                rows = pl.ds(row, 8)
                z, d, o, r = e0[c, p, rows, :], dirn[c, p, rows, :], old[c, p, rows, :], res[c, p, rows, :]
                new = r - s0[c, ip, ir, :]
                for n, term in enumerate((z * o, d * o, z * new, r * z, r * d)):
                    totals[n] = totals[n] + (term if keep is None else jnp.where(keep, term, 0.0))
        return tuple(totals)

    totals = lax.fori_loop(0, PLANES, dots, (jnp.zeros((8, LANES), jnp.float32),) * 5)
    for n, total in enumerate(totals):
        part_out[pl.ds(n, 1), :] = jnp.sum(total, axis=0, keepdims=True)

    def share(axis, at, count, source, target, which):
        def copy(k):
            return pltpu.make_async_remote_copy(
                src_ref=source,
                dst_ref=target.at[k],
                send_sem=sum_send.at[which, k],
                recv_sem=sum_recv.at[which, k],
                device_id={axis: lax.rem(at + k, count)},
                device_id_type=MESH,
            )

        lax.fori_loop(1, count, lambda k, _: (copy(k).start(), 0)[1], 0)
        lax.fori_loop(1, count, lambda k, _: (copy(k).wait_recv(), 0)[1], 0)
        total = source[...]
        total = lax.fori_loop(1, count, lambda k, t: t + target[k], total)
        return total, copy

    line, slab_copy = share("slab", slab_at, slab_count, part_out, slab_in, 0)
    line_out[...] = line
    whole, pencil_copy = share("pencil", pencil_at, pencil_count, line_out, pencil_in, 1)
    summed = jnp.sum(whole, axis=1, keepdims=True)
    t = [summed[n : n + 1, :] for n in range(5)]
    beta = -t[0] / t[1]
    along = t[3] + beta * t[4]
    curvature = t[2] + 2.0 * beta * t[0] + beta * beta * t[1]
    step = along / curvature

    loads[3].wait()

    for c in COMPS:
        for p in range(PLANES):
            for first, count in ((0, 8), (8, 4)):
                rows, there_rows = pl.ds(first, count), strided(p, first, count)
                z, d, o, r = e0[c, p, rows, :], dirn[c, p, rows, :], old[c, p, rows, :], res[c, p, rows, :]
                new = r - s0[c, p + FINE_O[0], pl.ds(first + FINE_O[1], count), :]
                nd = z + beta * d
                image = new + beta * o
                dir_in[c, there_rows, :] = nd
                sol_in[c, there_rows, :] = sol_in[c, there_rows, :] + step * nd
                res_in[c, there_rows, :] = r - step * image
    stores = [
        pltpu.make_async_copy(source, target, local_sem.at[n])
        for n, (source, target) in enumerate(
            ((dir_in, next_direction_ref), (sol_in, next_solution_ref), (res_in, next_residual_ref))
        )
    ]
    for store in stores:
        store.start()

    for number, (name, oz, oy, key, rows) in enumerate(all_messages):

        @pl.when(there(-oz, -oy))
        def _(number=number, oz=oz, oy=oy, key=key, rows=rows):
            copy_of(number, oz, oy, key, rows).wait_send()

    lax.fori_loop(1, slab_count, lambda k, _: (slab_copy(k).wait_send(), 0)[1], 0)
    lax.fori_loop(1, pencil_count, lambda k, _: (pencil_copy(k).wait_send(), 0)[1], 0)
    for store in stores:
        store.wait()


def per_device(slab_count, pencil_count, solution, residual, direction, material, fixed):
    del fixed
    _, send_rows, _, receive_rows = layout()
    count = len(messages())
    f32 = jnp.float32
    flat = (3, ROWS * PLANES, LANES)
    padded = (3, PLANES, 16, LANES)

    def vmem(*shape):
        return pltpu.VMEM(shape, f32)

    def window(size):
        planes, rows = size
        return planes, rows, LANES

    hbm = pl.BlockSpec(memory_space=pl.ANY)
    out = jax.ShapeDtypeStruct(flat, f32)
    results = pl.pallas_call(
        functools.partial(kernel, slab_count, pencil_count),
        out_shape=(out, out, out),
        in_specs=[hbm] * 4,
        out_specs=(hbm, hbm, hbm),
        scratch_shapes=[
            vmem(*flat),
            vmem(*flat),
            vmem(*flat),
            pltpu.VMEM(flat[1:], jnp.int32),
            vmem(*padded),
            vmem(*padded),
            vmem(3, *window(FINE_S)),
            vmem(*padded),
            vmem(*padded),
            vmem(*window(FINE_S)),
            vmem(*window(FINE_S)),
            vmem(1, *window(FINE_S)),
            vmem(6, *window(FINE_S)),
            vmem(12, *window(FINE_S)),
            vmem(3, *window(MID_S)),
            vmem(3, *window(MID_S)),
            vmem(3, *window(MID_S)),
            vmem(*window(MID_S)),
            vmem(*window(MID_S)),
            vmem(2, *window(MID_S)),
            vmem(6, *window(MID_S)),
            vmem(12, *window(MID_S)),
            vmem(3, *window(LOW_S)),
            vmem(*window(LOW_S)),
            vmem(*window(LOW_S)),
            vmem(*window(LOW_S)),
            vmem(2, *window(LOW_S)),
            vmem(6, *window(LOW_S)),
            vmem(12, *window(LOW_S)),
            vmem(send_rows, LANES),
            vmem(receive_rows, LANES),
            vmem(8, LANES),
            vmem(slab_count, 8, LANES),
            vmem(8, LANES),
            vmem(pencil_count, 8, LANES),
            pltpu.SemaphoreType.DMA((4,)),
            pltpu.SemaphoreType.DMA((count,)),
            pltpu.SemaphoreType.DMA((count,)),
            pltpu.SemaphoreType.DMA((2, max(slab_count, pencil_count))),
            pltpu.SemaphoreType.DMA((2, max(slab_count, pencil_count))),
        ],
        compiler_params=pltpu.CompilerParams(collective_id=0, has_side_effects=True),
    )(*(inward(field) for field in (solution, residual, direction, material)))
    return tuple(outward(field) for field in results)


def inward(field):
    axes = (0, 2, 1, 3) if field.ndim == 4 else (1, 0, 2)
    return field.transpose(axes).reshape(field.shape[:-3] + (ROWS * PLANES, LANES))


def outward(field):
    return field.reshape(3, ROWS, PLANES, LANES).transpose(0, 2, 1, 3)


def solution(mesh):
    field = P(None, "slab", "pencil", "parts")
    mask = P("slab", "pencil", "parts")
    return jax.shard_map(
        functools.partial(per_device, mesh.shape["slab"], mesh.shape["pencil"]),
        mesh=mesh,
        in_specs=(field, field, field, mask, mask),
        out_specs=(field, field, field),
        check_vma=False,
    )
```

```python
import functools

import jax
import jax.numpy as jnp
import numpy as np
from jax import lax
from jax.experimental import pallas as pl
from jax.experimental.pallas import tpu as pltpu
from jax.sharding import PartitionSpec as P

SWEEPS = 4
POISSON = 0.3
VOID_MODULUS = 0.1
DAMPING = 0.6
LAME = POISSON / ((1.0 + POISSON) * (1.0 - 2.0 * POISSON))
SHEAR = 0.5 / (1.0 + POISSON)
LANES = 128
COMPS = range(3)
MESH = pl.DeviceIdType.MESH

PLANES, ROWS = 4, 12
REACH, STAGES = 3, 6
FINE_O, FINE_S = (6, 8), (14, 32)
MID_O, MID_S = (3, 4), (8, 24)
LOW_O, LOW_S = (3, 4), (7, 24)


def diagonal_entries(lengths):
    volume = lengths[0] * lengths[1] * lengths[2]
    entries = []
    for c in COMPS:
        total = 0.0
        for axis in COMPS:
            weight = (LAME + 2.0 * SHEAR) if axis == c else SHEAR
            total += weight / lengths[axis] ** 2 / 9.0
        entries.append(total * volume)
    return entries


def scaled(value, factor):
    return value if factor == 1.0 else value * factor


def element_forces(modes, modulus, lengths):
    volume = lengths[0] * lengths[1] * lengths[2]
    inv = [1.0 / length for length in lengths]

    def key(*axes):
        return tuple(1 if axis in axes else 0 for axis in COMPS)

    out = [dict() for _ in COMPS]
    e_norm = modulus * (volume / 16.0)
    e_pair = modulus * (volume / 48.0)
    e_last = modulus * (volume / 144.0)
    stretch = [scaled(modes[c][key(c)], inv[c]) for c in COMPS]
    trace = (stretch[0] + stretch[1] + stretch[2]) * LAME
    for c in COMPS:
        out[c][key(c)] = scaled(trace + stretch[c] * (2.0 * SHEAR), inv[c]) * e_norm
    for b, t in ((0, 1), (0, 2), (1, 2)):
        glide = (scaled(modes[b][key(t)], inv[t]) + scaled(modes[t][key(b)], inv[b])) * SHEAR
        glide = glide * e_norm
        out[b][key(t)] = scaled(glide, inv[t])
        out[t][key(b)] = scaled(glide, inv[b])
    for b in COMPS:
        c, t = [axis for axis in COMPS if axis != b]
        one, two = modes[c][key(c, b)], modes[t][key(t, b)]
        both = (scaled(one, inv[c]) + scaled(two, inv[t])) * LAME
        for comp, mine in ((c, one), (t, two)):
            own = 2.0 * SHEAR * inv[comp] ** 2 + SHEAR * inv[b] ** 2
            out[comp][key(comp, b)] = (scaled(both, inv[comp]) + mine * own) * e_pair
    for c in COMPS:
        b, t = [axis for axis in COMPS if axis != c]
        mine = modes[c][key(b, t)]
        first = scaled(mine, inv[b]) + scaled(modes[b][key(c, t)], inv[c])
        second = scaled(mine, inv[t]) + scaled(modes[t][key(c, b)], inv[c])
        both = scaled(first, inv[b]) + scaled(second, inv[t])
        out[c][key(b, t)] = both * SHEAR * e_pair
    for c in COMPS:
        total = 0.0
        for axis in COMPS:
            total += ((LAME + 2.0 * SHEAR) if axis == c else SHEAR) * inv[axis] ** 2
        out[c][key(0, 1, 2)] = modes[c][key(0, 1, 2)] * total * e_last
    return out


class Plane:
    def __init__(self, count, shift, factor=1):
        self.count, self.shift, self.factor = count, shift, factor

    def __add__(self, other):
        return Plane(self.count, self.shift + other, self.factor)

    def doubled(self, extra):
        return Plane(self.count, 2 * self.shift + extra, 2 * self.factor)

    def index(self, origin=0):
        return self.count * self.factor + (self.shift + origin)


def place(plane, origin):
    return plane.index(origin) if isinstance(plane, Plane) else plane + origin


def twice(plane, extra):
    return plane.doubled(extra) if isinstance(plane, Plane) else 2 * plane + extra


def over(planes, body, group=14):
    count = planes[1] + 1 - planes[0]
    group = max(n for n in range(1, group + 1) if count % n == 0)

    def step(i, _):
        stores = []
        for n in range(group):
            stores += body(Plane(i * group if group > 1 else i, planes[0] + n))
        for ref, index, value in stores:
            ref[index] = value
        return 0

    if group == count:
        stores = [store for n in range(count) for store in body(planes[0] + n)]
        for ref, index, value in stores:
            ref[index] = value
    else:
        lax.fori_loop(0, count // group, step, 0)


ALL = slice(None)


class Level:
    def __init__(self, origin, lengths, split, sums, modulus, inverse, free):
        self.oz, self.oy = origin
        self.lengths = lengths
        self.split, self.sums = split, sums
        self.modulus, self.inverse, self.free = modulus, inverse, free
        entries = diagonal_entries(lengths)
        self.entries = [entries[0]] if lengths[0] == lengths[1] else [entries[0], entries[1]]

    def at(self, plane, row):
        return place(plane, self.oz), pl.ds(row + self.oy, 8)

    def which(self, c):
        return min(c, len(self.entries) - 1)

    def inverse_of(self, c, plane, row):
        p, r = self.at(plane, row)
        return self.inverse[self.which(c), p, r, :]

    def put_split(self, c, plane, row, value):
        p, r = self.at(plane, row)
        after = pltpu.roll(value, LANES - 1, 1)
        return [
            (self.split, (2 * c, p, r, ALL), value + after),
            (self.split, (2 * c + 1, p, r, ALL), after - value),
        ]

    def set_diagonal(self, planes, rows):
        def body(plane):
            stores = []
            for row in rows:
                p, r = self.at(plane, row)
                free = self.free[p, r, :]
                total = self.node_total(plane, row)
                for n, entry in enumerate(self.entries):
                    value = DAMPING / (free * total * entry + (1.0 - free))
                    stores.append((self.inverse, (n, p, r, ALL), value))
            return stores

        over(planes, body)

    def node_total(self, plane, row):
        total = None
        for dz in (-1, 0):
            for dy in (-1, 0):
                p, r = self.at(plane + dz, row + dy)
                piece = self.modulus[p, r, :]
                total = piece if total is None else total + piece
        return total + pltpu.roll(total, 1, 1)

    def voxels(self, planes, rows):
        def pieces(plane, row):
            found = []
            for cm in range(6):
                p, r = self.at(plane, row)
                near = self.split[cm, p, r, :]
                p, r = self.at(plane, row + 1)
                far = self.split[cm, p, r, :]
                found += [near + far, far - near]
            return found

        for row in rows:

            def body(count, carry, row=row):
                plane = Plane(count, planes[0])
                lower, held = carry
                upper = pieces(plane + 1, row)
                p, r = self.at(plane, row)
                modes = []
                for c in COMPS:
                    mine = {}
                    for m in range(2):
                        for iy in range(2):
                            k = (2 * c + m) * 2 + iy
                            if m + iy > 0:
                                mine[(m, iy, 0)] = lower[k] + upper[k]
                            mine[(m, iy, 1)] = upper[k] - lower[k]
                    modes.append(mine)
                forces = element_forces(modes, self.modulus[p, r, :], self.lengths)
                keep = []
                for c in COMPS:
                    for m in range(2):
                        node = []
                        for iy in range(2):
                            k = (2 * c + m) * 2 + iy
                            diff = forces[c][(m, iy, 1)]
                            if m + iy > 0:
                                same = forces[c][(m, iy, 0)]
                                node.append(held[k] + (same - diff))
                                keep.append(same + diff)
                            else:
                                node.append(held[k] - diff)
                                keep.append(diff)
                        self.sums[(2 * c + m) * 2, p, r, :] = node[0] - node[1]
                        self.sums[(2 * c + m) * 2 + 1, p, r, :] = node[0] + node[1]
                return upper, keep

            zero = [jnp.zeros((8, LANES), jnp.float32)] * 12
            lax.fori_loop(0, planes[1] + 1 - planes[0], body, (pieces(planes[0], row), zero))

    def applied(self, c, plane, row):
        parts = []
        for m in range(2):
            k = (2 * c + m) * 2
            p, r = self.at(plane, row)
            here = self.sums[k, p, r, :]
            p, r = self.at(plane, row - 1)
            parts.append(here + self.sums[k + 1, p, r, :])
        return (parts[0] - parts[1]) + pltpu.roll(parts[0] + parts[1], 1, 1)


def messages():
    found = []
    for oz in (0, -1, 1):
        for oy in (0, -1, 1):
            if (oz, oy) != (0, 0):
                found.append(("wide", oz, oy, ("wide", oy), {0: 192, -1: 72, 1: 64}[oy]))
    for oy in (0, -1, 1):
        found.append(("far", -2, oy, ("far", oy), {0: 24, -1: 16, 1: 8}[oy]))
    for oz in (0, -1, 1):
        for oy in (0, -1, 1):
            if (oz, oy) != (0, 0):
                rows = (8 if oy else 40) if oz else 16
                found.append(("dir", oz, oy, ("dir", oz, oy), rows))
    for oz in (0, -1, 1, -2, 2, -3, 3):
        for oy in (0, -1, 1):
            if (oz, oy) != (0, 0):
                found.append(("fixlow", oz, oy, ("fixlow",), 16))
    for oz in (0, -1, 1, -2, 2, -3, 3):
        for oy in (0, -1, 1):
            if (oz, oy) != (0, 0):
                found.append(("low", oz, oy, ("low",), 16))
    for oz in (0, -1, 1):
        for oy in (0, -1, 1):
            if (oz, oy) != (0, 0):
                found.append(("mid", oz, oy, ("mid", oy), 24 if oy else 72))
    for oz in (0, -1, 1, -2, 2):
        for oy in (0, -1, 1):
            if (oz, oy) != (0, 0):
                each = 16 if oy else 24
                part = {-2: 1, 2: 0}.get(oz)
                found.append(("lift", oz, oy, ("lift", oy, part), each if part is not None else 2 * each))
    return found


def layout():
    sends, receives = {}, {}
    at_send = at_receive = 0
    for oy in (0, -1, 1):
        each = 16 if oy else 24
        sends[("lift", oy, None)] = at_send
        sends[("lift", oy, 0)] = at_send
        sends[("lift", oy, 1)] = at_send + each
        at_send += 2 * each
    for name, oz, oy, key, rows in messages():
        if key not in sends:
            sends[key] = at_send
            at_send += rows
        receives[(name, oz, oy)] = at_receive
        at_receive += rows
    return sends, at_send, receives, at_receive


def kernel(
    slab_count,
    pencil_count,
    solution_ref,
    residual_ref,
    direction_ref,
    material_ref,
    next_solution_ref,
    next_residual_ref,
    next_direction_ref,
    sol_in,
    res_in,
    dir_in,
    mat,
    res,
    dirn,
    s0,
    e0,
    old,
    e_fine,
    f_fine,
    i_fine,
    x_fine,
    b_fine,
    s1,
    u1,
    c1,
    e_mid,
    f_mid,
    i_mid,
    x_mid,
    b_mid,
    s2,
    e_low,
    f_low,
    m_low,
    i_low,
    x_low,
    b_low,
    outbox,
    inbox,
    part_out,
    slab_in,
    line_out,
    pencil_in,
    local_sem,
    send_sem,
    recv_sem,
    sum_send,
    sum_recv,
    word_sem,
):
    slab_at, pencil_at = lax.axis_index("slab"), lax.axis_index("pencil")
    sends, _, receives, _ = layout()
    all_messages = messages()
    fine = Level(FINE_O, (1.0, 1.0, 1.0), x_fine, b_fine, e_fine, i_fine, f_fine)
    mid = Level(MID_O, (1.0, 2.0, 2.0), x_mid, b_mid, e_mid, i_mid, f_mid)
    low = Level(LOW_O, (1.0, 4.0, 4.0), x_low, b_low, e_low, i_low, f_low)

    loads = [
        pltpu.make_async_copy(source, target, local_sem.at[n])
        for n, (source, target) in enumerate(
            ((material_ref, mat), (residual_ref, res_in), (direction_ref, dir_in), (solution_ref, sol_in))
        )
    ]
    for load in loads:
        load.start()

    def there(oz, oy):
        z, y = slab_at + oz, pencil_at + oy
        return (z >= 0) & (z < slab_count) & (y >= 0) & (y < pencil_count)

    inbox[...] = jnp.zeros_like(inbox)

    barrier = pltpu.get_barrier_semaphore()
    greeted = jnp.int32(0)
    for oz in range(-REACH, REACH + 1):
        for oy in (-1, 0, 1):
            if (oz, oy) != (0, 0):
                near = there(oz, oy)
                greeted = greeted + jnp.where(near, 1, 0)

                @pl.when(near)
                def _(oz=oz, oy=oy):
                    pl.semaphore_signal(
                        barrier,
                        inc=1,
                        device_id={"slab": slab_at + oz, "pencil": pencil_at + oy},
                        device_id_type=MESH,
                    )

    def stages(count, known):
        steps = []
        while known < count - 1:
            step = min(known, count - 1 - known)
            steps.append(step)
            known += step
        return steps

    plan = [("slab", stages(slab_count, REACH)), ("pencil", stages(pencil_count, 1))]

    def sides(axis, step):
        return [(step * sign if axis == "slab" else 0, step * sign if axis == "pencil" else 0) for sign in (-1, 1)]

    def tell(stage):
        for which, (axis, steps) in enumerate(plan):
            if stage < len(steps):
                for side, (oz, oy) in enumerate(sides(axis, steps[stage])):

                    @pl.when(there(oz, oy))
                    def _(oz=oz, oy=oy):
                        pl.semaphore_signal(
                            word_sem.at[which, stage, 1 - side],
                            inc=1,
                            device_id={"slab": slab_at + oz, "pencil": pencil_at + oy},
                            device_id_type=MESH,
                        )

    def hear(stage):
        for which, (axis, steps) in enumerate(plan):
            if stage < len(steps):
                for side, (oz, oy) in enumerate(sides(axis, steps[stage])):

                    @pl.when(there(oz, oy))
                    def _():
                        pl.semaphore_wait(word_sem.at[which, stage, side], 1)

    for ref in (s0, e_fine, x_fine, b_fine, s1, u1, c1, x_mid, b_mid, s2, e_low, f_low, m_low, i_low, x_low, b_low):
        ref[...] = jnp.zeros_like(ref)
    e_mid[...] = jnp.zeros_like(e_mid)
    f_mid[...] = jnp.zeros_like(f_mid)
    i_mid[...] = jnp.zeros_like(i_mid)
    f_fine[...] = jnp.zeros_like(f_fine)
    i_fine[...] = jnp.zeros_like(i_fine)

    def copy_of(number, oz, oy, key, rows):
        name = all_messages[number][0]
        return pltpu.make_async_remote_copy(
            src_ref=outbox.at[pl.ds(sends[key], rows)],
            dst_ref=inbox.at[pl.ds(receives[(name, oz, oy)], rows)],
            send_sem=send_sem.at[number],
            recv_sem=recv_sem.at[number],
            device_id={"slab": slab_at - oz, "pencil": pencil_at - oy},
            device_id_type=MESH,
        )

    def start(*names):
        for number, (name, oz, oy, key, rows) in enumerate(all_messages):
            if name in names:

                @pl.when(there(-oz, -oy))
                def _(number=number, oz=oz, oy=oy, key=key, rows=rows):
                    copy_of(number, oz, oy, key, rows).start()

    def arrive(*names):
        for number, (name, oz, oy, key, rows) in enumerate(all_messages):
            if name in names:

                @pl.when(there(oz, oy))
                def _(number=number, oz=oz, oy=oy, key=key, rows=rows):
                    copy_of(number, oz, oy, key, rows).wait_recv()

    def take(name, oz, oy):
        return receives[(name, oz, oy)]

    def strided(p, first, count):
        return pl.ds(p + PLANES * first, count, stride=PLANES)

    def planes_first(source, target):
        for c in COMPS:
            for p in range(PLANES):
                for first, count in ((0, 8), (8, 4)):
                    target[c, p, pl.ds(first, count), :] = source[c, strided(p, first, count), :]

    loads[0].wait()
    loads[1].wait()
    planes_first(res_in, res)

    taken_rows = {0: (0, 12), -1: (8, 4), 1: (0, 4)}
    voxel_rows = {0: (0, 12), -1: (6, 6), 1: (0, 4)}
    for oy in (0, -1, 1):
        at = sends[("wide", oy)]
        first, count = taken_rows[oy]
        for c in COMPS:
            for p in range(PLANES):
                outbox[pl.ds(at, count), :] = res[c, p, pl.ds(first, count), :]
                at += count
        first, count = voxel_rows[oy]
        for p in range(PLANES):
            outbox[pl.ds(at, count), :] = (mat[strided(p, first, count), :] == 1).astype(jnp.float32)
            at += count
        at = sends[("far", oy)]
        for p in (2, 3):
            outbox[pl.ds(at, count), :] = (mat[strided(p, first, count), :] == 1).astype(jnp.float32)
            at += count

    loads[2].wait()
    planes_first(dir_in, dirn)
    for name, oz, oy, key, rows in all_messages:
        if name == "dir":
            at = sends[key]
            planes = {0: range(PLANES), -1: (3,), 1: (0,)}[oz]
            first, count = {0: (0, 12), -1: (11, 1), 1: (0, 1)}[oy]
            for c in COMPS:
                for p in planes:
                    outbox[pl.ds(at, count), :] = dirn[c, p, pl.ds(first, count), :]
                    at += count

    pl.semaphore_wait(barrier, greeted)
    start("wide", "far")
    start("dir")
    tell(0)

    for c in COMPS:
        for p in range(PLANES):
            s0[c, p + FINE_O[0], pl.ds(FINE_O[1], ROWS), :] = res[c, p, pl.ds(0, ROWS), :]
    for p in range(PLANES):
        for first, count in ((0, 8), (8, 4)):
            e_fine[p + FINE_O[0], pl.ds(first + FINE_O[1], count), :] = (mat[strided(p, first, count), :] == 1).astype(
                jnp.float32
            )

    arrive("wide", "far")
    hear(0)
    tell(1)
    for oz in (0, -1, 1):
        for oy in (0, -1, 1):
            if (oz, oy) == (0, 0):
                continue
            at = receives[("wide", oz, oy)]
            first, count = {0: (0, 12), -1: (-4, 4), 1: (12, 4)}[oy]
            for c in COMPS:
                for p in range(PLANES):
                    s0[c, p + oz * PLANES + FINE_O[0], pl.ds(first + FINE_O[1], count), :] = inbox[pl.ds(at, count), :]
                    at += count
            first, count = {0: (0, 12), -1: (-6, 6), 1: (12, 4)}[oy]
            for p in range(PLANES):
                e_fine[p + oz * PLANES + FINE_O[0], pl.ds(first + FINE_O[1], count), :] = inbox[pl.ds(at, count), :]
                at += count
    for oy in (0, -1, 1):
        at = receives[("far", -2, oy)]
        first, count = {0: (0, 12), -1: (-6, 6), 1: (12, 4)}[oy]
        for p in (-6, -5):
            e_fine[p + FINE_O[0], pl.ds(first + FINE_O[1], count), :] = inbox[pl.ds(at, count), :]
            at += count

    total_planes, total_rows = slab_count * PLANES, pencil_count * ROWS
    row_iota = lax.broadcasted_iota(jnp.int32, (8, LANES), 0)
    lane_iota = lax.broadcasted_iota(jnp.int32, (8, LANES), 1)

    def moduli_body(p):
        plane = slab_at * PLANES + place(p, 0)
        plane_ok = (plane >= 0) & (plane < total_planes - 1)
        stores = []
        for row in (-8, 0, 8):
            ip, ir = fine.at(p, row)
            rows = row_iota + (pencil_at * ROWS + row)
            keep = (rows >= 0) & (rows < total_rows - 1) & (lane_iota < LANES - 1) & plane_ok
            value = jnp.where(e_fine[ip, ir, :] > 0.5, 1.0, VOID_MODULUS)
            stores.append((e_fine, (ip, ir, ALL), jnp.where(keep, value, 0.0)))
        return stores

    over((-6, 7), moduli_body)

    def fine_body(p):
        plane = slab_at * PLANES + place(p, 0)
        inside = (plane > 0) & (plane < total_planes - 1)
        stores = []
        for row in (-5, 3, 8):
            ip, ir = fine.at(p, row)
            total = fine.node_total(p, row)
            free = jnp.where((total > 0.9) & inside, 1.0, 0.0)
            weight = DAMPING / (free * total * fine.entries[0] + (1.0 - free))
            stores += [(f_fine, (ip, ir, ALL), free), (i_fine, (0, ip, ir, ALL), weight)]
        return stores

    over((-5, 7), fine_body)

    def first_update(p):
        stores = []
        for row in (-4, 4, 8):
            ip, ir = fine.at(p, row)
            weight = i_fine[0, ip, ir, :] * f_fine[ip, ir, :]
            for c in COMPS:
                stores += fine.put_split(c, p, row, s0[c, ip, ir, :] * weight)
        return stores

    over((-4, 7), first_update)

    def halves(ref, c, p, row):
        found = []
        for dp in range(2):
            for dr in range(2):
                r = pl.ds(2 * row + dr + FINE_O[1], 8, stride=2)
                ip = place(twice(p, dp), FINE_O[0])
                found.append(ref[ip, r, :] if c is None else ref[c, ip, r, :])
        return found

    def mid_moduli(p):
        plane_ok = slab_at * (PLANES // 2) + place(p, 0) < total_planes // 2 - 1
        stores = []
        for row in (-3, 0):
            ip, ir = mid.at(p, row)
            a, b, c, d = halves(e_fine, None, p, row)
            rows = row_iota + (pencil_at * (ROWS // 2) + row)
            keep = (rows < total_rows // 2 - 1) & plane_ok
            stores.append((e_mid, (ip, ir, ALL), jnp.where(keep, (a + b + c + d) * 0.25, 0.0)))
        return stores

    over((-3, 3), mid_moduli)

    def mid_free(p):
        stores = []
        for row in (-2, 0):
            ip, ir = mid.at(p, row)
            a, b, c, d = halves(f_fine, None, p, row)
            stores.append((f_mid, (ip, ir, ALL), jnp.maximum(jnp.maximum(a, b), jnp.maximum(c, d))))
        return stores

    over((-2, 3), mid_free)
    mid.set_diagonal((-2, 3), (-2, 0))

    def mid_pair(ref, c, p, row):
        found = []
        for dp in range(2):
            for dr in range(2):
                r = pl.ds(2 * row + dr + MID_O[1], 8, stride=2)
                ip = place(twice(p, dp), MID_O[0])
                found.append(ref[ip, r, :] if c is None else ref[c, ip, r, :])
        return found

    for p in (-1, 0):
        ip, ir = low.at(p, -1)
        a, b, c, d = mid_pair(e_mid, None, p, -1)
        rows = row_iota + (pencil_at * (ROWS // 4) - 1)
        keep = (rows < total_rows // 4 - 1) & (slab_at * (PLANES // 4) + p < total_planes // 4 - 1) & (row_iota < 4)
        e_low[ip, ir, :] = jnp.where(keep, (a + b + c + d) * 0.25, 0.0)
    a, b, c, d = mid_pair(f_mid, None, 0, 0)
    ip, ir = low.at(0, 0)
    f_low[ip, ir, :] = jnp.where(row_iota < 3, jnp.maximum(jnp.maximum(a, b), jnp.maximum(c, d)), 0.0)
    m_low[ip, ir, :] = jnp.where(row_iota < 3, low.node_total(0, 0), 0.0)
    at = sends[("fixlow",)]
    own_rows = pl.ds(LOW_O[1], 3)
    for n, ref in enumerate((e_low, f_low, m_low)):
        outbox[pl.ds(at + 3 * n, 3), :] = ref[LOW_O[0], own_rows, :]
    start("fixlow")

    fine.voxels((-4, 6), (-4, 4, 12))

    def fine_step(rows, starting):
        def body(p):
            stores = []
            for row in rows:
                ip, ir = fine.at(p, row)
                free = f_fine[ip, ir, :]
                weight = i_fine[0, ip, ir, :]
                for c in COMPS:
                    remain = s0[c, ip, ir, :]
                    update = weight * remain
                    remain = remain - free * fine.applied(c, p, row) - (1.0 - free) * update
                    stores.append((s0, (c, ip, ir, ALL), remain))
                    if starting:
                        stores += fine.put_split(c, p, row, free * (weight * remain))
            return stores

        return body

    def estimate_add(starting):
        def body(p):
            stores = []
            for row in (0, 8):
                ip, ir = fine.at(p, row)
                weight = i_fine[0, ip, ir, :]
                for c in COMPS:
                    update = weight * s0[c, ip, ir, :]
                    own = (c, place(p, 0), pl.ds(row, 8), ALL)
                    stores.append((e0, own, update if starting else e0[own] + update))
            return stores

        over((0, 3), body)

    estimate_add(True)
    over((-3, 6), fine_step((-3, 5, 13), True))
    estimate_add(False)
    fine.voxels((-3, 5), (-3, 5, 13))
    over((-2, 5), fine_step((-2, 6), False))

    def mid_first(p):
        ip, ir = mid.at(p, -1)
        free = f_mid[ip, ir, :]
        masks = halves(f_fine, None, p, -1)
        stores = []
        for c in COMPS:
            parts = halves(s0, c, p, -1)
            rhs = free * (
                (parts[0] * masks[0] + parts[1] * masks[1]) + (parts[2] * masks[2] + parts[3] * masks[3])
            )
            update = mid.inverse_of(c, p, -1) * rhs
            stores += [(s1, (c, ip, ir, ALL), rhs), (u1, (c, ip, ir, ALL), update)]
            stores += mid.put_split(c, p, -1, free * update)
        return stores

    over((-1, 2), mid_first)
    mid.voxels((-1, 1), (-1,))

    def mid_remain(p):
        ip, ir = mid.at(p, 0)
        free = f_mid[ip, ir, :]
        stores = []
        for c in COMPS:
            remain = s1[c, ip, ir, :] - free * mid.applied(c, p, 0) - (1.0 - free) * u1[c, ip, ir, :]
            stores.append((s1, (c, ip, ir, ALL), remain))
        return stores

    over((0, 1), mid_remain)

    masks = mid_pair(f_mid, None, 0, 0)
    ip, ir = low.at(0, 0)
    free = f_low[ip, ir, :]
    at = sends[("low",)]
    for c in COMPS:
        parts = mid_pair(s1, c, 0, 0)
        rhs = free * ((parts[0] * masks[0] + parts[1] * masks[1]) + (parts[2] * masks[2] + parts[3] * masks[3]))
        rhs = jnp.where(row_iota < 3, rhs, 0.0)
        s2[c, ip, ir, :] = rhs
        outbox[pl.ds(at + 3 * c, 3), :] = rhs[0:3, :]
    start("low")
    mid_rows = {0: (0, 6), -1: (4, 2), 1: (0, 2)}
    for oy in (0, -1, 1):
        at = sends[("mid", oy)]
        first, count = mid_rows[oy]
        for ref in (s1, u1):
            for c in COMPS:
                for p in range(2):
                    outbox[pl.ds(at, count), :] = ref[c, p + MID_O[0], pl.ds(first + MID_O[1], count), :]
                    at += count
    start("mid")

    hear(1)
    tell(2)
    arrive("dir")
    arrive("fixlow")
    def direction_rows(plane, first, count, c, value):
        ip, ir = plane + FINE_O[0], pl.ds(first + FINE_O[1], count)
        value = value * f_fine[ip, ir, :]
        after = pltpu.roll(value, LANES - 1, 1)
        x_fine[2 * c, ip, ir, :] = value + after
        x_fine[2 * c + 1, ip, ir, :] = after - value

    for oz in (0, -1, 1):
        for oy in (0, -1, 1):
            planes = {0: range(PLANES), -1: (-1,), 1: (PLANES,)}[oz]
            first, count = {0: (0, 12), -1: (-1, 1), 1: (12, 1)}[oy]
            at = None if (oz, oy) == (0, 0) else receives[("dir", oz, oy)]
            for c in COMPS:
                for p in planes:
                    if at is None:
                        direction_rows(p, first, count, c, dirn[c, p, pl.ds(0, ROWS), :])
                    else:
                        direction_rows(p, first, count, c, inbox[pl.ds(at, count), :])
                        at += count
    fine.voxels((-1, 3), (-1, 7))

    def old_image(p):
        stores = []
        for row in (0, 4):
            ip, ir = fine.at(p, row)
            free = f_fine[ip, ir, :]
            for c in COMPS:
                value = dirn[c, place(p, 0), pl.ds(row, 8), :]
                image = free * fine.applied(c, p, row) + (1.0 - free) * value
                stores.append((old, (c, place(p, 0), pl.ds(row, 8), ALL), image))
        return stores

    over((0, 3), old_image)

    def low_window(name, refs):
        for oz in (0, -1, 1, -2, 2, -3, 3):
            for oy in (0, -1, 1):
                if (oz, oy) == (0, 0):
                    continue
                at = receives[(name, oz, oy)]
                for n, ref in enumerate(refs):
                    ref[oz + LOW_O[0], pl.ds(3 * oy + LOW_O[1], 3), :] = inbox[pl.ds(at + 3 * n, 3), :]

    low_window("fixlow", (e_low, f_low, m_low))

    def low_inverse(p):
        stores = []
        for row in (-4, 4):
            ip, ir = low.at(p, row)
            free = f_low[ip, ir, :]
            total = m_low[ip, ir, :]
            for n, entry in enumerate(low.entries):
                stores.append((i_low, (n, ip, ir, ALL), DAMPING / (free * total * entry + (1.0 - free))))
        return stores

    over((-3, 3), low_inverse)

    arrive("low")
    hear(2)
    tell(3)
    low_window("low", [s2.at[c] for c in COMPS])

    def low_split(planes, rows):
        def body(p):
            stores = []
            for row in rows:
                ip, ir = low.at(p, row)
                free = f_low[ip, ir, :]
                for c in COMPS:
                    stores += low.put_split(c, p, row, free * (low.inverse_of(c, p, row) * s2[c, ip, ir, :]))
            return stores

        over(planes, body, 7)

    ip, ir = low.at(0, 0)
    bottom = [low.inverse_of(c, 0, 0) * s2[c, ip, ir, :] for c in COMPS]
    low_split((-3, 3), (-3, 5))
    for depth in (2, 1, 0):
        low.voxels((-1 - depth, depth), (-1 - depth,))

        def low_step(p, depth=depth):
            row = -depth
            ip, ir = low.at(p, row)
            free = f_low[ip, ir, :]
            stores = []
            for c in COMPS:
                remain = s2[c, ip, ir, :]
                update = low.inverse_of(c, p, row) * remain
                remain = remain - free * low.applied(c, p, row) - (1.0 - free) * update
                stores.append((s2, (c, ip, ir, ALL), remain))
                if depth:
                    stores += low.put_split(c, p, row, free * (low.inverse_of(c, p, row) * remain))
            return stores

        over((-depth, depth), low_step, 5)
        ip, ir = low.at(0, 0)
        for c in COMPS:
            bottom[c] = bottom[c] + low.inverse_of(c, 0, 0) * s2[c, ip, ir, :]

    for c in COMPS:
        for p in range(2):
            for dr in range(2):
                c1[c, p + MID_O[0], pl.ds(MID_O[1] + dr, 3, stride=2), :] = bottom[c][0:3, :]
    for c in COMPS:
        for p in range(2):
            ip, ir = p + MID_O[0], pl.ds(MID_O[1], 6)
            c1[c, ip, ir, :] = c1[c, ip, ir, :] * f_mid[ip, ir, :]
    for oy in (0, -1, 1):
        first, count = {0: (0, 6), -1: (3, 3), 1: (0, 3)}[oy]
        for p in range(2):
            at = sends[("lift", oy, p)]
            for c in COMPS:
                outbox[pl.ds(at, count), :] = c1[c, p + MID_O[0], pl.ds(first + MID_O[1], count), :]
                at += count
    start("lift")
    arrive("mid")
    for oz in (0, -1, 1):
        for oy in (0, -1, 1):
            if (oz, oy) == (0, 0):
                continue
            at = receives[("mid", oz, oy)]
            first, count = {0: (0, 6), -1: (-2, 2), 1: (6, 2)}[oy]
            for ref in (s1, u1):
                for c in COMPS:
                    for p in range(2):
                        ref[c, p + 2 * oz + MID_O[0], pl.ds(first + MID_O[1], count), :] = inbox[pl.ds(at, count), :]
                        at += count
    arrive("lift")
    for stage in range(3, STAGES):
        if stage > 3:
            tell(stage)
        hear(stage)
    for oz in (0, -1, 1, -2, 2):
        for oy in (0, -1, 1):
            if (oz, oy) == (0, 0):
                continue
            base = receives[("lift", oz, oy)]
            first, count = {0: (0, 6), -1: (-3, 3), 1: (6, 3)}[oy]
            planes = {-2: (-3,), 2: (4,)}.get(oz, (2 * oz, 2 * oz + 1))
            for n, p in enumerate(planes):
                at = base + n * (16 if oy else 24)
                for c in COMPS:
                    c1[c, p + MID_O[0], pl.ds(first + MID_O[1], count), :] = inbox[pl.ds(at, count), :]
                    at += count

    def lift_split(p):
        stores = []
        for row in (-3, 5):
            ip, ir = mid.at(p, row)
            for c in COMPS:
                stores += mid.put_split(c, p, row, c1[c, ip, ir, :])
        return stores

    over((-3, 4), lift_split)
    mid.voxels((-3, 3), (-3, 5))

    def mid_second(p):
        stores = []
        for row in (-2, 6):
            ip, ir = mid.at(p, row)
            free = f_mid[ip, ir, :]
            for c in COMPS:
                remain = s1[c, ip, ir, :] - free * mid.applied(c, p, row)
                here = (c, ip, ir, ALL)
                stores.append((u1, here, u1[here] + c1[here] + mid.inverse_of(c, p, row) * remain))
        return stores

    over((-2, 3), mid_second)

    def lift_fine(p):
        stores = []
        for row in (-2, 0):
            ip, ir = mid.at(p, row)
            for c in COMPS:
                value = u1[c, ip, ir, :]
                for dp in range(2):
                    for dr in range(2):
                        out = pl.ds(2 * row + dr + FINE_O[1], 8, stride=2)
                        stores.append((x_fine, (2 * c, place(twice(p, dp), FINE_O[0]), out, ALL), value))
        return stores

    over((-2, 3), lift_fine)

    def lift_parts(p):
        stores = []
        for row in (-4, 4, 12):
            ip, ir = fine.at(p, row)
            free = f_fine[ip, ir, :]
            for c in COMPS:
                stores += fine.put_split(c, p, row, free * x_fine[2 * c, ip, ir, :])
        return stores

    def lift_own(p):
        stores = []
        for row in (0, 8):
            ip, ir = fine.at(p, row)
            free = f_fine[ip, ir, :]
            for c in COMPS:
                part = free * x_fine[2 * c, ip, ir, :]
                own = (c, place(p, 0), pl.ds(row, 8), ALL)
                stores.append((e0, own, e0[own] + part))
        return stores

    over((0, 3), lift_own)
    over((-4, 7), lift_parts)
    fine.voxels((-3, 5), (-3, 5, 13))

    def lift_step(p):
        stores = []
        for row in (-2, 6):
            ip, ir = fine.at(p, row)
            free = f_fine[ip, ir, :]
            weight = i_fine[0, ip, ir, :]
            for c in COMPS:
                remain = s0[c, ip, ir, :] - free * fine.applied(c, p, row)
                stores.append((s0, (c, ip, ir, ALL), remain))
                stores += fine.put_split(c, p, row, free * (weight * remain))
        return stores

    over((-2, 5), lift_step)
    estimate_add(False)
    fine.voxels((-2, 4), (-2, 6))
    over((-1, 4), fine_step((-1, 7), True))
    estimate_add(False)
    fine.voxels((-1, 3), (-1, 7))
    over((0, 3), fine_step((0, 8), False))

    def dots(p, totals):
        totals = list(totals)
        for row in (0, 4):
            ip, ir = p + FINE_O[0], pl.ds(row + FINE_O[1], 8)
            keep = None if row == 0 else row_iota >= 4
            for c in COMPS:
                rows = pl.ds(row, 8)
                z, d, o, r = e0[c, p, rows, :], dirn[c, p, rows, :], old[c, p, rows, :], res[c, p, rows, :]
                new = r - s0[c, ip, ir, :]
                for n, term in enumerate((z * o, d * o, z * new, r * z, r * d)):
                    totals[n] = totals[n] + (term if keep is None else jnp.where(keep, term, 0.0))
        return tuple(totals)

    totals = lax.fori_loop(0, PLANES, dots, (jnp.zeros((8, LANES), jnp.float32),) * 5)
    for n, total in enumerate(totals):
        part_out[pl.ds(n, 1), :] = jnp.sum(total, axis=0, keepdims=True)

    def share(axis, at, count, source, target, which):
        def copy(k):
            return pltpu.make_async_remote_copy(
                src_ref=source,
                dst_ref=target.at[k],
                send_sem=sum_send.at[which, k],
                recv_sem=sum_recv.at[which, k],
                device_id={axis: lax.rem(at + k, count)},
                device_id_type=MESH,
            )

        lax.fori_loop(1, count, lambda k, _: (copy(k).start(), 0)[1], 0)
        lax.fori_loop(1, count, lambda k, _: (copy(k).wait_recv(), 0)[1], 0)
        total = source[...]
        total = lax.fori_loop(1, count, lambda k, t: t + target[k], total)
        return total, copy

    line, slab_copy = share("slab", slab_at, slab_count, part_out, slab_in, 0)
    line_out[...] = line
    whole, pencil_copy = share("pencil", pencil_at, pencil_count, line_out, pencil_in, 1)
    summed = jnp.sum(whole, axis=1, keepdims=True)
    t = [summed[n : n + 1, :] for n in range(5)]
    beta = -t[0] / t[1]
    along = t[3] + beta * t[4]
    curvature = t[2] + 2.0 * beta * t[0] + beta * beta * t[1]
    step = along / curvature

    loads[3].wait()

    for c in COMPS:
        for p in range(PLANES):
            for first, count in ((0, 8), (8, 4)):
                rows, there_rows = pl.ds(first, count), strided(p, first, count)
                z, d, o, r = e0[c, p, rows, :], dirn[c, p, rows, :], old[c, p, rows, :], res[c, p, rows, :]
                new = r - s0[c, p + FINE_O[0], pl.ds(first + FINE_O[1], count), :]
                nd = z + beta * d
                image = new + beta * o
                next_direction_ref[c, there_rows, :] = nd
                next_solution_ref[c, there_rows, :] = sol_in[c, there_rows, :] + step * nd
                next_residual_ref[c, there_rows, :] = r - step * image
    for number, (name, oz, oy, key, rows) in enumerate(all_messages):

        @pl.when(there(-oz, -oy))
        def _(number=number, oz=oz, oy=oy, key=key, rows=rows):
            copy_of(number, oz, oy, key, rows).wait_send()

    lax.fori_loop(1, slab_count, lambda k, _: (slab_copy(k).wait_send(), 0)[1], 0)
    lax.fori_loop(1, pencil_count, lambda k, _: (pencil_copy(k).wait_send(), 0)[1], 0)


def per_device(slab_count, pencil_count, solution, residual, direction, material, fixed):
    del fixed
    _, send_rows, _, receive_rows = layout()
    count = len(messages())
    f32 = jnp.float32
    flat = (3, ROWS * PLANES, LANES)
    padded = (3, PLANES, 16, LANES)

    def vmem(*shape):
        return pltpu.VMEM(shape, f32)

    def window(size):
        planes, rows = size
        return planes, rows, LANES

    hbm = pl.BlockSpec(memory_space=pl.ANY)
    out = jax.ShapeDtypeStruct(flat, f32)
    results = pl.pallas_call(
        functools.partial(kernel, slab_count, pencil_count),
        out_shape=(out, out, out),
        in_specs=[hbm] * 4,
        out_specs=(pl.BlockSpec(memory_space=pltpu.VMEM),) * 3,
        scratch_shapes=[
            vmem(*flat),
            vmem(*flat),
            vmem(*flat),
            pltpu.VMEM(flat[1:], jnp.int32),
            vmem(*padded),
            vmem(*padded),
            vmem(3, *window(FINE_S)),
            vmem(*padded),
            vmem(*padded),
            vmem(*window(FINE_S)),
            vmem(*window(FINE_S)),
            vmem(1, *window(FINE_S)),
            vmem(6, *window(FINE_S)),
            vmem(12, *window(FINE_S)),
            vmem(3, *window(MID_S)),
            vmem(3, *window(MID_S)),
            vmem(3, *window(MID_S)),
            vmem(*window(MID_S)),
            vmem(*window(MID_S)),
            vmem(2, *window(MID_S)),
            vmem(6, *window(MID_S)),
            vmem(12, *window(MID_S)),
            vmem(3, *window(LOW_S)),
            vmem(*window(LOW_S)),
            vmem(*window(LOW_S)),
            vmem(*window(LOW_S)),
            vmem(2, *window(LOW_S)),
            vmem(6, *window(LOW_S)),
            vmem(12, *window(LOW_S)),
            vmem(send_rows, LANES),
            vmem(receive_rows, LANES),
            vmem(8, LANES),
            vmem(slab_count, 8, LANES),
            vmem(8, LANES),
            vmem(pencil_count, 8, LANES),
            pltpu.SemaphoreType.DMA((4,)),
            pltpu.SemaphoreType.DMA((count,)),
            pltpu.SemaphoreType.DMA((count,)),
            pltpu.SemaphoreType.DMA((2, max(slab_count, pencil_count))),
            pltpu.SemaphoreType.DMA((2, max(slab_count, pencil_count))),
            pltpu.SemaphoreType.REGULAR((2, STAGES, 2)),
        ],
        compiler_params=pltpu.CompilerParams(collective_id=0, has_side_effects=True),
    )(*(inward(field) for field in (solution, residual, direction, material)))
    return tuple(outward(field) for field in results)


def inward(field):
    axes = (0, 2, 1, 3) if field.ndim == 4 else (1, 0, 2)
    return field.transpose(axes).reshape(field.shape[:-3] + (ROWS * PLANES, LANES))


def outward(field):
    return field.reshape(3, ROWS, PLANES, LANES).transpose(0, 2, 1, 3)


def solution(mesh):
    field = P(None, "slab", "pencil", "parts")
    mask = P("slab", "pencil", "parts")
    return jax.shard_map(
        functools.partial(per_device, mesh.shape["slab"], mesh.shape["pencil"]),
        mesh=mesh,
        in_specs=(field, field, field, mask, mask),
        out_specs=(field, field, field),
        check_vma=False,
    )
```

```python
import functools

import jax
import jax.numpy as jnp
import numpy as np
from jax import lax
from jax.experimental import pallas as pl
from jax.experimental.pallas import tpu as pltpu
from jax.sharding import PartitionSpec as P

SWEEPS = 4
POISSON = 0.3
VOID_MODULUS = 0.1
DAMPING = 0.6
LAME = POISSON / ((1.0 + POISSON) * (1.0 - 2.0 * POISSON))
SHEAR = 0.5 / (1.0 + POISSON)
LANES = 128
COMPS = range(3)
MESH = pl.DeviceIdType.MESH

PLANES, ROWS = 4, 12
REACH, STAGES = 2, 6
FINE_O, FINE_S = (6, 8), (14, 32)
MID_O, MID_S = (3, 4), (8, 24)
LOW_O, LOW_S = (3, 4), (7, 24)


def diagonal_entries(lengths):
    volume = lengths[0] * lengths[1] * lengths[2]
    entries = []
    for c in COMPS:
        total = 0.0
        for axis in COMPS:
            weight = (LAME + 2.0 * SHEAR) if axis == c else SHEAR
            total += weight / lengths[axis] ** 2 / 9.0
        entries.append(total * volume)
    return entries


def scaled(value, factor):
    return value if factor == 1.0 else value * factor


def element_forces(modes, modulus, lengths):
    volume = lengths[0] * lengths[1] * lengths[2]
    inv = [1.0 / length for length in lengths]

    def key(*axes):
        return tuple(1 if axis in axes else 0 for axis in COMPS)

    out = [dict() for _ in COMPS]
    e_norm = modulus * (volume / 16.0)
    e_pair = modulus * (volume / 48.0)
    e_last = modulus * (volume / 144.0)
    stretch = [scaled(modes[c][key(c)], inv[c]) for c in COMPS]
    trace = (stretch[0] + stretch[1] + stretch[2]) * LAME
    for c in COMPS:
        out[c][key(c)] = scaled(trace + stretch[c] * (2.0 * SHEAR), inv[c]) * e_norm
    for b, t in ((0, 1), (0, 2), (1, 2)):
        glide = (scaled(modes[b][key(t)], inv[t]) + scaled(modes[t][key(b)], inv[b])) * SHEAR
        glide = glide * e_norm
        out[b][key(t)] = scaled(glide, inv[t])
        out[t][key(b)] = scaled(glide, inv[b])
    for b in COMPS:
        c, t = [axis for axis in COMPS if axis != b]
        one, two = modes[c][key(c, b)], modes[t][key(t, b)]
        both = (scaled(one, inv[c]) + scaled(two, inv[t])) * LAME
        for comp, mine in ((c, one), (t, two)):
            own = 2.0 * SHEAR * inv[comp] ** 2 + SHEAR * inv[b] ** 2
            out[comp][key(comp, b)] = (scaled(both, inv[comp]) + mine * own) * e_pair
    for c in COMPS:
        b, t = [axis for axis in COMPS if axis != c]
        mine = modes[c][key(b, t)]
        first = scaled(mine, inv[b]) + scaled(modes[b][key(c, t)], inv[c])
        second = scaled(mine, inv[t]) + scaled(modes[t][key(c, b)], inv[c])
        both = scaled(first, inv[b]) + scaled(second, inv[t])
        out[c][key(b, t)] = both * SHEAR * e_pair
    for c in COMPS:
        total = 0.0
        for axis in COMPS:
            total += ((LAME + 2.0 * SHEAR) if axis == c else SHEAR) * inv[axis] ** 2
        out[c][key(0, 1, 2)] = modes[c][key(0, 1, 2)] * total * e_last
    return out


class Plane:
    def __init__(self, count, shift, factor=1):
        self.count, self.shift, self.factor = count, shift, factor

    def __add__(self, other):
        return Plane(self.count, self.shift + other, self.factor)

    def doubled(self, extra):
        return Plane(self.count, 2 * self.shift + extra, 2 * self.factor)

    def index(self, origin=0):
        return self.count * self.factor + (self.shift + origin)


def place(plane, origin):
    return plane.index(origin) if isinstance(plane, Plane) else plane + origin


def twice(plane, extra):
    return plane.doubled(extra) if isinstance(plane, Plane) else 2 * plane + extra


def over(planes, body, group=14):
    count = planes[1] + 1 - planes[0]
    group = max(n for n in range(1, group + 1) if count % n == 0)

    def step(i, _):
        stores = []
        for n in range(group):
            stores += body(Plane(i * group if group > 1 else i, planes[0] + n))
        for ref, index, value in stores:
            ref[index] = value
        return 0

    if group == count:
        stores = [store for n in range(count) for store in body(planes[0] + n)]
        for ref, index, value in stores:
            ref[index] = value
    else:
        lax.fori_loop(0, count // group, step, 0)


ALL = slice(None)


class Level:
    def __init__(self, origin, lengths, split, sums, modulus, inverse, free):
        self.oz, self.oy = origin
        self.lengths = lengths
        self.split, self.sums = split, sums
        self.modulus, self.inverse, self.free = modulus, inverse, free
        entries = diagonal_entries(lengths)
        self.entries = [entries[0]] if lengths[0] == lengths[1] else [entries[0], entries[1]]

    def at(self, plane, row):
        return place(plane, self.oz), pl.ds(row + self.oy, 8)

    def which(self, c):
        return min(c, len(self.entries) - 1)

    def inverse_of(self, c, plane, row):
        p, r = self.at(plane, row)
        return self.inverse[self.which(c), p, r, :]

    def put_split(self, c, plane, row, value):
        p, r = self.at(plane, row)
        after = pltpu.roll(value, LANES - 1, 1)
        return [
            (self.split, (2 * c, p, r, ALL), value + after),
            (self.split, (2 * c + 1, p, r, ALL), after - value),
        ]

    def set_diagonal(self, planes, rows):
        def body(plane):
            stores = []
            for row in rows:
                p, r = self.at(plane, row)
                free = self.free[p, r, :]
                total = self.node_total(plane, row)
                for n, entry in enumerate(self.entries):
                    value = DAMPING / (free * total * entry + (1.0 - free))
                    stores.append((self.inverse, (n, p, r, ALL), value))
            return stores

        over(planes, body)

    def node_total(self, plane, row):
        total = None
        for dz in (-1, 0):
            for dy in (-1, 0):
                p, r = self.at(plane + dz, row + dy)
                piece = self.modulus[p, r, :]
                total = piece if total is None else total + piece
        return total + pltpu.roll(total, 1, 1)

    def voxels(self, planes, rows):
        def pieces(plane, row):
            found = []
            for cm in range(6):
                p, r = self.at(plane, row)
                near = self.split[cm, p, r, :]
                p, r = self.at(plane, row + 1)
                far = self.split[cm, p, r, :]
                found += [near + far, far - near]
            return found

        for row in rows:

            def body(count, carry, row=row):
                plane = Plane(count, planes[0])
                lower, held = carry
                upper = pieces(plane + 1, row)
                p, r = self.at(plane, row)
                modes = []
                for c in COMPS:
                    mine = {}
                    for m in range(2):
                        for iy in range(2):
                            k = (2 * c + m) * 2 + iy
                            if m + iy > 0:
                                mine[(m, iy, 0)] = lower[k] + upper[k]
                            mine[(m, iy, 1)] = upper[k] - lower[k]
                    modes.append(mine)
                forces = element_forces(modes, self.modulus[p, r, :], self.lengths)
                keep = []
                for c in COMPS:
                    for m in range(2):
                        node = []
                        for iy in range(2):
                            k = (2 * c + m) * 2 + iy
                            diff = forces[c][(m, iy, 1)]
                            if m + iy > 0:
                                same = forces[c][(m, iy, 0)]
                                node.append(held[k] + (same - diff))
                                keep.append(same + diff)
                            else:
                                node.append(held[k] - diff)
                                keep.append(diff)
                        self.sums[(2 * c + m) * 2, p, r, :] = node[0] - node[1]
                        self.sums[(2 * c + m) * 2 + 1, p, r, :] = node[0] + node[1]
                return upper, keep

            zero = [jnp.zeros((8, LANES), jnp.float32)] * 12
            carry = (pieces(planes[0], row), zero)
            for count in range(planes[1] + 1 - planes[0]):
                carry = body(count, carry)

    def applied(self, c, plane, row):
        parts = []
        for m in range(2):
            k = (2 * c + m) * 2
            p, r = self.at(plane, row)
            here = self.sums[k, p, r, :]
            p, r = self.at(plane, row - 1)
            parts.append(here + self.sums[k + 1, p, r, :])
        return (parts[0] - parts[1]) + pltpu.roll(parts[0] + parts[1], 1, 1)


NAMES = ("wide", "far", "dir", "fixlow", "low", "mid", "lift")


def messages():
    found = []
    for oz in (0, -1, 1):
        for oy in (0, -1, 1):
            if (oz, oy) != (0, 0):
                found.append(("wide", oz, oy, ("wide", oy), {0: 192, -1: 72, 1: 64}[oy]))
    for oy in (0, -1, 1):
        found.append(("far", -2, oy, ("far", oy), {0: 24, -1: 16, 1: 8}[oy]))
    for oz in (0, -1, 1):
        for oy in (0, -1, 1):
            if (oz, oy) != (0, 0):
                rows = (8 if oy else 40) if oz else 16
                found.append(("dir", oz, oy, ("dir", oz, oy), rows))
    for oz in (0, -1, 1, -2, 2, -3, 3):
        for oy in (0, -1, 1):
            if (oz, oy) != (0, 0):
                found.append(("fixlow", oz, oy, ("fixlow",), 9))
    for oz in (0, -1, 1, -2, 2, -3, 3):
        for oy in (0, -1, 1):
            if (oz, oy) != (0, 0):
                found.append(("low", oz, oy, ("low",), 9))
    for oz in (0, -1, 1):
        for oy in (0, -1, 1):
            if (oz, oy) != (0, 0):
                found.append(("mid", oz, oy, ("mid", oy), 24 if oy else 72))
    for oz in (0, -1, 1, -2, 2):
        for oy in (0, -1, 1):
            if (oz, oy) != (0, 0):
                each = 9 if oy else 18
                part = {-2: 1, 2: 0}.get(oz)
                found.append(("lift", oz, oy, ("lift", oy, part), each if part is not None else 2 * each))
    found.sort(key=lambda m: (NAMES.index(m[0]), -abs(m[1]) - 2 * abs(m[2])))
    return found


def layout():
    sends, receives = {}, {}
    at_send = at_receive = 0
    for oy in (0, -1, 1):
        each = 9 if oy else 18
        sends[("lift", oy, None)] = at_send
        sends[("lift", oy, 0)] = at_send
        sends[("lift", oy, 1)] = at_send + each
        at_send += -(-2 * each // 8) * 8
    for name, oz, oy, key, rows in messages():
        if key not in sends:
            sends[key] = at_send
            at_send += -(-rows // 8) * 8
        receives[(name, oz, oy)] = at_receive
        at_receive += -(-rows // 8) * 8
    return sends, at_send, receives, at_receive


def kernel(
    slab_count,
    pencil_count,
    solution_ref,
    residual_ref,
    direction_ref,
    material_ref,
    next_solution_ref,
    next_residual_ref,
    next_direction_ref,
    sol_in,
    res_in,
    dir_in,
    mat,
    res,
    dirn,
    s0,
    e0,
    old,
    e_fine,
    f_fine,
    i_fine,
    x_fine,
    b_fine,
    s1,
    u1,
    c1,
    e_mid,
    f_mid,
    i_mid,
    x_mid,
    b_mid,
    s2,
    e_low,
    f_low,
    m_low,
    i_low,
    x_low,
    b_low,
    outbox,
    inbox,
    part_out,
    slab_in,
    line_out,
    pencil_in,
    local_sem,
    send_sem,
    recv_sem,
    sum_send,
    sum_recv,
    word_sem,
):
    slab_at, pencil_at = lax.axis_index("slab"), lax.axis_index("pencil")
    sends, _, receives, _ = layout()
    all_messages = messages()
    fine = Level(FINE_O, (1.0, 1.0, 1.0), x_fine, b_fine, e_fine, i_fine, f_fine)
    mid = Level(MID_O, (1.0, 2.0, 2.0), x_mid, b_mid, e_mid, i_mid, f_mid)
    low = Level(LOW_O, (1.0, 4.0, 4.0), x_low, b_low, e_low, i_low, f_low)

    loads = [
        pltpu.make_async_copy(source, target, local_sem.at[n])
        for n, (source, target) in enumerate(
            ((material_ref, mat), (residual_ref, res_in), (direction_ref, dir_in), (solution_ref, sol_in))
        )
    ]
    for load in loads:
        load.start()

    def there(oz, oy):
        z, y = slab_at + oz, pencil_at + oy
        return (z >= 0) & (z < slab_count) & (y >= 0) & (y < pencil_count)

    inbox[...] = jnp.zeros_like(inbox)

    barrier = pltpu.get_barrier_semaphore()
    greeted = jnp.int32(0)
    for oz in range(-REACH, REACH + 1):
        for oy in (-1, 0, 1):
            if (oz, oy) != (0, 0):
                near = there(oz, oy)
                greeted = greeted + jnp.where(near, 1, 0)

                @pl.when(near)
                def _(oz=oz, oy=oy):
                    pl.semaphore_signal(
                        barrier,
                        inc=1,
                        device_id={"slab": slab_at + oz, "pencil": pencil_at + oy},
                        device_id_type=MESH,
                    )

    def stages(count, known):
        steps = []
        while known < count - 1:
            step = min(known, count - 1 - known)
            steps.append(step)
            known += step
        return steps

    plan = [("slab", stages(slab_count, REACH)), ("pencil", stages(pencil_count, 1))]

    def sides(axis, step):
        return [(step * sign if axis == "slab" else 0, step * sign if axis == "pencil" else 0) for sign in (-1, 1)]

    def tell(stage):
        for which, (axis, steps) in enumerate(plan):
            if stage < len(steps):
                for side, (oz, oy) in enumerate(sides(axis, steps[stage])):

                    @pl.when(there(oz, oy))
                    def _(oz=oz, oy=oy):
                        pl.semaphore_signal(
                            word_sem.at[which, stage, 1 - side],
                            inc=1,
                            device_id={"slab": slab_at + oz, "pencil": pencil_at + oy},
                            device_id_type=MESH,
                        )

    def hear(stage):
        for which, (axis, steps) in enumerate(plan):
            if stage < len(steps):
                for side, (oz, oy) in enumerate(sides(axis, steps[stage])):

                    @pl.when(there(oz, oy))
                    def _():
                        pl.semaphore_wait(word_sem.at[which, stage, side], 1)

    for ref in (s0, e_fine, x_fine, b_fine, s1, u1, c1, x_mid, b_mid, s2, e_low, f_low, m_low, i_low, x_low, b_low):
        ref[...] = jnp.zeros_like(ref)
    e_mid[...] = jnp.zeros_like(e_mid)
    f_mid[...] = jnp.zeros_like(f_mid)
    i_mid[...] = jnp.zeros_like(i_mid)
    f_fine[...] = jnp.zeros_like(f_fine)
    i_fine[...] = jnp.zeros_like(i_fine)

    def copy_of(number, oz, oy, key, rows):
        name = all_messages[number][0]
        return pltpu.make_async_remote_copy(
            src_ref=outbox.at[pl.ds(sends[key], rows)],
            dst_ref=inbox.at[pl.ds(receives[(name, oz, oy)], rows)],
            send_sem=send_sem.at[number],
            recv_sem=recv_sem.at[number],
            device_id={"slab": slab_at - oz, "pencil": pencil_at - oy},
            device_id_type=MESH,
        )

    def start(*names):
        for number, (name, oz, oy, key, rows) in enumerate(all_messages):
            if name in names:

                @pl.when(there(-oz, -oy))
                def _(number=number, oz=oz, oy=oy, key=key, rows=rows):
                    copy_of(number, oz, oy, key, rows).start()

    def arrive(*names):
        for number, (name, oz, oy, key, rows) in enumerate(all_messages):
            if name in names:

                @pl.when(there(oz, oy))
                def _(number=number, oz=oz, oy=oy, key=key, rows=rows):
                    copy_of(number, oz, oy, key, rows).wait_recv()

    def arrivals(*names):
        for number, (name, oz, oy, key, rows) in reversed(list(enumerate(all_messages))):
            if name in names:

                @pl.when(there(oz, oy))
                def _(number=number, oz=oz, oy=oy, key=key, rows=rows):
                    copy_of(number, oz, oy, key, rows).wait_recv()

                yield oz, oy, receives[(name, oz, oy)]

    def left(*names):
        for number, (name, oz, oy, key, rows) in enumerate(all_messages):
            if name in names:

                @pl.when(there(-oz, -oy))
                def _(number=number, oz=oz, oy=oy, key=key, rows=rows):
                    copy_of(number, oz, oy, key, rows).wait_send()

    def strided(p, first, count):
        return pl.ds(p + PLANES * first, count, stride=PLANES)

    def planes_first(source, target):
        for c in COMPS:
            for p in range(PLANES):
                for first, count in ((0, 8), (8, 4)):
                    target[c, p, pl.ds(first, count), :] = source[c, strided(p, first, count), :]

    loads[0].wait()
    loads[1].wait()
    planes_first(res_in, res)

    taken_rows = {0: (0, 12), -1: (8, 4), 1: (0, 4)}
    voxel_rows = {0: (0, 12), -1: (6, 6), 1: (0, 4)}
    for oy in (0, -1, 1):
        at = sends[("wide", oy)]
        first, count = taken_rows[oy]
        for c in COMPS:
            for p in range(PLANES):
                outbox[pl.ds(at, count), :] = res[c, p, pl.ds(first, count), :]
                at += count
        first, count = voxel_rows[oy]
        for p in range(PLANES):
            outbox[pl.ds(at, count), :] = (mat[strided(p, first, count), :] == 1).astype(jnp.float32)
            at += count
        at = sends[("far", oy)]
        for p in (2, 3):
            outbox[pl.ds(at, count), :] = (mat[strided(p, first, count), :] == 1).astype(jnp.float32)
            at += count

    pl.semaphore_wait(barrier, greeted)
    start("wide", "far")
    tell(0)

    loads[2].wait()
    loads[3].wait()
    planes_first(dir_in, dirn)
    for name, oz, oy, key, rows in all_messages:
        if name == "dir":
            at = sends[key]
            planes = {0: range(PLANES), -1: (3,), 1: (0,)}[oz]
            first, count = {0: (0, 12), -1: (11, 1), 1: (0, 1)}[oy]
            for c in COMPS:
                for p in planes:
                    outbox[pl.ds(at, count), :] = dirn[c, p, pl.ds(first, count), :]
                    at += count
    start("dir")

    for c in COMPS:
        for p in range(PLANES):
            s0[c, p + FINE_O[0], pl.ds(FINE_O[1], ROWS), :] = res[c, p, pl.ds(0, ROWS), :]
    for p in range(PLANES):
        for first, count in ((0, 8), (8, 4)):
            e_fine[p + FINE_O[0], pl.ds(first + FINE_O[1], count), :] = (mat[strided(p, first, count), :] == 1).astype(
                jnp.float32
            )

    for oz, oy, at in arrivals("wide"):
        first, count = {0: (0, 12), -1: (-4, 4), 1: (12, 4)}[oy]
        for c in COMPS:
            for p in range(PLANES):
                s0[c, p + oz * PLANES + FINE_O[0], pl.ds(first + FINE_O[1], count), :] = inbox[pl.ds(at, count), :]
                at += count
        first, count = {0: (0, 12), -1: (-6, 6), 1: (12, 4)}[oy]
        for p in range(PLANES):
            e_fine[p + oz * PLANES + FINE_O[0], pl.ds(first + FINE_O[1], count), :] = inbox[pl.ds(at, count), :]
            at += count
    hear(0)
    tell(1)
    for _, oy, at in arrivals("far"):
        first, count = {0: (0, 12), -1: (-6, 6), 1: (12, 4)}[oy]
        for p in (-6, -5):
            e_fine[p + FINE_O[0], pl.ds(first + FINE_O[1], count), :] = inbox[pl.ds(at, count), :]
            at += count

    total_planes, total_rows = slab_count * PLANES, pencil_count * ROWS
    row_iota = lax.broadcasted_iota(jnp.int32, (8, LANES), 0)
    lane_iota = lax.broadcasted_iota(jnp.int32, (8, LANES), 1)

    def moduli_body(p):
        plane = slab_at * PLANES + place(p, 0)
        plane_ok = (plane >= 0) & (plane < total_planes - 1)
        stores = []
        for row in (-8, 0, 8):
            ip, ir = fine.at(p, row)
            rows = row_iota + (pencil_at * ROWS + row)
            keep = (rows >= 0) & (rows < total_rows - 1) & (lane_iota < LANES - 1) & plane_ok
            value = jnp.where(e_fine[ip, ir, :] > 0.5, 1.0, VOID_MODULUS)
            stores.append((e_fine, (ip, ir, ALL), jnp.where(keep, value, 0.0)))
        return stores

    over((-6, 7), moduli_body)

    def fine_body(p):
        plane = slab_at * PLANES + place(p, 0)
        inside = (plane > 0) & (plane < total_planes - 1)
        stores = []
        for row in (-5, 3, 8):
            ip, ir = fine.at(p, row)
            total = fine.node_total(p, row)
            free = jnp.where((total > 0.9) & inside, 1.0, 0.0)
            weight = DAMPING / (free * total * fine.entries[0] + (1.0 - free))
            stores += [(f_fine, (ip, ir, ALL), free), (i_fine, (0, ip, ir, ALL), weight)]
        return stores

    over((-5, 7), fine_body)

    def first_update(p):
        stores = []
        for row in (-4, 4, 8):
            ip, ir = fine.at(p, row)
            weight = i_fine[0, ip, ir, :] * f_fine[ip, ir, :]
            for c in COMPS:
                stores += fine.put_split(c, p, row, s0[c, ip, ir, :] * weight)
        return stores

    over((-4, 7), first_update)

    def halves(ref, c, p, row):
        found = []
        for dp in range(2):
            for dr in range(2):
                r = pl.ds(2 * row + dr + FINE_O[1], 8, stride=2)
                ip = place(twice(p, dp), FINE_O[0])
                found.append(ref[ip, r, :] if c is None else ref[c, ip, r, :])
        return found

    def mid_moduli(p):
        plane_ok = slab_at * (PLANES // 2) + place(p, 0) < total_planes // 2 - 1
        stores = []
        for row in (-3, 0):
            ip, ir = mid.at(p, row)
            a, b, c, d = halves(e_fine, None, p, row)
            rows = row_iota + (pencil_at * (ROWS // 2) + row)
            keep = (rows < total_rows // 2 - 1) & plane_ok
            stores.append((e_mid, (ip, ir, ALL), jnp.where(keep, (a + b + c + d) * 0.25, 0.0)))
        return stores

    over((-3, 3), mid_moduli)

    def mid_free(p):
        stores = []
        for row in (-2, 0):
            ip, ir = mid.at(p, row)
            a, b, c, d = halves(f_fine, None, p, row)
            stores.append((f_mid, (ip, ir, ALL), jnp.maximum(jnp.maximum(a, b), jnp.maximum(c, d))))
        return stores

    over((-2, 3), mid_free)
    mid.set_diagonal((-2, 3), (-2, 0))

    def mid_pair(ref, c, p, row):
        found = []
        for dp in range(2):
            for dr in range(2):
                r = pl.ds(2 * row + dr + MID_O[1], 8, stride=2)
                ip = place(twice(p, dp), MID_O[0])
                found.append(ref[ip, r, :] if c is None else ref[c, ip, r, :])
        return found

    for p in (-1, 0):
        ip, ir = low.at(p, -1)
        a, b, c, d = mid_pair(e_mid, None, p, -1)
        rows = row_iota + (pencil_at * (ROWS // 4) - 1)
        keep = (rows < total_rows // 4 - 1) & (slab_at * (PLANES // 4) + p < total_planes // 4 - 1) & (row_iota < 4)
        e_low[ip, ir, :] = jnp.where(keep, (a + b + c + d) * 0.25, 0.0)
    a, b, c, d = mid_pair(f_mid, None, 0, 0)
    ip, ir = low.at(0, 0)
    f_low[ip, ir, :] = jnp.where(row_iota < 3, jnp.maximum(jnp.maximum(a, b), jnp.maximum(c, d)), 0.0)
    m_low[ip, ir, :] = jnp.where(row_iota < 3, low.node_total(0, 0), 0.0)
    at = sends[("fixlow",)]
    own_rows = pl.ds(LOW_O[1], 3)
    for n, ref in enumerate((e_low, f_low, m_low)):
        outbox[pl.ds(at + 3 * n, 3), :] = ref[LOW_O[0], own_rows, :]
    start("fixlow")

    fine.voxels((-4, 6), (-4, 4, 12))

    def fine_step(rows, starting):
        def body(p):
            stores = []
            for row in rows:
                ip, ir = fine.at(p, row)
                free = f_fine[ip, ir, :]
                weight = i_fine[0, ip, ir, :]
                for c in COMPS:
                    remain = s0[c, ip, ir, :]
                    update = weight * remain
                    remain = remain - free * fine.applied(c, p, row) - (1.0 - free) * update
                    stores.append((s0, (c, ip, ir, ALL), remain))
                    if starting:
                        stores += fine.put_split(c, p, row, free * (weight * remain))
            return stores

        return body

    def estimate_add(starting):
        def body(p):
            stores = []
            for row in (0, 8):
                ip, ir = fine.at(p, row)
                weight = i_fine[0, ip, ir, :]
                for c in COMPS:
                    update = weight * s0[c, ip, ir, :]
                    own = (c, place(p, 0), pl.ds(row, 8), ALL)
                    stores.append((e0, own, update if starting else e0[own] + update))
            return stores

        over((0, 3), body)

    estimate_add(True)
    over((-3, 6), fine_step((-3, 5, 13), True))
    estimate_add(False)
    fine.voxels((-3, 5), (-3, 5, 13))
    over((-2, 5), fine_step((-2, 6), False))

    def mid_first(p):
        ip, ir = mid.at(p, -1)
        free = f_mid[ip, ir, :]
        masks = halves(f_fine, None, p, -1)
        stores = []
        for c in COMPS:
            parts = halves(s0, c, p, -1)
            rhs = free * (
                (parts[0] * masks[0] + parts[1] * masks[1]) + (parts[2] * masks[2] + parts[3] * masks[3])
            )
            update = mid.inverse_of(c, p, -1) * rhs
            stores += [(s1, (c, ip, ir, ALL), rhs), (u1, (c, ip, ir, ALL), update)]
            stores += mid.put_split(c, p, -1, free * update)
        return stores

    over((-1, 2), mid_first)
    mid.voxels((-1, 1), (-1,))

    def mid_remain(p):
        ip, ir = mid.at(p, 0)
        free = f_mid[ip, ir, :]
        stores = []
        for c in COMPS:
            remain = s1[c, ip, ir, :] - free * mid.applied(c, p, 0) - (1.0 - free) * u1[c, ip, ir, :]
            stores.append((s1, (c, ip, ir, ALL), remain))
        return stores

    over((0, 1), mid_remain)

    masks = mid_pair(f_mid, None, 0, 0)
    ip, ir = low.at(0, 0)
    free = f_low[ip, ir, :]
    at = sends[("low",)]
    for c in COMPS:
        parts = mid_pair(s1, c, 0, 0)
        rhs = free * ((parts[0] * masks[0] + parts[1] * masks[1]) + (parts[2] * masks[2] + parts[3] * masks[3]))
        rhs = jnp.where(row_iota < 3, rhs, 0.0)
        s2[c, ip, ir, :] = rhs
        outbox[pl.ds(at + 3 * c, 3), :] = rhs[0:3, :]
    start("low")
    mid_rows = {0: (0, 6), -1: (4, 2), 1: (0, 2)}
    for oy in (0, -1, 1):
        at = sends[("mid", oy)]
        first, count = mid_rows[oy]
        for ref in (s1, u1):
            for c in COMPS:
                for p in range(2):
                    outbox[pl.ds(at, count), :] = ref[c, p + MID_O[0], pl.ds(first + MID_O[1], count), :]
                    at += count
    start("mid")

    hear(1)
    tell(2)
    arrive("dir")
    def direction_rows(plane, first, count, c, value):
        ip, ir = plane + FINE_O[0], pl.ds(first + FINE_O[1], count)
        value = value * f_fine[ip, ir, :]
        after = pltpu.roll(value, LANES - 1, 1)
        x_fine[2 * c, ip, ir, :] = value + after
        x_fine[2 * c + 1, ip, ir, :] = after - value

    for oz in (0, -1, 1):
        for oy in (0, -1, 1):
            planes = {0: range(PLANES), -1: (-1,), 1: (PLANES,)}[oz]
            first, count = {0: (0, 12), -1: (-1, 1), 1: (12, 1)}[oy]
            at = None if (oz, oy) == (0, 0) else receives[("dir", oz, oy)]
            for c in COMPS:
                for p in planes:
                    if at is None:
                        direction_rows(p, first, count, c, dirn[c, p, pl.ds(0, ROWS), :])
                    else:
                        direction_rows(p, first, count, c, inbox[pl.ds(at, count), :])
                        at += count
    fine.voxels((-1, 3), (-1, 7))

    def old_image(p):
        stores = []
        for row in (0, 4):
            ip, ir = fine.at(p, row)
            free = f_fine[ip, ir, :]
            for c in COMPS:
                value = dirn[c, place(p, 0), pl.ds(row, 8), :]
                image = free * fine.applied(c, p, row) + (1.0 - free) * value
                stores.append((old, (c, place(p, 0), pl.ds(row, 8), ALL), image))
        return stores

    over((0, 3), old_image)

    def low_window(name, refs):
        for oz, oy, at in arrivals(name):
            for n, ref in enumerate(refs):
                ref[oz + LOW_O[0], pl.ds(3 * oy + LOW_O[1], 3), :] = inbox[pl.ds(at + 3 * n, 3), :]

    low_window("fixlow", (e_low, f_low, m_low))

    def low_inverse(p):
        stores = []
        for row in (-4, 4):
            ip, ir = low.at(p, row)
            free = f_low[ip, ir, :]
            total = m_low[ip, ir, :]
            for n, entry in enumerate(low.entries):
                stores.append((i_low, (n, ip, ir, ALL), DAMPING / (free * total * entry + (1.0 - free))))
        return stores

    over((-3, 3), low_inverse)

    low_window("low", [s2.at[c] for c in COMPS])
    hear(2)
    tell(3)

    def low_split(planes, rows):
        def body(p):
            stores = []
            for row in rows:
                ip, ir = low.at(p, row)
                free = f_low[ip, ir, :]
                for c in COMPS:
                    stores += low.put_split(c, p, row, free * (low.inverse_of(c, p, row) * s2[c, ip, ir, :]))
            return stores

        over(planes, body, 7)

    ip, ir = low.at(0, 0)
    bottom = [low.inverse_of(c, 0, 0) * s2[c, ip, ir, :] for c in COMPS]
    low_split((-3, 3), (-3, 5))
    for depth in (2, 1, 0):
        low.voxels((-1 - depth, depth), (-1 - depth,))

        def low_step(p, depth=depth):
            row = -depth
            ip, ir = low.at(p, row)
            free = f_low[ip, ir, :]
            stores = []
            for c in COMPS:
                remain = s2[c, ip, ir, :]
                update = low.inverse_of(c, p, row) * remain
                remain = remain - free * low.applied(c, p, row) - (1.0 - free) * update
                stores.append((s2, (c, ip, ir, ALL), remain))
                if depth:
                    stores += low.put_split(c, p, row, free * (low.inverse_of(c, p, row) * remain))
            return stores

        over((-depth, depth), low_step, 5)
        ip, ir = low.at(0, 0)
        for c in COMPS:
            bottom[c] = bottom[c] + low.inverse_of(c, 0, 0) * s2[c, ip, ir, :]

    for c in COMPS:
        for p in range(2):
            for dr in range(2):
                c1[c, p + MID_O[0], pl.ds(MID_O[1] + dr, 3, stride=2), :] = bottom[c][0:3, :]
    for c in COMPS:
        for p in range(2):
            ip, ir = p + MID_O[0], pl.ds(MID_O[1], 6)
            c1[c, ip, ir, :] = c1[c, ip, ir, :] * f_mid[ip, ir, :]
    for oy in (0, -1, 1):
        first, count = {0: (0, 6), -1: (3, 3), 1: (0, 3)}[oy]
        for p in range(2):
            at = sends[("lift", oy, p)]
            for c in COMPS:
                outbox[pl.ds(at, count), :] = c1[c, p + MID_O[0], pl.ds(first + MID_O[1], count), :]
                at += count
    start("lift")
    for oz, oy, at in arrivals("mid"):
        first, count = {0: (0, 6), -1: (-2, 2), 1: (6, 2)}[oy]
        for ref in (s1, u1):
            for c in COMPS:
                for p in range(2):
                    ref[c, p + 2 * oz + MID_O[0], pl.ds(first + MID_O[1], count), :] = inbox[pl.ds(at, count), :]
                    at += count
    left("wide", "far", "dir", "fixlow", "low", "mid")
    for oz, oy, base in arrivals("lift"):
        first, count = {0: (0, 6), -1: (-3, 3), 1: (6, 3)}[oy]
        planes = {-2: (-3,), 2: (4,)}.get(oz, (2 * oz, 2 * oz + 1))
        for n, p in enumerate(planes):
            at = base + n * (9 if oy else 18)
            for c in COMPS:
                c1[c, p + MID_O[0], pl.ds(first + MID_O[1], count), :] = inbox[pl.ds(at, count), :]
                at += count

    def lift_split(p):
        stores = []
        for row in (-3, 5):
            ip, ir = mid.at(p, row)
            for c in COMPS:
                stores += mid.put_split(c, p, row, c1[c, ip, ir, :])
        return stores

    over((-3, 4), lift_split)
    mid.voxels((-3, 3), (-3, 5))

    def mid_second(p):
        stores = []
        for row in (-2, 6):
            ip, ir = mid.at(p, row)
            free = f_mid[ip, ir, :]
            for c in COMPS:
                remain = s1[c, ip, ir, :] - free * mid.applied(c, p, row)
                here = (c, ip, ir, ALL)
                stores.append((u1, here, u1[here] + c1[here] + mid.inverse_of(c, p, row) * remain))
        return stores

    over((-2, 3), mid_second)

    def lift_fine(p):
        stores = []
        for row in (-2, 0):
            ip, ir = mid.at(p, row)
            for c in COMPS:
                value = u1[c, ip, ir, :]
                for dp in range(2):
                    for dr in range(2):
                        out = pl.ds(2 * row + dr + FINE_O[1], 8, stride=2)
                        stores.append((x_fine, (2 * c, place(twice(p, dp), FINE_O[0]), out, ALL), value))
        return stores

    over((-2, 3), lift_fine)

    def lift_parts(p):
        stores = []
        for row in (-4, 4, 12):
            ip, ir = fine.at(p, row)
            free = f_fine[ip, ir, :]
            for c in COMPS:
                stores += fine.put_split(c, p, row, free * x_fine[2 * c, ip, ir, :])
        return stores

    def lift_own(p):
        stores = []
        for row in (0, 8):
            ip, ir = fine.at(p, row)
            free = f_fine[ip, ir, :]
            for c in COMPS:
                part = free * x_fine[2 * c, ip, ir, :]
                own = (c, place(p, 0), pl.ds(row, 8), ALL)
                stores.append((e0, own, e0[own] + part))
        return stores

    over((0, 3), lift_own)
    over((-4, 7), lift_parts)
    fine.voxels((-3, 5), (-3, 5, 13))

    def lift_step(p):
        stores = []
        for row in (-2, 6):
            ip, ir = fine.at(p, row)
            free = f_fine[ip, ir, :]
            weight = i_fine[0, ip, ir, :]
            for c in COMPS:
                remain = s0[c, ip, ir, :] - free * fine.applied(c, p, row)
                stores.append((s0, (c, ip, ir, ALL), remain))
                stores += fine.put_split(c, p, row, free * (weight * remain))
        return stores

    over((-2, 5), lift_step)
    estimate_add(False)
    fine.voxels((-2, 4), (-2, 6))
    over((-1, 4), fine_step((-1, 7), True))
    estimate_add(False)
    fine.voxels((-1, 3), (-1, 7))
    over((0, 3), fine_step((0, 8), False))

    def dots(p, totals):
        totals = list(totals)
        for row in (0, 4):
            ip, ir = p + FINE_O[0], pl.ds(row + FINE_O[1], 8)
            keep = None if row == 0 else row_iota >= 4
            for c in COMPS:
                rows = pl.ds(row, 8)
                z, d, o, r = e0[c, p, rows, :], dirn[c, p, rows, :], old[c, p, rows, :], res[c, p, rows, :]
                new = r - s0[c, ip, ir, :]
                for n, term in enumerate((z * o, d * o, z * new, r * z, r * d)):
                    totals[n] = totals[n] + (term if keep is None else jnp.where(keep, term, 0.0))
        return tuple(totals)

    totals = lax.fori_loop(0, PLANES, dots, (jnp.zeros((8, LANES), jnp.float32),) * 5)
    for n, total in enumerate(totals):
        part_out[pl.ds(n, 1), :] = jnp.sum(total, axis=0, keepdims=True)

    def share(axis, at, count, source, target, which, meanwhile):
        def copy(k):
            return pltpu.make_async_remote_copy(
                src_ref=source,
                dst_ref=target.at[k],
                send_sem=sum_send.at[which, k],
                recv_sem=sum_recv.at[which, k],
                device_id={axis: lax.rem(at + k, count)},
                device_id_type=MESH,
            )

        for k in order(count):
            copy(k).start()
        meanwhile()
        for k in range(1, count):
            copy(k).wait_recv()
        parts = [source[...]] + [target[k] for k in range(1, count)]
        while len(parts) > 1:
            parts = [a + b for a, b in zip(parts[::2], parts[1::2])] + parts[len(parts) // 2 * 2 :]
        return parts[0], copy

    def order(count):
        return sorted(range(1, count), key=lambda k: -min(k, count - k))

    def settle():
        left("lift")
        for stage in range(3, STAGES):
            if stage > 3:
                tell(stage)
            hear(stage)

    def settle_slab():
        for k in range(1, slab_count):
            slab_copy(k).wait_send()

    line, slab_copy = share("slab", slab_at, slab_count, part_out, slab_in, 0, settle)
    line_out[...] = line
    whole, pencil_copy = share("pencil", pencil_at, pencil_count, line_out, pencil_in, 1, settle_slab)
    summed = jnp.sum(whole, axis=1, keepdims=True)
    t = [summed[n : n + 1, :] for n in range(5)]
    beta = -t[0] / t[1]
    along = t[3] + beta * t[4]
    curvature = t[2] + 2.0 * beta * t[0] + beta * beta * t[1]
    step = along / curvature

    for c in COMPS:
        for p in range(PLANES):
            for first, count in ((0, 8), (8, 4)):
                rows, there_rows = pl.ds(first, count), strided(p, first, count)
                z, d, o, r = e0[c, p, rows, :], dirn[c, p, rows, :], old[c, p, rows, :], res[c, p, rows, :]
                new = r - s0[c, p + FINE_O[0], pl.ds(first + FINE_O[1], count), :]
                nd = z + beta * d
                image = new + beta * o
                next_direction_ref[c, there_rows, :] = nd
                next_solution_ref[c, there_rows, :] = sol_in[c, there_rows, :] + step * nd
                next_residual_ref[c, there_rows, :] = r - step * image
    for k in range(1, pencil_count):
        pencil_copy(k).wait_send()


def per_device(slab_count, pencil_count, solution, residual, direction, material, fixed):
    del fixed
    _, send_rows, _, receive_rows = layout()
    count = len(messages())
    f32 = jnp.float32
    flat = (3, ROWS * PLANES, LANES)
    padded = (3, PLANES, 16, LANES)

    def vmem(*shape):
        return pltpu.VMEM(shape, f32)

    def window(size):
        planes, rows = size
        return planes, rows, LANES

    hbm = pl.BlockSpec(memory_space=pl.ANY)
    out = jax.ShapeDtypeStruct(flat, f32)
    results = pl.pallas_call(
        functools.partial(kernel, slab_count, pencil_count),
        out_shape=(out, out, out),
        in_specs=[hbm] * 4,
        out_specs=(pl.BlockSpec(memory_space=pltpu.VMEM),) * 3,
        scratch_shapes=[
            vmem(*flat),
            vmem(*flat),
            vmem(*flat),
            pltpu.VMEM(flat[1:], jnp.int32),
            vmem(*padded),
            vmem(*padded),
            vmem(3, *window(FINE_S)),
            vmem(*padded),
            vmem(*padded),
            vmem(*window(FINE_S)),
            vmem(*window(FINE_S)),
            vmem(1, *window(FINE_S)),
            vmem(6, *window(FINE_S)),
            vmem(12, *window(FINE_S)),
            vmem(3, *window(MID_S)),
            vmem(3, *window(MID_S)),
            vmem(3, *window(MID_S)),
            vmem(*window(MID_S)),
            vmem(*window(MID_S)),
            vmem(2, *window(MID_S)),
            vmem(6, *window(MID_S)),
            vmem(12, *window(MID_S)),
            vmem(3, *window(LOW_S)),
            vmem(*window(LOW_S)),
            vmem(*window(LOW_S)),
            vmem(*window(LOW_S)),
            vmem(2, *window(LOW_S)),
            vmem(6, *window(LOW_S)),
            vmem(12, *window(LOW_S)),
            vmem(send_rows, LANES),
            vmem(receive_rows, LANES),
            vmem(8, LANES),
            vmem(slab_count, 8, LANES),
            vmem(8, LANES),
            vmem(pencil_count, 8, LANES),
            pltpu.SemaphoreType.DMA((4,)),
            pltpu.SemaphoreType.DMA((count,)),
            pltpu.SemaphoreType.DMA((count,)),
            pltpu.SemaphoreType.DMA((2, max(slab_count, pencil_count))),
            pltpu.SemaphoreType.DMA((2, max(slab_count, pencil_count))),
            pltpu.SemaphoreType.REGULAR((2, STAGES, 2)),
        ],
        compiler_params=pltpu.CompilerParams(collective_id=0, has_side_effects=True, vmem_limit_bytes=24 * 1024 * 1024),
    )(*(pltpu.with_memory_space_constraint(inward(field), pltpu.HBM) for field in (solution, residual, direction, material)))
    return tuple(outward(field) for field in results)


def inward(field):
    axes = (0, 2, 1, 3) if field.ndim == 4 else (1, 0, 2)
    return field.transpose(axes).reshape(field.shape[:-3] + (ROWS * PLANES, LANES))


def outward(field):
    return field.reshape(3, ROWS, PLANES, LANES).transpose(0, 2, 1, 3)


def solution(mesh):
    field = P(None, "slab", "pencil", "parts")
    mask = P("slab", "pencil", "parts")
    return jax.shard_map(
        functools.partial(per_device, mesh.shape["slab"], mesh.shape["pencil"]),
        mesh=mesh,
        in_specs=(field, field, field, mask, mask),
        out_specs=(field, field, field),
        check_vma=False,
    )
```

```python
import functools

import jax
import jax.numpy as jnp
import numpy as np
from jax import lax
from jax.experimental import pallas as pl
from jax.experimental.pallas import tpu as pltpu
from jax.sharding import PartitionSpec as P

SWEEPS = 4
POISSON = 0.3
VOID_MODULUS = 0.1
DAMPING = 0.6
LAME = POISSON / ((1.0 + POISSON) * (1.0 - 2.0 * POISSON))
SHEAR = 0.5 / (1.0 + POISSON)
LANES = 128
COMPS = range(3)
MESH = pl.DeviceIdType.MESH

PLANES, ROWS = 4, 12
REACH, STAGES = 2, 6
FINE_O, FINE_S = (6, 8), (14, 32)
MID_O, MID_S = (3, 4), (8, 24)
LOW_O, LOW_S = (3, 4), (7, 24)


def diagonal_entries(lengths):
    volume = lengths[0] * lengths[1] * lengths[2]
    entries = []
    for c in COMPS:
        total = 0.0
        for axis in COMPS:
            weight = (LAME + 2.0 * SHEAR) if axis == c else SHEAR
            total += weight / lengths[axis] ** 2 / 9.0
        entries.append(total * volume)
    return entries


def scaled(value, factor):
    return value if factor == 1.0 else value * factor


def element_forces(modes, modulus, lengths):
    volume = lengths[0] * lengths[1] * lengths[2]
    inv = [1.0 / length for length in lengths]

    def key(*axes):
        return tuple(1 if axis in axes else 0 for axis in COMPS)

    out = [dict() for _ in COMPS]
    e_norm = modulus * (volume / 16.0)
    e_pair = modulus * (volume / 48.0)
    e_last = modulus * (volume / 144.0)
    stretch = [scaled(modes[c][key(c)], inv[c]) for c in COMPS]
    trace = (stretch[0] + stretch[1] + stretch[2]) * LAME
    for c in COMPS:
        out[c][key(c)] = scaled(trace + stretch[c] * (2.0 * SHEAR), inv[c]) * e_norm
    for b, t in ((0, 1), (0, 2), (1, 2)):
        glide = (scaled(modes[b][key(t)], inv[t]) + scaled(modes[t][key(b)], inv[b])) * SHEAR
        glide = glide * e_norm
        out[b][key(t)] = scaled(glide, inv[t])
        out[t][key(b)] = scaled(glide, inv[b])
    for b in COMPS:
        c, t = [axis for axis in COMPS if axis != b]
        one, two = modes[c][key(c, b)], modes[t][key(t, b)]
        both = (scaled(one, inv[c]) + scaled(two, inv[t])) * LAME
        for comp, mine in ((c, one), (t, two)):
            own = 2.0 * SHEAR * inv[comp] ** 2 + SHEAR * inv[b] ** 2
            out[comp][key(comp, b)] = (scaled(both, inv[comp]) + mine * own) * e_pair
    for c in COMPS:
        b, t = [axis for axis in COMPS if axis != c]
        mine = modes[c][key(b, t)]
        first = scaled(mine, inv[b]) + scaled(modes[b][key(c, t)], inv[c])
        second = scaled(mine, inv[t]) + scaled(modes[t][key(c, b)], inv[c])
        both = scaled(first, inv[b]) + scaled(second, inv[t])
        out[c][key(b, t)] = both * SHEAR * e_pair
    for c in COMPS:
        total = 0.0
        for axis in COMPS:
            total += ((LAME + 2.0 * SHEAR) if axis == c else SHEAR) * inv[axis] ** 2
        out[c][key(0, 1, 2)] = modes[c][key(0, 1, 2)] * total * e_last
    return out


class Plane:
    def __init__(self, count, shift, factor=1):
        self.count, self.shift, self.factor = count, shift, factor

    def __add__(self, other):
        return Plane(self.count, self.shift + other, self.factor)

    def doubled(self, extra):
        return Plane(self.count, 2 * self.shift + extra, 2 * self.factor)

    def index(self, origin=0):
        return self.count * self.factor + (self.shift + origin)


def place(plane, origin):
    return plane.index(origin) if isinstance(plane, Plane) else plane + origin


def twice(plane, extra):
    return plane.doubled(extra) if isinstance(plane, Plane) else 2 * plane + extra


def over(planes, body, group=14):
    count = planes[1] + 1 - planes[0]
    group = max(n for n in range(1, group + 1) if count % n == 0)

    def step(i, _):
        stores = []
        for n in range(group):
            stores += body(Plane(i * group if group > 1 else i, planes[0] + n))
        for ref, index, value in stores:
            ref[index] = value
        return 0

    if group == count:
        stores = [store for n in range(count) for store in body(planes[0] + n)]
        for ref, index, value in stores:
            ref[index] = value
    else:
        lax.fori_loop(0, count // group, step, 0)


ALL = slice(None)


class Level:
    def __init__(self, origin, lengths, split, sums, modulus, inverse, free):
        self.oz, self.oy = origin
        self.lengths = lengths
        self.split, self.sums = split, sums
        self.modulus, self.inverse, self.free = modulus, inverse, free
        entries = diagonal_entries(lengths)
        self.entries = [entries[0]] if lengths[0] == lengths[1] else [entries[0], entries[1]]

    def at(self, plane, row):
        return place(plane, self.oz), pl.ds(row + self.oy, 8)

    def which(self, c):
        return min(c, len(self.entries) - 1)

    def inverse_of(self, c, plane, row):
        p, r = self.at(plane, row)
        return self.inverse[self.which(c), p, r, :]

    def put_split(self, c, plane, row, value):
        p, r = self.at(plane, row)
        after = pltpu.roll(value, LANES - 1, 1)
        return [
            (self.split, (2 * c, p, r, ALL), value + after),
            (self.split, (2 * c + 1, p, r, ALL), after - value),
        ]

    def set_diagonal(self, planes, rows):
        def body(plane):
            stores = []
            for row in rows:
                p, r = self.at(plane, row)
                free = self.free[p, r, :]
                total = self.node_total(plane, row)
                for n, entry in enumerate(self.entries):
                    value = DAMPING / (free * total * entry + (1.0 - free))
                    stores.append((self.inverse, (n, p, r, ALL), value))
            return stores

        over(planes, body)

    def node_total(self, plane, row):
        total = None
        for dz in (-1, 0):
            for dy in (-1, 0):
                p, r = self.at(plane + dz, row + dy)
                piece = self.modulus[p, r, :]
                total = piece if total is None else total + piece
        return total + pltpu.roll(total, 1, 1)

    def voxels(self, planes, rows):
        def pieces(plane, row):
            found = []
            for cm in range(6):
                p, r = self.at(plane, row)
                near = self.split[cm, p, r, :]
                p, r = self.at(plane, row + 1)
                far = self.split[cm, p, r, :]
                found += [near + far, far - near]
            return found

        for row in rows:

            def body(count, carry, row=row):
                plane = Plane(count, planes[0])
                lower, held = carry
                upper = pieces(plane + 1, row)
                p, r = self.at(plane, row)
                modes = []
                for c in COMPS:
                    mine = {}
                    for m in range(2):
                        for iy in range(2):
                            k = (2 * c + m) * 2 + iy
                            if m + iy > 0:
                                mine[(m, iy, 0)] = lower[k] + upper[k]
                            mine[(m, iy, 1)] = upper[k] - lower[k]
                    modes.append(mine)
                forces = element_forces(modes, self.modulus[p, r, :], self.lengths)
                keep = []
                for c in COMPS:
                    for m in range(2):
                        node = []
                        for iy in range(2):
                            k = (2 * c + m) * 2 + iy
                            diff = forces[c][(m, iy, 1)]
                            if m + iy > 0:
                                same = forces[c][(m, iy, 0)]
                                node.append(held[k] + (same - diff))
                                keep.append(same + diff)
                            else:
                                node.append(held[k] - diff)
                                keep.append(diff)
                        self.sums[(2 * c + m) * 2, p, r, :] = node[0] - node[1]
                        self.sums[(2 * c + m) * 2 + 1, p, r, :] = node[0] + node[1]
                return upper, keep

            zero = [jnp.zeros((8, LANES), jnp.float32)] * 12
            carry = (pieces(planes[0], row), zero)
            for count in range(planes[1] + 1 - planes[0]):
                carry = body(count, carry)

    def applied(self, c, plane, row):
        parts = []
        for m in range(2):
            k = (2 * c + m) * 2
            p, r = self.at(plane, row)
            here = self.sums[k, p, r, :]
            p, r = self.at(plane, row - 1)
            parts.append(here + self.sums[k + 1, p, r, :])
        return (parts[0] - parts[1]) + pltpu.roll(parts[0] + parts[1], 1, 1)


NAMES = ("wide", "far", "dir", "fixlow", "low", "mid", "lift")


def messages():
    found = []
    for oz in (0, -1, 1):
        for oy in (0, -1, 1):
            if (oz, oy) != (0, 0):
                found.append(("wide", oz, oy, ("wide", oy), {0: 192, -1: 72, 1: 64}[oy]))
    for oy in (0, -1, 1):
        found.append(("far", -2, oy, ("far", oy), {0: 24, -1: 16, 1: 8}[oy]))
    for oz in (0, -1, 1):
        for oy in (0, -1, 1):
            if (oz, oy) != (0, 0):
                rows = (8 if oy else 40) if oz else 16
                found.append(("dir", oz, oy, ("dir", oz, oy), rows))
    for oz in (0, -1, 1, -2, 2, -3, 3):
        for oy in (0, -1, 1):
            if (oz, oy) != (0, 0):
                found.append(("fixlow", oz, oy, ("fixlow",), 9))
    for oz in (0, -1, 1, -2, 2, -3, 3):
        for oy in (0, -1, 1):
            if (oz, oy) != (0, 0):
                found.append(("low", oz, oy, ("low",), 9))
    for oz in (0, -1, 1):
        for oy in (0, -1, 1):
            if (oz, oy) != (0, 0):
                found.append(("mid", oz, oy, ("mid", oy), 24 if oy else 72))
    for oz in (0, -1, 1, -2, 2):
        for oy in (0, -1, 1):
            if (oz, oy) != (0, 0):
                each = 9 if oy else 18
                part = {-2: 1, 2: 0}.get(oz)
                found.append(("lift", oz, oy, ("lift", oy, part), each if part is not None else 2 * each))
    found.sort(key=lambda m: (NAMES.index(m[0]), -abs(m[1]) - 2 * abs(m[2])))
    return found


def layout():
    sends, receives = {}, {}
    at_send = at_receive = 0
    for oy in (0, -1, 1):
        each = 9 if oy else 18
        sends[("lift", oy, None)] = at_send
        sends[("lift", oy, 0)] = at_send
        sends[("lift", oy, 1)] = at_send + each
        at_send += -(-2 * each // 8) * 8
    for name, oz, oy, key, rows in messages():
        if key not in sends:
            sends[key] = at_send
            at_send += -(-rows // 8) * 8
        receives[(name, oz, oy)] = at_receive
        at_receive += -(-rows // 8) * 8
    return sends, at_send, receives, at_receive


def kernel(
    slab_count,
    pencil_count,
    solution_ref,
    residual_ref,
    direction_ref,
    material_ref,
    next_solution_ref,
    next_residual_ref,
    next_direction_ref,
    sol_in,
    res_in,
    dir_in,
    mat,
    res,
    dirn,
    s0,
    e0,
    old,
    e_fine,
    f_fine,
    i_fine,
    x_fine,
    b_fine,
    s1,
    u1,
    c1,
    e_mid,
    f_mid,
    i_mid,
    x_mid,
    b_mid,
    s2,
    e_low,
    f_low,
    m_low,
    i_low,
    x_low,
    b_low,
    outbox,
    inbox,
    slab_in,
    pencil_in,
    local_sem,
    send_sem,
    recv_sem,
    sum_send,
    sum_recv,
    word_sem,
):
    slab_at, pencil_at = lax.axis_index("slab"), lax.axis_index("pencil")
    sends, _, receives, _ = layout()
    all_messages = messages()
    fine = Level(FINE_O, (1.0, 1.0, 1.0), x_fine, b_fine, e_fine, i_fine, f_fine)
    mid = Level(MID_O, (1.0, 2.0, 2.0), x_mid, b_mid, e_mid, i_mid, f_mid)
    low = Level(LOW_O, (1.0, 4.0, 4.0), x_low, b_low, e_low, i_low, f_low)

    loads = [
        pltpu.make_async_copy(source, target, local_sem.at[n])
        for n, (source, target) in enumerate(
            ((material_ref, mat), (residual_ref, res_in), (direction_ref, dir_in), (solution_ref, sol_in))
        )
    ]
    for load in loads:
        load.start()

    def there(oz, oy):
        z, y = slab_at + oz, pencil_at + oy
        return (z >= 0) & (z < slab_count) & (y >= 0) & (y < pencil_count)

    inbox[...] = jnp.zeros_like(inbox)

    barrier = pltpu.get_barrier_semaphore()
    greeted = jnp.int32(0)
    for oz in range(-REACH, REACH + 1):
        for oy in (-1, 0, 1):
            if (oz, oy) != (0, 0):
                near = there(oz, oy)
                greeted = greeted + jnp.where(near, 1, 0)

                @pl.when(near)
                def _(oz=oz, oy=oy):
                    pl.semaphore_signal(
                        barrier,
                        inc=1,
                        device_id={"slab": slab_at + oz, "pencil": pencil_at + oy},
                        device_id_type=MESH,
                    )

    def stages(count, known):
        steps = []
        while known < count - 1:
            step = min(known, count - 1 - known)
            steps.append(step)
            known += step
        return steps

    plan = [("slab", stages(slab_count, REACH)), ("pencil", stages(pencil_count, 1))]

    def sides(axis, step):
        return [(step * sign if axis == "slab" else 0, step * sign if axis == "pencil" else 0) for sign in (-1, 1)]

    def tell(stage):
        for which, (axis, steps) in enumerate(plan):
            if stage < len(steps):
                for side, (oz, oy) in enumerate(sides(axis, steps[stage])):

                    @pl.when(there(oz, oy))
                    def _(oz=oz, oy=oy):
                        pl.semaphore_signal(
                            word_sem.at[which, stage, 1 - side],
                            inc=1,
                            device_id={"slab": slab_at + oz, "pencil": pencil_at + oy},
                            device_id_type=MESH,
                        )

    def hear(stage):
        for which, (axis, steps) in enumerate(plan):
            if stage < len(steps):
                for side, (oz, oy) in enumerate(sides(axis, steps[stage])):

                    @pl.when(there(oz, oy))
                    def _():
                        pl.semaphore_wait(word_sem.at[which, stage, side], 1)

    for ref in (s0, e_fine, x_fine, b_fine, s1, u1, c1, x_mid, b_mid, s2, e_low, f_low, m_low, i_low, x_low, b_low):
        ref[...] = jnp.zeros_like(ref)
    e_mid[...] = jnp.zeros_like(e_mid)
    f_mid[...] = jnp.zeros_like(f_mid)
    i_mid[...] = jnp.zeros_like(i_mid)
    f_fine[...] = jnp.zeros_like(f_fine)
    i_fine[...] = jnp.zeros_like(i_fine)

    def copy_of(number, oz, oy, key, rows):
        name = all_messages[number][0]
        return pltpu.make_async_remote_copy(
            src_ref=outbox.at[pl.ds(sends[key], rows)],
            dst_ref=inbox.at[pl.ds(receives[(name, oz, oy)], rows)],
            send_sem=send_sem.at[number],
            recv_sem=recv_sem.at[number],
            device_id={"slab": slab_at - oz, "pencil": pencil_at - oy},
            device_id_type=MESH,
        )

    def start(*names):
        for number, (name, oz, oy, key, rows) in enumerate(all_messages):
            if name in names:

                @pl.when(there(-oz, -oy))
                def _(number=number, oz=oz, oy=oy, key=key, rows=rows):
                    copy_of(number, oz, oy, key, rows).start()

    def arrive(*names):
        for number, (name, oz, oy, key, rows) in enumerate(all_messages):
            if name in names:

                @pl.when(there(oz, oy))
                def _(number=number, oz=oz, oy=oy, key=key, rows=rows):
                    copy_of(number, oz, oy, key, rows).wait_recv()

    def arrivals(*names):
        for number, (name, oz, oy, key, rows) in reversed(list(enumerate(all_messages))):
            if name in names:

                @pl.when(there(oz, oy))
                def _(number=number, oz=oz, oy=oy, key=key, rows=rows):
                    copy_of(number, oz, oy, key, rows).wait_recv()

                yield oz, oy, receives[(name, oz, oy)]

    def left(*names):
        for number, (name, oz, oy, key, rows) in enumerate(all_messages):
            if name in names:

                @pl.when(there(-oz, -oy))
                def _(number=number, oz=oz, oy=oy, key=key, rows=rows):
                    copy_of(number, oz, oy, key, rows).wait_send()

    def strided(p, first, count):
        return pl.ds(p + PLANES * first, count, stride=PLANES)

    def planes_first(source, target):
        for c in COMPS:
            for p in range(PLANES):
                for first, count in ((0, 8), (8, 4)):
                    target[c, p, pl.ds(first, count), :] = source[c, strided(p, first, count), :]

    loads[0].wait()
    loads[1].wait()
    planes_first(res_in, res)

    taken_rows = {0: (0, 12), -1: (8, 4), 1: (0, 4)}
    voxel_rows = {0: (0, 12), -1: (6, 6), 1: (0, 4)}
    for oy in (0, -1, 1):
        at = sends[("wide", oy)]
        first, count = taken_rows[oy]
        for c in COMPS:
            for p in range(PLANES):
                outbox[pl.ds(at, count), :] = res[c, p, pl.ds(first, count), :]
                at += count
        first, count = voxel_rows[oy]
        for p in range(PLANES):
            outbox[pl.ds(at, count), :] = (mat[strided(p, first, count), :] == 1).astype(jnp.float32)
            at += count
        at = sends[("far", oy)]
        for p in (2, 3):
            outbox[pl.ds(at, count), :] = (mat[strided(p, first, count), :] == 1).astype(jnp.float32)
            at += count

    pl.semaphore_wait(barrier, greeted)
    start("wide", "far")
    tell(0)

    loads[2].wait()
    loads[3].wait()
    planes_first(dir_in, dirn)
    for name, oz, oy, key, rows in all_messages:
        if name == "dir":
            at = sends[key]
            planes = {0: range(PLANES), -1: (3,), 1: (0,)}[oz]
            first, count = {0: (0, 12), -1: (11, 1), 1: (0, 1)}[oy]
            for c in COMPS:
                for p in planes:
                    outbox[pl.ds(at, count), :] = dirn[c, p, pl.ds(first, count), :]
                    at += count
    start("dir")

    for c in COMPS:
        for p in range(PLANES):
            s0[c, p + FINE_O[0], pl.ds(FINE_O[1], ROWS), :] = res[c, p, pl.ds(0, ROWS), :]
    for p in range(PLANES):
        for first, count in ((0, 8), (8, 4)):
            e_fine[p + FINE_O[0], pl.ds(first + FINE_O[1], count), :] = (mat[strided(p, first, count), :] == 1).astype(
                jnp.float32
            )

    for oz, oy, at in arrivals("wide"):
        first, count = {0: (0, 12), -1: (-4, 4), 1: (12, 4)}[oy]
        for c in COMPS:
            for p in range(PLANES):
                s0[c, p + oz * PLANES + FINE_O[0], pl.ds(first + FINE_O[1], count), :] = inbox[pl.ds(at, count), :]
                at += count
        first, count = {0: (0, 12), -1: (-6, 6), 1: (12, 4)}[oy]
        for p in range(PLANES):
            e_fine[p + oz * PLANES + FINE_O[0], pl.ds(first + FINE_O[1], count), :] = inbox[pl.ds(at, count), :]
            at += count
    hear(0)
    tell(1)
    for _, oy, at in arrivals("far"):
        first, count = {0: (0, 12), -1: (-6, 6), 1: (12, 4)}[oy]
        for p in (-6, -5):
            e_fine[p + FINE_O[0], pl.ds(first + FINE_O[1], count), :] = inbox[pl.ds(at, count), :]
            at += count

    total_planes, total_rows = slab_count * PLANES, pencil_count * ROWS
    row_iota = lax.broadcasted_iota(jnp.int32, (8, LANES), 0)
    lane_iota = lax.broadcasted_iota(jnp.int32, (8, LANES), 1)

    def moduli_body(p):
        plane = slab_at * PLANES + place(p, 0)
        plane_ok = (plane >= 0) & (plane < total_planes - 1)
        stores = []
        for row in (-8, 0, 8):
            ip, ir = fine.at(p, row)
            rows = row_iota + (pencil_at * ROWS + row)
            keep = (rows >= 0) & (rows < total_rows - 1) & (lane_iota < LANES - 1) & plane_ok
            value = jnp.where(e_fine[ip, ir, :] > 0.5, 1.0, VOID_MODULUS)
            stores.append((e_fine, (ip, ir, ALL), jnp.where(keep, value, 0.0)))
        return stores

    over((-6, 7), moduli_body)

    def fine_body(p):
        plane = slab_at * PLANES + place(p, 0)
        inside = (plane > 0) & (plane < total_planes - 1)
        stores = []
        for row in (-5, 3, 8):
            ip, ir = fine.at(p, row)
            total = fine.node_total(p, row)
            free = jnp.where((total > 0.9) & inside, 1.0, 0.0)
            weight = DAMPING / (free * total * fine.entries[0] + (1.0 - free))
            stores += [(f_fine, (ip, ir, ALL), free), (i_fine, (0, ip, ir, ALL), weight)]
        return stores

    over((-5, 7), fine_body)

    def first_update(p):
        stores = []
        for row in (-4, 4, 8):
            ip, ir = fine.at(p, row)
            weight = i_fine[0, ip, ir, :] * f_fine[ip, ir, :]
            for c in COMPS:
                stores += fine.put_split(c, p, row, s0[c, ip, ir, :] * weight)
        return stores

    over((-4, 7), first_update)

    def halves(ref, c, p, row):
        found = []
        for dp in range(2):
            for dr in range(2):
                r = pl.ds(2 * row + dr + FINE_O[1], 8, stride=2)
                ip = place(twice(p, dp), FINE_O[0])
                found.append(ref[ip, r, :] if c is None else ref[c, ip, r, :])
        return found

    def mid_moduli(p):
        plane_ok = slab_at * (PLANES // 2) + place(p, 0) < total_planes // 2 - 1
        stores = []
        for row in (-3, 0):
            ip, ir = mid.at(p, row)
            a, b, c, d = halves(e_fine, None, p, row)
            rows = row_iota + (pencil_at * (ROWS // 2) + row)
            keep = (rows < total_rows // 2 - 1) & plane_ok
            stores.append((e_mid, (ip, ir, ALL), jnp.where(keep, (a + b + c + d) * 0.25, 0.0)))
        return stores

    over((-3, 3), mid_moduli)

    def mid_free(p):
        stores = []
        for row in (-2, 0):
            ip, ir = mid.at(p, row)
            a, b, c, d = halves(f_fine, None, p, row)
            stores.append((f_mid, (ip, ir, ALL), jnp.maximum(jnp.maximum(a, b), jnp.maximum(c, d))))
        return stores

    over((-2, 3), mid_free)
    mid.set_diagonal((-2, 3), (-2, 0))

    def mid_pair(ref, c, p, row):
        found = []
        for dp in range(2):
            for dr in range(2):
                r = pl.ds(2 * row + dr + MID_O[1], 8, stride=2)
                ip = place(twice(p, dp), MID_O[0])
                found.append(ref[ip, r, :] if c is None else ref[c, ip, r, :])
        return found

    for p in (-1, 0):
        ip, ir = low.at(p, -1)
        a, b, c, d = mid_pair(e_mid, None, p, -1)
        rows = row_iota + (pencil_at * (ROWS // 4) - 1)
        keep = (rows < total_rows // 4 - 1) & (slab_at * (PLANES // 4) + p < total_planes // 4 - 1) & (row_iota < 4)
        e_low[ip, ir, :] = jnp.where(keep, (a + b + c + d) * 0.25, 0.0)
    a, b, c, d = mid_pair(f_mid, None, 0, 0)
    ip, ir = low.at(0, 0)
    f_low[ip, ir, :] = jnp.where(row_iota < 3, jnp.maximum(jnp.maximum(a, b), jnp.maximum(c, d)), 0.0)
    m_low[ip, ir, :] = jnp.where(row_iota < 3, low.node_total(0, 0), 0.0)
    at = sends[("fixlow",)]
    own_rows = pl.ds(LOW_O[1], 3)
    for n, ref in enumerate((e_low, f_low, m_low)):
        outbox[pl.ds(at + 3 * n, 3), :] = ref[LOW_O[0], own_rows, :]
    start("fixlow")

    fine.voxels((-4, 6), (-4, 4, 12))

    def fine_step(rows, starting):
        def body(p):
            stores = []
            for row in rows:
                ip, ir = fine.at(p, row)
                free = f_fine[ip, ir, :]
                weight = i_fine[0, ip, ir, :]
                for c in COMPS:
                    remain = s0[c, ip, ir, :]
                    update = weight * remain
                    remain = remain - free * fine.applied(c, p, row) - (1.0 - free) * update
                    stores.append((s0, (c, ip, ir, ALL), remain))
                    if starting:
                        stores += fine.put_split(c, p, row, free * (weight * remain))
            return stores

        return body

    def estimate_add(starting):
        def body(p):
            stores = []
            for row in (0, 8):
                ip, ir = fine.at(p, row)
                weight = i_fine[0, ip, ir, :]
                for c in COMPS:
                    update = weight * s0[c, ip, ir, :]
                    own = (c, place(p, 0), pl.ds(row, 8), ALL)
                    stores.append((e0, own, update if starting else e0[own] + update))
            return stores

        over((0, 3), body)

    estimate_add(True)
    over((-3, 6), fine_step((-3, 5, 13), True))
    estimate_add(False)
    fine.voxels((-3, 5), (-3, 5, 13))
    over((-2, 5), fine_step((-2, 6), False))

    def mid_first(p):
        ip, ir = mid.at(p, -1)
        free = f_mid[ip, ir, :]
        masks = halves(f_fine, None, p, -1)
        stores = []
        for c in COMPS:
            parts = halves(s0, c, p, -1)
            rhs = free * (
                (parts[0] * masks[0] + parts[1] * masks[1]) + (parts[2] * masks[2] + parts[3] * masks[3])
            )
            update = mid.inverse_of(c, p, -1) * rhs
            stores += [(s1, (c, ip, ir, ALL), rhs), (u1, (c, ip, ir, ALL), update)]
            stores += mid.put_split(c, p, -1, free * update)
        return stores

    over((-1, 2), mid_first)
    mid.voxels((-1, 1), (-1,))

    def mid_remain(p):
        ip, ir = mid.at(p, 0)
        free = f_mid[ip, ir, :]
        stores = []
        for c in COMPS:
            remain = s1[c, ip, ir, :] - free * mid.applied(c, p, 0) - (1.0 - free) * u1[c, ip, ir, :]
            stores.append((s1, (c, ip, ir, ALL), remain))
        return stores

    over((0, 1), mid_remain)

    masks = mid_pair(f_mid, None, 0, 0)
    ip, ir = low.at(0, 0)
    free = f_low[ip, ir, :]
    at = sends[("low",)]
    for c in COMPS:
        parts = mid_pair(s1, c, 0, 0)
        rhs = free * ((parts[0] * masks[0] + parts[1] * masks[1]) + (parts[2] * masks[2] + parts[3] * masks[3]))
        rhs = jnp.where(row_iota < 3, rhs, 0.0)
        s2[c, ip, ir, :] = rhs
        outbox[pl.ds(at + 3 * c, 3), :] = rhs[0:3, :]
    start("low")
    mid_rows = {0: (0, 6), -1: (4, 2), 1: (0, 2)}
    for oy in (0, -1, 1):
        at = sends[("mid", oy)]
        first, count = mid_rows[oy]
        for ref in (s1, u1):
            for c in COMPS:
                for p in range(2):
                    outbox[pl.ds(at, count), :] = ref[c, p + MID_O[0], pl.ds(first + MID_O[1], count), :]
                    at += count
    start("mid")

    hear(1)
    tell(2)
    arrive("dir")
    def direction_rows(plane, first, count, c, value):
        ip, ir = plane + FINE_O[0], pl.ds(first + FINE_O[1], count)
        value = value * f_fine[ip, ir, :]
        after = pltpu.roll(value, LANES - 1, 1)
        x_fine[2 * c, ip, ir, :] = value + after
        x_fine[2 * c + 1, ip, ir, :] = after - value

    for oz in (0, -1, 1):
        for oy in (0, -1, 1):
            planes = {0: range(PLANES), -1: (-1,), 1: (PLANES,)}[oz]
            first, count = {0: (0, 12), -1: (-1, 1), 1: (12, 1)}[oy]
            at = None if (oz, oy) == (0, 0) else receives[("dir", oz, oy)]
            for c in COMPS:
                for p in planes:
                    if at is None:
                        direction_rows(p, first, count, c, dirn[c, p, pl.ds(0, ROWS), :])
                    else:
                        direction_rows(p, first, count, c, inbox[pl.ds(at, count), :])
                        at += count
    fine.voxels((-1, 3), (-1, 7))

    def old_image(p):
        stores = []
        for row in (0, 4):
            ip, ir = fine.at(p, row)
            free = f_fine[ip, ir, :]
            for c in COMPS:
                value = dirn[c, place(p, 0), pl.ds(row, 8), :]
                image = free * fine.applied(c, p, row) + (1.0 - free) * value
                stores.append((old, (c, place(p, 0), pl.ds(row, 8), ALL), image))
        return stores

    over((0, 3), old_image)

    def low_window(name, refs):
        for oz, oy, at in arrivals(name):
            for n, ref in enumerate(refs):
                ref[oz + LOW_O[0], pl.ds(3 * oy + LOW_O[1], 3), :] = inbox[pl.ds(at + 3 * n, 3), :]

    low_window("fixlow", (e_low, f_low, m_low))

    def low_inverse(p):
        stores = []
        for row in (-4, 4):
            ip, ir = low.at(p, row)
            free = f_low[ip, ir, :]
            total = m_low[ip, ir, :]
            for n, entry in enumerate(low.entries):
                stores.append((i_low, (n, ip, ir, ALL), DAMPING / (free * total * entry + (1.0 - free))))
        return stores

    over((-3, 3), low_inverse)

    low_window("low", [s2.at[c] for c in COMPS])
    hear(2)
    tell(3)

    def low_split(planes, rows):
        def body(p):
            stores = []
            for row in rows:
                ip, ir = low.at(p, row)
                free = f_low[ip, ir, :]
                for c in COMPS:
                    stores += low.put_split(c, p, row, free * (low.inverse_of(c, p, row) * s2[c, ip, ir, :]))
            return stores

        over(planes, body, 7)

    ip, ir = low.at(0, 0)
    bottom = [low.inverse_of(c, 0, 0) * s2[c, ip, ir, :] for c in COMPS]
    low_split((-3, 3), (-3, 5))
    for depth in (2, 1, 0):
        low.voxels((-1 - depth, depth), (-1 - depth,))

        def low_step(p, depth=depth):
            row = -depth
            ip, ir = low.at(p, row)
            free = f_low[ip, ir, :]
            stores = []
            for c in COMPS:
                remain = s2[c, ip, ir, :]
                update = low.inverse_of(c, p, row) * remain
                remain = remain - free * low.applied(c, p, row) - (1.0 - free) * update
                stores.append((s2, (c, ip, ir, ALL), remain))
                if depth:
                    stores += low.put_split(c, p, row, free * (low.inverse_of(c, p, row) * remain))
            return stores

        over((-depth, depth), low_step, 5)
        ip, ir = low.at(0, 0)
        for c in COMPS:
            bottom[c] = bottom[c] + low.inverse_of(c, 0, 0) * s2[c, ip, ir, :]

    for c in COMPS:
        for p in range(2):
            for dr in range(2):
                c1[c, p + MID_O[0], pl.ds(MID_O[1] + dr, 3, stride=2), :] = bottom[c][0:3, :]
    for c in COMPS:
        for p in range(2):
            ip, ir = p + MID_O[0], pl.ds(MID_O[1], 6)
            c1[c, ip, ir, :] = c1[c, ip, ir, :] * f_mid[ip, ir, :]
    for oy in (0, -1, 1):
        first, count = {0: (0, 6), -1: (3, 3), 1: (0, 3)}[oy]
        for p in range(2):
            at = sends[("lift", oy, p)]
            for c in COMPS:
                outbox[pl.ds(at, count), :] = c1[c, p + MID_O[0], pl.ds(first + MID_O[1], count), :]
                at += count
    start("lift")
    for oz, oy, at in arrivals("mid"):
        first, count = {0: (0, 6), -1: (-2, 2), 1: (6, 2)}[oy]
        for ref in (s1, u1):
            for c in COMPS:
                for p in range(2):
                    ref[c, p + 2 * oz + MID_O[0], pl.ds(first + MID_O[1], count), :] = inbox[pl.ds(at, count), :]
                    at += count
    left("wide", "far", "dir", "fixlow", "low", "mid")
    for oz, oy, base in arrivals("lift"):
        first, count = {0: (0, 6), -1: (-3, 3), 1: (6, 3)}[oy]
        planes = {-2: (-3,), 2: (4,)}.get(oz, (2 * oz, 2 * oz + 1))
        for n, p in enumerate(planes):
            at = base + n * (9 if oy else 18)
            for c in COMPS:
                c1[c, p + MID_O[0], pl.ds(first + MID_O[1], count), :] = inbox[pl.ds(at, count), :]
                at += count

    def lift_split(p):
        stores = []
        for row in (-3, 5):
            ip, ir = mid.at(p, row)
            for c in COMPS:
                stores += mid.put_split(c, p, row, c1[c, ip, ir, :])
        return stores

    over((-3, 4), lift_split)
    mid.voxels((-3, 3), (-3, 5))

    def mid_second(p):
        stores = []
        for row in (-2, 6):
            ip, ir = mid.at(p, row)
            free = f_mid[ip, ir, :]
            for c in COMPS:
                remain = s1[c, ip, ir, :] - free * mid.applied(c, p, row)
                here = (c, ip, ir, ALL)
                stores.append((u1, here, u1[here] + c1[here] + mid.inverse_of(c, p, row) * remain))
        return stores

    over((-2, 3), mid_second)

    def lift_fine(p):
        stores = []
        for row in (-2, 0):
            ip, ir = mid.at(p, row)
            for c in COMPS:
                value = u1[c, ip, ir, :]
                for dp in range(2):
                    for dr in range(2):
                        out = pl.ds(2 * row + dr + FINE_O[1], 8, stride=2)
                        stores.append((x_fine, (2 * c, place(twice(p, dp), FINE_O[0]), out, ALL), value))
        return stores

    over((-2, 3), lift_fine)

    def lift_parts(p):
        stores = []
        for row in (-4, 4, 12):
            ip, ir = fine.at(p, row)
            free = f_fine[ip, ir, :]
            for c in COMPS:
                stores += fine.put_split(c, p, row, free * x_fine[2 * c, ip, ir, :])
        return stores

    def lift_own(p):
        stores = []
        for row in (0, 8):
            ip, ir = fine.at(p, row)
            free = f_fine[ip, ir, :]
            for c in COMPS:
                part = free * x_fine[2 * c, ip, ir, :]
                own = (c, place(p, 0), pl.ds(row, 8), ALL)
                stores.append((e0, own, e0[own] + part))
        return stores

    over((0, 3), lift_own)
    over((-4, 7), lift_parts)
    fine.voxels((-3, 5), (-3, 5, 13))

    def lift_step(p):
        stores = []
        for row in (-2, 6):
            ip, ir = fine.at(p, row)
            free = f_fine[ip, ir, :]
            weight = i_fine[0, ip, ir, :]
            for c in COMPS:
                remain = s0[c, ip, ir, :] - free * fine.applied(c, p, row)
                stores.append((s0, (c, ip, ir, ALL), remain))
                stores += fine.put_split(c, p, row, free * (weight * remain))
        return stores

    over((-2, 5), lift_step)
    estimate_add(False)
    fine.voxels((-2, 4), (-2, 6))
    over((-1, 4), fine_step((-1, 7), True))
    estimate_add(False)
    fine.voxels((-1, 3), (-1, 7))
    over((0, 3), fine_step((0, 8), False))

    def dots(p, totals):
        totals = list(totals)
        for row in (0, 4):
            ip, ir = p + FINE_O[0], pl.ds(row + FINE_O[1], 8)
            keep = None if row == 0 else row_iota >= 4
            for c in COMPS:
                rows = pl.ds(row, 8)
                z, d, o, r = e0[c, p, rows, :], dirn[c, p, rows, :], old[c, p, rows, :], res[c, p, rows, :]
                new = r - s0[c, ip, ir, :]
                for n, term in enumerate((z * o, d * o, z * new, r * z, r * d)):
                    totals[n] = totals[n] + (term if keep is None else jnp.where(keep, term, 0.0))
        return tuple(totals)

    totals = lax.fori_loop(0, PLANES, dots, (jnp.zeros((8, LANES), jnp.float32),) * 5)
    width = LANES // 8
    owner = lane_iota // width == row_iota
    rows = [jnp.sum(total, axis=0, keepdims=True) for total in totals]
    folded = jnp.concatenate(rows + [jnp.zeros((3, LANES), jnp.float32)], axis=0)
    shift = LANES // 2
    while shift >= width:
        folded = folded + pltpu.roll(folded, shift, 1)
        shift //= 2
    slab_in[pl.ds(0, 1), :] = jnp.sum(jnp.where(owner, folded, 0.0), axis=0, keepdims=True)

    def share(axis, at, count, target, which, meanwhile):
        def copy(k):
            return pltpu.make_async_remote_copy(
                src_ref=target.at[pl.ds(0, 1)],
                dst_ref=target.at[pl.ds(k, 1)],
                send_sem=sum_send.at[which, k],
                recv_sem=sum_recv.at[which, k],
                device_id={axis: lax.rem(at + k, count)},
                device_id_type=MESH,
            )

        for k in order(count):
            copy(k).start()
        meanwhile()
        for k in range(1, count):
            copy(k).wait_recv()
        return jnp.sum(target[...], axis=0, keepdims=True), copy

    def order(count):
        return sorted(range(1, count), key=lambda k: -min(k, count - k))

    def settle():
        left("lift")
        for stage in range(3, STAGES):
            if stage > 3:
                tell(stage)
            hear(stage)

    def settle_slab():
        for k in range(1, slab_count):
            slab_copy(k).wait_send()

    line, slab_copy = share("slab", slab_at, slab_count, slab_in, 0, settle)
    pencil_in[pl.ds(0, 1), :] = line
    whole, pencil_copy = share("pencil", pencil_at, pencil_count, pencil_in, 1, settle_slab)
    summed = jnp.sum(jnp.where(owner, jnp.broadcast_to(whole, (8, LANES)), 0.0), axis=1, keepdims=True)
    t = [summed[n : n + 1, :] for n in range(5)]
    beta = -t[0] / t[1]
    along = t[3] + beta * t[4]
    curvature = t[2] + 2.0 * beta * t[0] + beta * beta * t[1]
    step = along / curvature

    for c in COMPS:
        for p in range(PLANES):
            for first, count in ((0, 8), (8, 4)):
                rows, there_rows = pl.ds(first, count), strided(p, first, count)
                z, d, o, r = e0[c, p, rows, :], dirn[c, p, rows, :], old[c, p, rows, :], res[c, p, rows, :]
                new = r - s0[c, p + FINE_O[0], pl.ds(first + FINE_O[1], count), :]
                nd = z + beta * d
                image = new + beta * o
                next_direction_ref[c, there_rows, :] = nd
                next_solution_ref[c, there_rows, :] = sol_in[c, there_rows, :] + step * nd
                next_residual_ref[c, there_rows, :] = r - step * image
    for k in range(1, pencil_count):
        pencil_copy(k).wait_send()


def per_device(slab_count, pencil_count, solution, residual, direction, material, fixed):
    del fixed
    _, send_rows, _, receive_rows = layout()
    count = len(messages())
    f32 = jnp.float32
    flat = (3, ROWS * PLANES, LANES)
    padded = (3, PLANES, 16, LANES)

    def vmem(*shape):
        return pltpu.VMEM(shape, f32)

    def window(size):
        planes, rows = size
        return planes, rows, LANES

    hbm = pl.BlockSpec(memory_space=pl.ANY)
    out = jax.ShapeDtypeStruct(flat, f32)
    results = pl.pallas_call(
        functools.partial(kernel, slab_count, pencil_count),
        out_shape=(out, out, out),
        in_specs=[hbm] * 4,
        out_specs=(pl.BlockSpec(memory_space=pltpu.VMEM),) * 3,
        scratch_shapes=[
            vmem(*flat),
            vmem(*flat),
            vmem(*flat),
            pltpu.VMEM(flat[1:], jnp.int32),
            vmem(*padded),
            vmem(*padded),
            vmem(3, *window(FINE_S)),
            vmem(*padded),
            vmem(*padded),
            vmem(*window(FINE_S)),
            vmem(*window(FINE_S)),
            vmem(1, *window(FINE_S)),
            vmem(6, *window(FINE_S)),
            vmem(12, *window(FINE_S)),
            vmem(3, *window(MID_S)),
            vmem(3, *window(MID_S)),
            vmem(3, *window(MID_S)),
            vmem(*window(MID_S)),
            vmem(*window(MID_S)),
            vmem(2, *window(MID_S)),
            vmem(6, *window(MID_S)),
            vmem(12, *window(MID_S)),
            vmem(3, *window(LOW_S)),
            vmem(*window(LOW_S)),
            vmem(*window(LOW_S)),
            vmem(*window(LOW_S)),
            vmem(2, *window(LOW_S)),
            vmem(6, *window(LOW_S)),
            vmem(12, *window(LOW_S)),
            vmem(send_rows, LANES),
            vmem(receive_rows, LANES),
            vmem(slab_count, LANES),
            vmem(pencil_count, LANES),
            pltpu.SemaphoreType.DMA((4,)),
            pltpu.SemaphoreType.DMA((count,)),
            pltpu.SemaphoreType.DMA((count,)),
            pltpu.SemaphoreType.DMA((2, max(slab_count, pencil_count))),
            pltpu.SemaphoreType.DMA((2, max(slab_count, pencil_count))),
            pltpu.SemaphoreType.REGULAR((2, STAGES, 2)),
        ],
        compiler_params=pltpu.CompilerParams(collective_id=0, has_side_effects=True, vmem_limit_bytes=24 * 1024 * 1024),
    )(*(pltpu.with_memory_space_constraint(inward(field), pltpu.HBM) for field in (solution, residual, direction, material)))
    results = pl.pallas_call(
        hand_over,
        out_shape=(out, out, out),
        in_specs=[pl.BlockSpec(memory_space=pltpu.VMEM)] * 3,
        out_specs=(hbm, hbm, hbm),
        scratch_shapes=[pltpu.SemaphoreType.DMA((3,))],
        compiler_params=pltpu.CompilerParams(vmem_limit_bytes=24 * 1024 * 1024),
    )(*results)
    return tuple(outward(field) for field in results)


def hand_over(*refs):
    copies = [pltpu.make_async_copy(refs[n], refs[3 + n], refs[6].at[n]) for n in range(3)]
    for copy in copies:
        copy.start()
    for copy in copies:
        copy.wait()


def inward(field):
    axes = (0, 2, 1, 3) if field.ndim == 4 else (1, 0, 2)
    return field.transpose(axes).reshape(field.shape[:-3] + (ROWS * PLANES, LANES))


def outward(field):
    return field.reshape(3, ROWS, PLANES, LANES).transpose(0, 2, 1, 3)


def solution(mesh):
    field = P(None, "slab", "pencil", "parts")
    mask = P("slab", "pencil", "parts")
    return jax.shard_map(
        functools.partial(per_device, mesh.shape["slab"], mesh.shape["pencil"]),
        mesh=mesh,
        in_specs=(field, field, field, mask, mask),
        out_specs=(field, field, field),
        check_vma=False,
    )
```

```python
import functools

import jax
import jax.numpy as jnp
import numpy as np
from jax import lax
from jax.experimental import pallas as pl
from jax.experimental.pallas import tpu as pltpu
from jax.sharding import PartitionSpec as P

SWEEPS = 4
POISSON = 0.3
VOID_MODULUS = 0.1
DAMPING = 0.6
LAME = POISSON / ((1.0 + POISSON) * (1.0 - 2.0 * POISSON))
SHEAR = 0.5 / (1.0 + POISSON)
LANES = 128
COMPS = range(3)
MESH = pl.DeviceIdType.MESH

PLANES, ROWS = 4, 12
REACH, STAGES = 2, 6
FINE_O, FINE_S = (6, 8), (14, 32)
MID_O, MID_S = (3, 4), (8, 24)
LOW_O, LOW_S = (3, 4), (7, 24)


def diagonal_entries(lengths):
    volume = lengths[0] * lengths[1] * lengths[2]
    entries = []
    for c in COMPS:
        total = 0.0
        for axis in COMPS:
            weight = (LAME + 2.0 * SHEAR) if axis == c else SHEAR
            total += weight / lengths[axis] ** 2 / 9.0
        entries.append(total * volume)
    return entries


def scaled(value, factor):
    return value if factor == 1.0 else value * factor


def element_forces(modes, modulus, lengths):
    volume = lengths[0] * lengths[1] * lengths[2]
    inv = [1.0 / length for length in lengths]

    def key(*axes):
        return tuple(1 if axis in axes else 0 for axis in COMPS)

    out = [dict() for _ in COMPS]
    e_norm = modulus * (volume / 16.0)
    e_pair = modulus * (volume / 48.0)
    e_last = modulus * (volume / 144.0)
    stretch = [scaled(modes[c][key(c)], inv[c]) for c in COMPS]
    trace = (stretch[0] + stretch[1] + stretch[2]) * LAME
    for c in COMPS:
        out[c][key(c)] = scaled(trace + stretch[c] * (2.0 * SHEAR), inv[c]) * e_norm
    for b, t in ((0, 1), (0, 2), (1, 2)):
        glide = (scaled(modes[b][key(t)], inv[t]) + scaled(modes[t][key(b)], inv[b])) * SHEAR
        glide = glide * e_norm
        out[b][key(t)] = scaled(glide, inv[t])
        out[t][key(b)] = scaled(glide, inv[b])
    for b in COMPS:
        c, t = [axis for axis in COMPS if axis != b]
        one, two = modes[c][key(c, b)], modes[t][key(t, b)]
        both = (scaled(one, inv[c]) + scaled(two, inv[t])) * LAME
        for comp, mine in ((c, one), (t, two)):
            own = 2.0 * SHEAR * inv[comp] ** 2 + SHEAR * inv[b] ** 2
            out[comp][key(comp, b)] = (scaled(both, inv[comp]) + mine * own) * e_pair
    for c in COMPS:
        b, t = [axis for axis in COMPS if axis != c]
        mine = modes[c][key(b, t)]
        first = scaled(mine, inv[b]) + scaled(modes[b][key(c, t)], inv[c])
        second = scaled(mine, inv[t]) + scaled(modes[t][key(c, b)], inv[c])
        both = scaled(first, inv[b]) + scaled(second, inv[t])
        out[c][key(b, t)] = both * SHEAR * e_pair
    for c in COMPS:
        total = 0.0
        for axis in COMPS:
            total += ((LAME + 2.0 * SHEAR) if axis == c else SHEAR) * inv[axis] ** 2
        out[c][key(0, 1, 2)] = modes[c][key(0, 1, 2)] * total * e_last
    return out


class Plane:
    def __init__(self, count, shift, factor=1):
        self.count, self.shift, self.factor = count, shift, factor

    def __add__(self, other):
        return Plane(self.count, self.shift + other, self.factor)

    def doubled(self, extra):
        return Plane(self.count, 2 * self.shift + extra, 2 * self.factor)

    def index(self, origin=0):
        return self.count * self.factor + (self.shift + origin)


def place(plane, origin):
    return plane.index(origin) if isinstance(plane, Plane) else plane + origin


def twice(plane, extra):
    return plane.doubled(extra) if isinstance(plane, Plane) else 2 * plane + extra


def over(planes, body, group=14):
    count = planes[1] + 1 - planes[0]
    group = max(n for n in range(1, group + 1) if count % n == 0)

    def step(i, _):
        stores = []
        for n in range(group):
            stores += body(Plane(i * group if group > 1 else i, planes[0] + n))
        for ref, index, value in stores:
            ref[index] = value
        return 0

    if group == count:
        stores = [store for n in range(count) for store in body(planes[0] + n)]
        for ref, index, value in stores:
            ref[index] = value
    else:
        lax.fori_loop(0, count // group, step, 0)


ALL = slice(None)


class Level:
    def __init__(self, origin, lengths, split, sums, modulus, inverse, free):
        self.oz, self.oy = origin
        self.lengths = lengths
        self.split, self.sums = split, sums
        self.modulus, self.inverse, self.free = modulus, inverse, free
        entries = diagonal_entries(lengths)
        self.entries = [entries[0]] if lengths[0] == lengths[1] else [entries[0], entries[1]]

    def at(self, plane, row):
        return place(plane, self.oz), pl.ds(row + self.oy, 8)

    def which(self, c):
        return min(c, len(self.entries) - 1)

    def inverse_of(self, c, plane, row):
        p, r = self.at(plane, row)
        return self.inverse[self.which(c), p, r, :]

    def put_split(self, c, plane, row, value):
        p, r = self.at(plane, row)
        after = pltpu.roll(value, LANES - 1, 1)
        return [
            (self.split, (2 * c, p, r, ALL), value + after),
            (self.split, (2 * c + 1, p, r, ALL), after - value),
        ]

    def set_diagonal(self, planes, rows):
        def body(plane):
            stores = []
            for row in rows:
                p, r = self.at(plane, row)
                free = self.free[p, r, :]
                total = self.node_total(plane, row)
                for n, entry in enumerate(self.entries):
                    value = DAMPING / (free * total * entry + (1.0 - free))
                    stores.append((self.inverse, (n, p, r, ALL), value))
            return stores

        over(planes, body)

    def node_total(self, plane, row):
        total = None
        for dz in (-1, 0):
            for dy in (-1, 0):
                p, r = self.at(plane + dz, row + dy)
                piece = self.modulus[p, r, :]
                total = piece if total is None else total + piece
        return total + pltpu.roll(total, 1, 1)

    def voxels(self, planes, rows):
        def pieces(plane, row):
            found = []
            for cm in range(6):
                p, r = self.at(plane, row)
                near = self.split[cm, p, r, :]
                p, r = self.at(plane, row + 1)
                far = self.split[cm, p, r, :]
                found += [near + far, far - near]
            return found

        for row in rows:

            def body(count, carry, row=row):
                plane = Plane(count, planes[0])
                lower, held = carry
                upper = pieces(plane + 1, row)
                p, r = self.at(plane, row)
                modes = []
                for c in COMPS:
                    mine = {}
                    for m in range(2):
                        for iy in range(2):
                            k = (2 * c + m) * 2 + iy
                            if m + iy > 0:
                                mine[(m, iy, 0)] = lower[k] + upper[k]
                            mine[(m, iy, 1)] = upper[k] - lower[k]
                    modes.append(mine)
                forces = element_forces(modes, self.modulus[p, r, :], self.lengths)
                keep = []
                for c in COMPS:
                    for m in range(2):
                        node = []
                        for iy in range(2):
                            k = (2 * c + m) * 2 + iy
                            diff = forces[c][(m, iy, 1)]
                            if m + iy > 0:
                                same = forces[c][(m, iy, 0)]
                                node.append(held[k] + (same - diff))
                                keep.append(same + diff)
                            else:
                                node.append(held[k] - diff)
                                keep.append(diff)
                        self.sums[(2 * c + m) * 2, p, r, :] = node[0] - node[1]
                        self.sums[(2 * c + m) * 2 + 1, p, r, :] = node[0] + node[1]
                return upper, keep

            zero = [jnp.zeros((8, LANES), jnp.float32)] * 12
            carry = (pieces(planes[0], row), zero)
            for count in range(planes[1] + 1 - planes[0]):
                carry = body(count, carry)

    def applied(self, c, plane, row):
        parts = []
        for m in range(2):
            k = (2 * c + m) * 2
            p, r = self.at(plane, row)
            here = self.sums[k, p, r, :]
            p, r = self.at(plane, row - 1)
            parts.append(here + self.sums[k + 1, p, r, :])
        return (parts[0] - parts[1]) + pltpu.roll(parts[0] + parts[1], 1, 1)


NAMES = ("wide", "far", "dir", "fixlow", "low", "mid", "lift")


def messages():
    found = []
    for oz in (0, -1, 1):
        for oy in (0, -1, 1):
            if (oz, oy) != (0, 0):
                found.append(("wide", oz, oy, ("wide", oy), {0: 192, -1: 72, 1: 64}[oy]))
    for oy in (0, -1, 1):
        found.append(("far", -2, oy, ("far", oy), {0: 24, -1: 16, 1: 8}[oy]))
    for oz in (0, -1, 1):
        for oy in (0, -1, 1):
            if (oz, oy) != (0, 0):
                rows = (8 if oy else 40) if oz else 16
                found.append(("dir", oz, oy, ("dir", oz, oy), rows))
    for oz in (0, -1, 1, -2, 2, -3, 3):
        for oy in (0, -1, 1):
            if (oz, oy) != (0, 0):
                found.append(("fixlow", oz, oy, ("fixlow",), 9))
    for oz in (0, -1, 1, -2, 2, -3, 3):
        for oy in (0, -1, 1):
            if (oz, oy) != (0, 0):
                found.append(("low", oz, oy, ("low",), 9))
    for oz in (0, -1, 1):
        for oy in (0, -1, 1):
            if (oz, oy) != (0, 0):
                found.append(("mid", oz, oy, ("mid", oy), 24 if oy else 72))
    for oz in (0, -1, 1, -2, 2):
        for oy in (0, -1, 1):
            if (oz, oy) != (0, 0):
                each = 9 if oy else 18
                part = {-2: 1, 2: 0}.get(oz)
                found.append(("lift", oz, oy, ("lift", oy, part), each if part is not None else 2 * each))
    found.sort(key=lambda m: (NAMES.index(m[0]), -abs(m[1]) - 2 * abs(m[2])))
    return found


def layout():
    sends, receives = {}, {}
    at_send = at_receive = 0
    for oy in (0, -1, 1):
        each = 9 if oy else 18
        sends[("lift", oy, None)] = at_send
        sends[("lift", oy, 0)] = at_send
        sends[("lift", oy, 1)] = at_send + each
        at_send += -(-2 * each // 8) * 8
    for name, oz, oy, key, rows in messages():
        if key not in sends:
            sends[key] = at_send
            at_send += -(-rows // 8) * 8
        receives[(name, oz, oy)] = at_receive
        at_receive += -(-rows // 8) * 8
    return sends, at_send, receives, at_receive


def kernel(
    slab_count,
    pencil_count,
    solution_ref,
    residual_ref,
    direction_ref,
    material_ref,
    next_solution_ref,
    next_residual_ref,
    next_direction_ref,
    sol_in,
    res_in,
    dir_in,
    mat,
    res,
    dirn,
    s0,
    e0,
    old,
    e_fine,
    f_fine,
    i_fine,
    x_fine,
    b_fine,
    s1,
    u1,
    c1,
    e_mid,
    f_mid,
    i_mid,
    x_mid,
    b_mid,
    s2,
    e_low,
    f_low,
    m_low,
    i_low,
    x_low,
    b_low,
    outbox,
    inbox,
    slab_in,
    pencil_in,
    local_sem,
    send_sem,
    recv_sem,
    sum_send,
    sum_recv,
    word_sem,
):
    slab_at, pencil_at = lax.axis_index("slab"), lax.axis_index("pencil")
    sends, _, receives, _ = layout()
    all_messages = messages()
    fine = Level(FINE_O, (1.0, 1.0, 1.0), x_fine, b_fine, e_fine, i_fine, f_fine)
    mid = Level(MID_O, (1.0, 2.0, 2.0), x_mid, b_mid, e_mid, i_mid, f_mid)
    low = Level(LOW_O, (1.0, 4.0, 4.0), x_low, b_low, e_low, i_low, f_low)

    loads = [
        pltpu.make_async_copy(source, target, local_sem.at[n])
        for n, (source, target) in enumerate(
            ((material_ref, mat), (residual_ref, res_in), (direction_ref, dir_in), (solution_ref, sol_in))
        )
    ]
    for load in loads:
        load.start()

    def there(oz, oy):
        z, y = slab_at + oz, pencil_at + oy
        return (z >= 0) & (z < slab_count) & (y >= 0) & (y < pencil_count)

    inbox[...] = jnp.zeros_like(inbox)

    barrier = pltpu.get_barrier_semaphore()
    greeted = jnp.int32(0)
    for oz in range(-REACH, REACH + 1):
        for oy in (-1, 0, 1):
            if (oz, oy) != (0, 0):
                near = there(oz, oy)
                greeted = greeted + jnp.where(near, 1, 0)

                @pl.when(near)
                def _(oz=oz, oy=oy):
                    pl.semaphore_signal(
                        barrier,
                        inc=1,
                        device_id={"slab": slab_at + oz, "pencil": pencil_at + oy},
                        device_id_type=MESH,
                    )

    def stages(count, known):
        steps = []
        while known < count - 1:
            step = min(known, count - 1 - known)
            steps.append(step)
            known += step
        return steps

    plan = [("slab", stages(slab_count, REACH)), ("pencil", stages(pencil_count, 1))]

    def sides(axis, step):
        return [(step * sign if axis == "slab" else 0, step * sign if axis == "pencil" else 0) for sign in (-1, 1)]

    def tell(stage):
        for which, (axis, steps) in enumerate(plan):
            if stage < len(steps):
                for side, (oz, oy) in enumerate(sides(axis, steps[stage])):

                    @pl.when(there(oz, oy))
                    def _(oz=oz, oy=oy):
                        pl.semaphore_signal(
                            word_sem.at[which, stage, 1 - side],
                            inc=1,
                            device_id={"slab": slab_at + oz, "pencil": pencil_at + oy},
                            device_id_type=MESH,
                        )

    def hear(stage):
        for which, (axis, steps) in enumerate(plan):
            if stage < len(steps):
                for side, (oz, oy) in enumerate(sides(axis, steps[stage])):

                    @pl.when(there(oz, oy))
                    def _():
                        pl.semaphore_wait(word_sem.at[which, stage, side], 1)

    for ref in (s0, e_fine, x_fine, b_fine, s1, u1, c1, x_mid, b_mid, s2, e_low, f_low, m_low, i_low, x_low, b_low):
        ref[...] = jnp.zeros_like(ref)
    e_mid[...] = jnp.zeros_like(e_mid)
    f_mid[...] = jnp.zeros_like(f_mid)
    i_mid[...] = jnp.zeros_like(i_mid)
    f_fine[...] = jnp.zeros_like(f_fine)
    i_fine[...] = jnp.zeros_like(i_fine)

    def copy_of(number, oz, oy, key, rows):
        name = all_messages[number][0]
        return pltpu.make_async_remote_copy(
            src_ref=outbox.at[pl.ds(sends[key], rows)],
            dst_ref=inbox.at[pl.ds(receives[(name, oz, oy)], rows)],
            send_sem=send_sem.at[number],
            recv_sem=recv_sem.at[number],
            device_id={"slab": slab_at - oz, "pencil": pencil_at - oy},
            device_id_type=MESH,
        )

    def start(*names):
        for number, (name, oz, oy, key, rows) in enumerate(all_messages):
            if name in names:

                @pl.when(there(-oz, -oy))
                def _(number=number, oz=oz, oy=oy, key=key, rows=rows):
                    copy_of(number, oz, oy, key, rows).start()

    def arrive(*names):
        for number, (name, oz, oy, key, rows) in enumerate(all_messages):
            if name in names:

                @pl.when(there(oz, oy))
                def _(number=number, oz=oz, oy=oy, key=key, rows=rows):
                    copy_of(number, oz, oy, key, rows).wait_recv()

    def arrivals(*names):
        for number, (name, oz, oy, key, rows) in reversed(list(enumerate(all_messages))):
            if name in names:

                @pl.when(there(oz, oy))
                def _(number=number, oz=oz, oy=oy, key=key, rows=rows):
                    copy_of(number, oz, oy, key, rows).wait_recv()

                yield oz, oy, receives[(name, oz, oy)]

    def left(*names):
        for number, (name, oz, oy, key, rows) in enumerate(all_messages):
            if name in names:

                @pl.when(there(-oz, -oy))
                def _(number=number, oz=oz, oy=oy, key=key, rows=rows):
                    copy_of(number, oz, oy, key, rows).wait_send()

    def strided(p, first, count):
        return pl.ds(p + PLANES * first, count, stride=PLANES)

    def planes_first(source, target):
        for c in COMPS:
            for p in range(PLANES):
                for first, count in ((0, 8), (8, 4)):
                    target[c, p, pl.ds(first, count), :] = source[c, strided(p, first, count), :]

    loads[0].wait()
    loads[1].wait()
    planes_first(res_in, res)

    taken_rows = {0: (0, 12), -1: (8, 4), 1: (0, 4)}
    voxel_rows = {0: (0, 12), -1: (6, 6), 1: (0, 4)}
    for oy in (0, -1, 1):
        at = sends[("wide", oy)]
        first, count = taken_rows[oy]
        for c in COMPS:
            for p in range(PLANES):
                outbox[pl.ds(at, count), :] = res[c, p, pl.ds(first, count), :]
                at += count
        first, count = voxel_rows[oy]
        for p in range(PLANES):
            outbox[pl.ds(at, count), :] = (mat[strided(p, first, count), :] == 1).astype(jnp.float32)
            at += count
        at = sends[("far", oy)]
        for p in (2, 3):
            outbox[pl.ds(at, count), :] = (mat[strided(p, first, count), :] == 1).astype(jnp.float32)
            at += count

    pl.semaphore_wait(barrier, greeted)
    start("wide", "far")
    tell(0)

    loads[2].wait()
    loads[3].wait()
    planes_first(dir_in, dirn)
    for name, oz, oy, key, rows in all_messages:
        if name == "dir":
            at = sends[key]
            planes = {0: range(PLANES), -1: (3,), 1: (0,)}[oz]
            first, count = {0: (0, 12), -1: (11, 1), 1: (0, 1)}[oy]
            for c in COMPS:
                for p in planes:
                    outbox[pl.ds(at, count), :] = dirn[c, p, pl.ds(first, count), :]
                    at += count

    for c in COMPS:
        for p in range(PLANES):
            s0[c, p + FINE_O[0], pl.ds(FINE_O[1], ROWS), :] = res[c, p, pl.ds(0, ROWS), :]
    for p in range(PLANES):
        for first, count in ((0, 8), (8, 4)):
            e_fine[p + FINE_O[0], pl.ds(first + FINE_O[1], count), :] = (mat[strided(p, first, count), :] == 1).astype(
                jnp.float32
            )

    for oz, oy, at in arrivals("wide"):
        first, count = {0: (0, 12), -1: (-4, 4), 1: (12, 4)}[oy]
        for c in COMPS:
            for p in range(PLANES):
                s0[c, p + oz * PLANES + FINE_O[0], pl.ds(first + FINE_O[1], count), :] = inbox[pl.ds(at, count), :]
                at += count
        first, count = {0: (0, 12), -1: (-6, 6), 1: (12, 4)}[oy]
        for p in range(PLANES):
            e_fine[p + oz * PLANES + FINE_O[0], pl.ds(first + FINE_O[1], count), :] = inbox[pl.ds(at, count), :]
            at += count
    start("dir")
    hear(0)
    tell(1)
    for _, oy, at in arrivals("far"):
        first, count = {0: (0, 12), -1: (-6, 6), 1: (12, 4)}[oy]
        for p in (-6, -5):
            e_fine[p + FINE_O[0], pl.ds(first + FINE_O[1], count), :] = inbox[pl.ds(at, count), :]
            at += count

    total_planes, total_rows = slab_count * PLANES, pencil_count * ROWS
    row_iota = lax.broadcasted_iota(jnp.int32, (8, LANES), 0)
    lane_iota = lax.broadcasted_iota(jnp.int32, (8, LANES), 1)

    def moduli_body(p):
        plane = slab_at * PLANES + place(p, 0)
        plane_ok = (plane >= 0) & (plane < total_planes - 1)
        stores = []
        for row in (-8, 0, 8):
            ip, ir = fine.at(p, row)
            rows = row_iota + (pencil_at * ROWS + row)
            keep = (rows >= 0) & (rows < total_rows - 1) & (lane_iota < LANES - 1) & plane_ok
            value = jnp.where(e_fine[ip, ir, :] > 0.5, 1.0, VOID_MODULUS)
            stores.append((e_fine, (ip, ir, ALL), jnp.where(keep, value, 0.0)))
        return stores

    over((-6, 7), moduli_body)

    def fine_body(p):
        plane = slab_at * PLANES + place(p, 0)
        inside = (plane > 0) & (plane < total_planes - 1)
        stores = []
        for row in (-5, 3, 8):
            ip, ir = fine.at(p, row)
            total = fine.node_total(p, row)
            free = jnp.where((total > 0.9) & inside, 1.0, 0.0)
            weight = DAMPING / (free * total * fine.entries[0] + (1.0 - free))
            stores += [(f_fine, (ip, ir, ALL), free), (i_fine, (0, ip, ir, ALL), weight)]
        return stores

    over((-5, 7), fine_body)

    def first_update(p):
        stores = []
        for row in (-4, 4, 8):
            ip, ir = fine.at(p, row)
            weight = i_fine[0, ip, ir, :] * f_fine[ip, ir, :]
            for c in COMPS:
                stores += fine.put_split(c, p, row, s0[c, ip, ir, :] * weight)
        return stores

    over((-4, 7), first_update)

    def halves(ref, c, p, row):
        found = []
        for dp in range(2):
            for dr in range(2):
                r = pl.ds(2 * row + dr + FINE_O[1], 8, stride=2)
                ip = place(twice(p, dp), FINE_O[0])
                found.append(ref[ip, r, :] if c is None else ref[c, ip, r, :])
        return found

    def mid_moduli(p):
        plane_ok = slab_at * (PLANES // 2) + place(p, 0) < total_planes // 2 - 1
        stores = []
        for row in (-3, 0):
            ip, ir = mid.at(p, row)
            a, b, c, d = halves(e_fine, None, p, row)
            rows = row_iota + (pencil_at * (ROWS // 2) + row)
            keep = (rows < total_rows // 2 - 1) & plane_ok
            stores.append((e_mid, (ip, ir, ALL), jnp.where(keep, (a + b + c + d) * 0.25, 0.0)))
        return stores

    over((-3, 3), mid_moduli)

    def mid_free(p):
        stores = []
        for row in (-2, 0):
            ip, ir = mid.at(p, row)
            a, b, c, d = halves(f_fine, None, p, row)
            stores.append((f_mid, (ip, ir, ALL), jnp.maximum(jnp.maximum(a, b), jnp.maximum(c, d))))
        return stores

    over((-2, 3), mid_free)
    mid.set_diagonal((-2, 3), (-2, 0))

    def mid_pair(ref, c, p, row):
        found = []
        for dp in range(2):
            for dr in range(2):
                r = pl.ds(2 * row + dr + MID_O[1], 8, stride=2)
                ip = place(twice(p, dp), MID_O[0])
                found.append(ref[ip, r, :] if c is None else ref[c, ip, r, :])
        return found

    for p in (-1, 0):
        ip, ir = low.at(p, -1)
        a, b, c, d = mid_pair(e_mid, None, p, -1)
        rows = row_iota + (pencil_at * (ROWS // 4) - 1)
        keep = (rows < total_rows // 4 - 1) & (slab_at * (PLANES // 4) + p < total_planes // 4 - 1) & (row_iota < 4)
        e_low[ip, ir, :] = jnp.where(keep, (a + b + c + d) * 0.25, 0.0)
    a, b, c, d = mid_pair(f_mid, None, 0, 0)
    ip, ir = low.at(0, 0)
    f_low[ip, ir, :] = jnp.where(row_iota < 3, jnp.maximum(jnp.maximum(a, b), jnp.maximum(c, d)), 0.0)
    m_low[ip, ir, :] = jnp.where(row_iota < 3, low.node_total(0, 0), 0.0)
    at = sends[("fixlow",)]
    own_rows = pl.ds(LOW_O[1], 3)
    for n, ref in enumerate((e_low, f_low, m_low)):
        outbox[pl.ds(at + 3 * n, 3), :] = ref[LOW_O[0], own_rows, :]
    start("fixlow")

    fine.voxels((-4, 6), (-4, 4, 12))

    def fine_step(rows, starting):
        def body(p):
            stores = []
            for row in rows:
                ip, ir = fine.at(p, row)
                free = f_fine[ip, ir, :]
                weight = i_fine[0, ip, ir, :]
                for c in COMPS:
                    remain = s0[c, ip, ir, :]
                    update = weight * remain
                    remain = remain - free * fine.applied(c, p, row) - (1.0 - free) * update
                    stores.append((s0, (c, ip, ir, ALL), remain))
                    if starting:
                        stores += fine.put_split(c, p, row, free * (weight * remain))
            return stores

        return body

    def estimate_add(starting):
        def body(p):
            stores = []
            for row in (0, 8):
                ip, ir = fine.at(p, row)
                weight = i_fine[0, ip, ir, :]
                for c in COMPS:
                    update = weight * s0[c, ip, ir, :]
                    own = (c, place(p, 0), pl.ds(row, 8), ALL)
                    stores.append((e0, own, update if starting else e0[own] + update))
            return stores

        over((0, 3), body)

    estimate_add(True)
    over((-3, 6), fine_step((-3, 5, 13), True))
    estimate_add(False)
    fine.voxels((-3, 5), (-3, 5, 13))
    over((-2, 5), fine_step((-2, 6), False))

    def mid_first(p):
        ip, ir = mid.at(p, -1)
        free = f_mid[ip, ir, :]
        masks = halves(f_fine, None, p, -1)
        stores = []
        for c in COMPS:
            parts = halves(s0, c, p, -1)
            rhs = free * (
                (parts[0] * masks[0] + parts[1] * masks[1]) + (parts[2] * masks[2] + parts[3] * masks[3])
            )
            update = mid.inverse_of(c, p, -1) * rhs
            stores += [(s1, (c, ip, ir, ALL), rhs), (u1, (c, ip, ir, ALL), update)]
            stores += mid.put_split(c, p, -1, free * update)
        return stores

    over((-1, 2), mid_first)
    mid.voxels((-1, 1), (-1,))

    def mid_remain(p):
        ip, ir = mid.at(p, 0)
        free = f_mid[ip, ir, :]
        stores = []
        for c in COMPS:
            remain = s1[c, ip, ir, :] - free * mid.applied(c, p, 0) - (1.0 - free) * u1[c, ip, ir, :]
            stores.append((s1, (c, ip, ir, ALL), remain))
        return stores

    over((0, 1), mid_remain)

    masks = mid_pair(f_mid, None, 0, 0)
    ip, ir = low.at(0, 0)
    free = f_low[ip, ir, :]
    at = sends[("low",)]
    for c in COMPS:
        parts = mid_pair(s1, c, 0, 0)
        rhs = free * ((parts[0] * masks[0] + parts[1] * masks[1]) + (parts[2] * masks[2] + parts[3] * masks[3]))
        rhs = jnp.where(row_iota < 3, rhs, 0.0)
        s2[c, ip, ir, :] = rhs
        outbox[pl.ds(at + 3 * c, 3), :] = rhs[0:3, :]
    start("low")
    mid_rows = {0: (0, 6), -1: (4, 2), 1: (0, 2)}
    for oy in (0, -1, 1):
        at = sends[("mid", oy)]
        first, count = mid_rows[oy]
        for ref in (s1, u1):
            for c in COMPS:
                for p in range(2):
                    outbox[pl.ds(at, count), :] = ref[c, p + MID_O[0], pl.ds(first + MID_O[1], count), :]
                    at += count
    start("mid")

    hear(1)
    tell(2)
    arrive("dir")
    def direction_rows(plane, first, count, c, value):
        ip, ir = plane + FINE_O[0], pl.ds(first + FINE_O[1], count)
        value = value * f_fine[ip, ir, :]
        after = pltpu.roll(value, LANES - 1, 1)
        x_fine[2 * c, ip, ir, :] = value + after
        x_fine[2 * c + 1, ip, ir, :] = after - value

    for oz in (0, -1, 1):
        for oy in (0, -1, 1):
            planes = {0: range(PLANES), -1: (-1,), 1: (PLANES,)}[oz]
            first, count = {0: (0, 12), -1: (-1, 1), 1: (12, 1)}[oy]
            at = None if (oz, oy) == (0, 0) else receives[("dir", oz, oy)]
            for c in COMPS:
                for p in planes:
                    if at is None:
                        direction_rows(p, first, count, c, dirn[c, p, pl.ds(0, ROWS), :])
                    else:
                        direction_rows(p, first, count, c, inbox[pl.ds(at, count), :])
                        at += count
    fine.voxels((-1, 3), (-1, 7))

    def old_image(p):
        stores = []
        for row in (0, 4):
            ip, ir = fine.at(p, row)
            free = f_fine[ip, ir, :]
            for c in COMPS:
                value = dirn[c, place(p, 0), pl.ds(row, 8), :]
                image = free * fine.applied(c, p, row) + (1.0 - free) * value
                stores.append((old, (c, place(p, 0), pl.ds(row, 8), ALL), image))
        return stores

    over((0, 3), old_image)

    def low_window(name, refs):
        for oz, oy, at in arrivals(name):
            for n, ref in enumerate(refs):
                ref[oz + LOW_O[0], pl.ds(3 * oy + LOW_O[1], 3), :] = inbox[pl.ds(at + 3 * n, 3), :]

    low_window("fixlow", (e_low, f_low, m_low))

    def low_inverse(p):
        stores = []
        for row in (-4, 4):
            ip, ir = low.at(p, row)
            free = f_low[ip, ir, :]
            total = m_low[ip, ir, :]
            for n, entry in enumerate(low.entries):
                stores.append((i_low, (n, ip, ir, ALL), DAMPING / (free * total * entry + (1.0 - free))))
        return stores

    over((-3, 3), low_inverse)

    low_window("low", [s2.at[c] for c in COMPS])
    hear(2)
    tell(3)

    def low_split(planes, rows):
        def body(p):
            stores = []
            for row in rows:
                ip, ir = low.at(p, row)
                free = f_low[ip, ir, :]
                for c in COMPS:
                    stores += low.put_split(c, p, row, free * (low.inverse_of(c, p, row) * s2[c, ip, ir, :]))
            return stores

        over(planes, body, 7)

    ip, ir = low.at(0, 0)
    bottom = [low.inverse_of(c, 0, 0) * s2[c, ip, ir, :] for c in COMPS]
    low_split((-3, 3), (-3, 5))
    for depth in (2, 1, 0):
        low.voxels((-1 - depth, depth), (-1 - depth,))

        def low_step(p, depth=depth):
            row = -depth
            ip, ir = low.at(p, row)
            free = f_low[ip, ir, :]
            stores = []
            for c in COMPS:
                remain = s2[c, ip, ir, :]
                update = low.inverse_of(c, p, row) * remain
                remain = remain - free * low.applied(c, p, row) - (1.0 - free) * update
                stores.append((s2, (c, ip, ir, ALL), remain))
                if depth:
                    stores += low.put_split(c, p, row, free * (low.inverse_of(c, p, row) * remain))
            return stores

        over((-depth, depth), low_step, 5)
        ip, ir = low.at(0, 0)
        for c in COMPS:
            bottom[c] = bottom[c] + low.inverse_of(c, 0, 0) * s2[c, ip, ir, :]

    for c in COMPS:
        for p in range(2):
            for dr in range(2):
                c1[c, p + MID_O[0], pl.ds(MID_O[1] + dr, 3, stride=2), :] = bottom[c][0:3, :]
    for c in COMPS:
        for p in range(2):
            ip, ir = p + MID_O[0], pl.ds(MID_O[1], 6)
            c1[c, ip, ir, :] = c1[c, ip, ir, :] * f_mid[ip, ir, :]
    for oy in (0, -1, 1):
        first, count = {0: (0, 6), -1: (3, 3), 1: (0, 3)}[oy]
        for p in range(2):
            at = sends[("lift", oy, p)]
            for c in COMPS:
                outbox[pl.ds(at, count), :] = c1[c, p + MID_O[0], pl.ds(first + MID_O[1], count), :]
                at += count
    start("lift")
    for oz, oy, at in arrivals("mid"):
        first, count = {0: (0, 6), -1: (-2, 2), 1: (6, 2)}[oy]
        for ref in (s1, u1):
            for c in COMPS:
                for p in range(2):
                    ref[c, p + 2 * oz + MID_O[0], pl.ds(first + MID_O[1], count), :] = inbox[pl.ds(at, count), :]
                    at += count
    left("wide", "far", "dir", "fixlow", "low", "mid")
    for oz, oy, base in arrivals("lift"):
        first, count = {0: (0, 6), -1: (-3, 3), 1: (6, 3)}[oy]
        planes = {-2: (-3,), 2: (4,)}.get(oz, (2 * oz, 2 * oz + 1))
        for n, p in enumerate(planes):
            at = base + n * (9 if oy else 18)
            for c in COMPS:
                c1[c, p + MID_O[0], pl.ds(first + MID_O[1], count), :] = inbox[pl.ds(at, count), :]
                at += count

    def lift_split(p):
        stores = []
        for row in (-3, 5):
            ip, ir = mid.at(p, row)
            for c in COMPS:
                stores += mid.put_split(c, p, row, c1[c, ip, ir, :])
        return stores

    over((-3, 4), lift_split)
    mid.voxels((-3, 3), (-3, 5))

    def mid_second(p):
        stores = []
        for row in (-2, 6):
            ip, ir = mid.at(p, row)
            free = f_mid[ip, ir, :]
            for c in COMPS:
                remain = s1[c, ip, ir, :] - free * mid.applied(c, p, row)
                here = (c, ip, ir, ALL)
                stores.append((u1, here, u1[here] + c1[here] + mid.inverse_of(c, p, row) * remain))
        return stores

    over((-2, 3), mid_second)

    def lift_fine(p):
        stores = []
        for row in (-2, 0):
            ip, ir = mid.at(p, row)
            for c in COMPS:
                value = u1[c, ip, ir, :]
                for dp in range(2):
                    for dr in range(2):
                        out = pl.ds(2 * row + dr + FINE_O[1], 8, stride=2)
                        stores.append((x_fine, (2 * c, place(twice(p, dp), FINE_O[0]), out, ALL), value))
        return stores

    over((-2, 3), lift_fine)

    def lift_parts(p):
        stores = []
        for row in (-4, 4, 12):
            ip, ir = fine.at(p, row)
            free = f_fine[ip, ir, :]
            for c in COMPS:
                stores += fine.put_split(c, p, row, free * x_fine[2 * c, ip, ir, :])
        return stores

    def lift_own(p):
        stores = []
        for row in (0, 8):
            ip, ir = fine.at(p, row)
            free = f_fine[ip, ir, :]
            for c in COMPS:
                part = free * x_fine[2 * c, ip, ir, :]
                own = (c, place(p, 0), pl.ds(row, 8), ALL)
                stores.append((e0, own, e0[own] + part))
        return stores

    over((0, 3), lift_own)
    over((-4, 7), lift_parts)
    fine.voxels((-3, 5), (-3, 5, 13))

    def lift_step(p):
        stores = []
        for row in (-2, 6):
            ip, ir = fine.at(p, row)
            free = f_fine[ip, ir, :]
            weight = i_fine[0, ip, ir, :]
            for c in COMPS:
                remain = s0[c, ip, ir, :] - free * fine.applied(c, p, row)
                stores.append((s0, (c, ip, ir, ALL), remain))
                stores += fine.put_split(c, p, row, free * (weight * remain))
        return stores

    over((-2, 5), lift_step)
    estimate_add(False)
    fine.voxels((-2, 4), (-2, 6))
    over((-1, 4), fine_step((-1, 7), True))
    estimate_add(False)
    fine.voxels((-1, 3), (-1, 7))
    over((0, 3), fine_step((0, 8), False))

    def dots(p, totals):
        totals = list(totals)
        for row in (0, 4):
            ip, ir = p + FINE_O[0], pl.ds(row + FINE_O[1], 8)
            keep = None if row == 0 else row_iota >= 4
            for c in COMPS:
                rows = pl.ds(row, 8)
                z, d, o, r = e0[c, p, rows, :], dirn[c, p, rows, :], old[c, p, rows, :], res[c, p, rows, :]
                new = r - s0[c, ip, ir, :]
                for n, term in enumerate((z * o, d * o, z * new, r * z, r * d)):
                    totals[n] = totals[n] + (term if keep is None else jnp.where(keep, term, 0.0))
        return tuple(totals)

    totals = lax.fori_loop(0, PLANES, dots, (jnp.zeros((8, LANES), jnp.float32),) * 5)
    width = LANES // 8
    owner = lane_iota // width == row_iota
    rows = [jnp.sum(total, axis=0, keepdims=True) for total in totals]
    folded = jnp.concatenate(rows + [jnp.zeros((3, LANES), jnp.float32)], axis=0)
    shift = LANES // 2
    while shift >= width:
        folded = folded + pltpu.roll(folded, shift, 1)
        shift //= 2
    slab_in[pl.ds(0, 1), :] = jnp.sum(jnp.where(owner, folded, 0.0), axis=0, keepdims=True)

    def share(axis, at, count, target, which, meanwhile):
        def copy(k):
            return pltpu.make_async_remote_copy(
                src_ref=target.at[pl.ds(0, 1)],
                dst_ref=target.at[pl.ds(k, 1)],
                send_sem=sum_send.at[which, k],
                recv_sem=sum_recv.at[which, k],
                device_id={axis: lax.rem(at + k, count)},
                device_id_type=MESH,
            )

        for k in order(count):
            copy(k).start()
        meanwhile()
        for k in range(1, count):
            copy(k).wait_recv()
        return jnp.sum(target[...], axis=0, keepdims=True), copy

    def order(count):
        return sorted(range(1, count), key=lambda k: -min(k, count - k))

    def settle():
        left("lift")
        for stage in range(3, STAGES):
            if stage > 3:
                tell(stage)
            hear(stage)

    def settle_slab():
        for k in range(1, slab_count):
            slab_copy(k).wait_send()

    line, slab_copy = share("slab", slab_at, slab_count, slab_in, 0, settle)
    pencil_in[pl.ds(0, 1), :] = line
    whole, pencil_copy = share("pencil", pencil_at, pencil_count, pencil_in, 1, settle_slab)
    summed = jnp.sum(jnp.where(owner, jnp.broadcast_to(whole, (8, LANES)), 0.0), axis=1, keepdims=True)
    t = [summed[n : n + 1, :] for n in range(5)]
    beta = -t[0] / t[1]
    along = t[3] + beta * t[4]
    curvature = t[2] + 2.0 * beta * t[0] + beta * beta * t[1]
    step = along / curvature

    for c in COMPS:
        for p in range(PLANES):
            for first, count in ((0, 8), (8, 4)):
                rows, there_rows = pl.ds(first, count), strided(p, first, count)
                z, d, o, r = e0[c, p, rows, :], dirn[c, p, rows, :], old[c, p, rows, :], res[c, p, rows, :]
                new = r - s0[c, p + FINE_O[0], pl.ds(first + FINE_O[1], count), :]
                nd = z + beta * d
                image = new + beta * o
                next_direction_ref[c, there_rows, :] = nd
                next_solution_ref[c, there_rows, :] = sol_in[c, there_rows, :] + step * nd
                next_residual_ref[c, there_rows, :] = r - step * image
    for k in range(1, pencil_count):
        pencil_copy(k).wait_send()


def per_device(slab_count, pencil_count, solution, residual, direction, material, fixed):
    del fixed
    _, send_rows, _, receive_rows = layout()
    count = len(messages())
    f32 = jnp.float32
    flat = (3, ROWS * PLANES, LANES)
    padded = (3, PLANES, 16, LANES)

    def vmem(*shape):
        return pltpu.VMEM(shape, f32)

    def window(size):
        planes, rows = size
        return planes, rows, LANES

    hbm = pl.BlockSpec(memory_space=pl.ANY)
    out = jax.ShapeDtypeStruct(flat, f32)
    results = pl.pallas_call(
        functools.partial(kernel, slab_count, pencil_count),
        out_shape=(out, out, out),
        in_specs=[hbm] * 4,
        out_specs=(pl.BlockSpec(memory_space=pltpu.VMEM),) * 3,
        scratch_shapes=[
            vmem(*flat),
            vmem(*flat),
            vmem(*flat),
            pltpu.VMEM(flat[1:], jnp.int32),
            vmem(*padded),
            vmem(*padded),
            vmem(3, *window(FINE_S)),
            vmem(*padded),
            vmem(*padded),
            vmem(*window(FINE_S)),
            vmem(*window(FINE_S)),
            vmem(1, *window(FINE_S)),
            vmem(6, *window(FINE_S)),
            vmem(12, *window(FINE_S)),
            vmem(3, *window(MID_S)),
            vmem(3, *window(MID_S)),
            vmem(3, *window(MID_S)),
            vmem(*window(MID_S)),
            vmem(*window(MID_S)),
            vmem(2, *window(MID_S)),
            vmem(6, *window(MID_S)),
            vmem(12, *window(MID_S)),
            vmem(3, *window(LOW_S)),
            vmem(*window(LOW_S)),
            vmem(*window(LOW_S)),
            vmem(*window(LOW_S)),
            vmem(2, *window(LOW_S)),
            vmem(6, *window(LOW_S)),
            vmem(12, *window(LOW_S)),
            vmem(send_rows, LANES),
            vmem(receive_rows, LANES),
            vmem(slab_count, LANES),
            vmem(pencil_count, LANES),
            pltpu.SemaphoreType.DMA((4,)),
            pltpu.SemaphoreType.DMA((count,)),
            pltpu.SemaphoreType.DMA((count,)),
            pltpu.SemaphoreType.DMA((2, max(slab_count, pencil_count))),
            pltpu.SemaphoreType.DMA((2, max(slab_count, pencil_count))),
            pltpu.SemaphoreType.REGULAR((2, STAGES, 2)),
        ],
        compiler_params=pltpu.CompilerParams(collective_id=0, has_side_effects=True, vmem_limit_bytes=24 * 1024 * 1024),
    )(*(pltpu.with_memory_space_constraint(inward(field), pltpu.HBM) for field in (solution, residual, direction, material)))
    results = pl.pallas_call(
        hand_over,
        out_shape=(out, out, out),
        in_specs=[pl.BlockSpec(memory_space=pltpu.VMEM)] * 3,
        out_specs=(hbm, hbm, hbm),
        scratch_shapes=[pltpu.SemaphoreType.DMA((3,))],
        compiler_params=pltpu.CompilerParams(vmem_limit_bytes=24 * 1024 * 1024),
    )(*results)
    return tuple(outward(field) for field in results)


def hand_over(*refs):
    copies = [pltpu.make_async_copy(refs[n], refs[3 + n], refs[6].at[n]) for n in range(3)]
    for copy in copies:
        copy.start()
    for copy in copies:
        copy.wait()


def inward(field):
    axes = (0, 2, 1, 3) if field.ndim == 4 else (1, 0, 2)
    return field.transpose(axes).reshape(field.shape[:-3] + (ROWS * PLANES, LANES))


def outward(field):
    return field.reshape(3, ROWS, PLANES, LANES).transpose(0, 2, 1, 3)


def solution(mesh):
    field = P(None, "slab", "pencil", "parts")
    mask = P("slab", "pencil", "parts")
    return jax.shard_map(
        functools.partial(per_device, mesh.shape["slab"], mesh.shape["pencil"]),
        mesh=mesh,
        in_specs=(field, field, field, mask, mask),
        out_specs=(field, field, field),
        check_vma=False,
    )
```
